256 devices in a mesh: rep: 32 (over z_hi, y, x), dom: 8 (over z_lo, core).
Axes of the slice: x: 4, y: 4, z: 8 (z_hi: 2, z_lo: 4; z = z_hi * 4 + z_lo), core: 2. Of those that a mesh axis runs over, the one named last changes fastest.
Arguments:
- protein_pos: float32 [3, 524288], P(None, ('rep', 'dom')), parts along dimension 1, may hold values from -4 to 4, as said below
- protein_vel: float32 [3, 524288], P(None, ('rep', 'dom')), parts along dimension 1, may hold values from -3 to 3
- inv_mass: float32 [524288], P(('rep', 'dom')), parts along dimension 0, may hold values from 0.0625 to 1
- bond_atoms: int32 [2, 327680], P(None, ('rep', 'dom')), parts along dimension 1, may hold values from 0 to 2047, as said below
- left_atoms: int32 [98304], P(('rep', 'dom')), parts along dimension 0, may hold values from 0 to 2047, as said below
- right_atoms: int32 [98304], P(('rep', 'dom')), parts along dimension 0, may hold values from 0 to 2047, as said below
- water_pos: float32 [9, 262144], P(None, ('rep', 'dom')), parts along dimension 1, may hold values from -3.2 to 3.2, as said below
- water_vel: float32 [9, 262144], P(None, ('rep', 'dom')), parts along dimension 1, may hold values from -3 to 3
Outputs:
- protein_velocity: float32 [3, 524288], P(None, ('rep', 'dom')), parts along dimension 1
- water_velocity: float32 [9, 262144], P(None, ('rep', 'dom')), parts along dimension 1
The draws below stay inside these ranges and needn't reach their ends.
There are 32 independent parts, one for each index of `rep`. The reference program is written for one: setup_inputs(seed, part) draws one part's arguments, and reference() takes and returns one part's arrays. A program takes and returns all parts, laid end to end along the dimension named above; each array names one. Nothing has to cross between parts.
Inputs may be any that keep to these rules, and one draw needn't show every extreme that they name: `bond_atoms`: indices within the domain's block of 2048 atoms; each column joins two different atoms; together with the cross bonds the bonds form a forest. `left_atoms`: distinct indices within the domain's block, none of them in right_atoms. `right_atoms`: distinct indices within the domain's block. `protein_pos`: every bond and every cross bond joins atoms 0.1 to 0.15 apart. `water_pos`: each column holds one rigid water: oxygen, then two hydrogens, 0.09572 from the oxygen and 0.15139 from each other.
All inputs are finite; a program needn't handle non-finite values.
Results may differ from the reference program's by a relative error of at most 0.0003.
Values sent between devices are 32-bit elements; how exact they have to be, the bound alone decides.
No kernel may reach another device: no remote copies, remote signals or barrier semaphores. Data moves between devices by JAX's collectives and lax.ppermute only.
A program may use at most 64 MiB of HBM per device.

```python
import math
import jax
import jax.numpy as jnp
from jax import lax

PROT_DEV = 2048
HALO = 384
ORDER = 4
ITER = 2
BOND_DEV = 1280
PROTEIN = 16384
BONDS = 10240
CROSS = 3072
WATERS = 8192
N_DOM = 8


oxygen_hydrogen = 0.09572


hydrogen_pair = 0.15139


def topology(key):
    base = jax.random.fold_in(key, 7)
    perms = jax.vmap(lambda single: jax.random.permutation(single, PROT_DEV))(jax.random.split(base, N_DOM)).astype(jnp.int32)
    mains = BOND_DEV - HALO
    nodes = jnp.arange(mains + 1, dtype=jnp.int32)
    parents = jnp.broadcast_to(jnp.maximum(nodes - 1, 0) // 3, (N_DOM, mains + 1)).astype(jnp.int32)
    return (perms, parents)


def draw_bond_atoms(key, part):
    perms, parents = topology(key)
    mains = BOND_DEV - HALO
    nodes = jnp.arange(1, mains + 1, dtype=jnp.int32)
    child_main = perms[:, HALO + 1:HALO + 1 + mains]
    parent_main = jnp.take_along_axis(perms, parents[:, nodes] + HALO, axis=1)
    child_cap = perms[:, HALO + mains + 1:HALO + mains + 1 + HALO]
    parent_cap = perms[:, :HALO]
    child = jnp.concatenate([child_main, child_cap], axis=1)
    parent = jnp.concatenate([parent_main, parent_cap], axis=1)
    return jnp.stack([child, parent]).reshape(2, N_DOM * BOND_DEV).astype(jnp.int32)


def draw_left_atoms(key, part):
    perms, parents = topology(key)
    return perms[:, :HALO].reshape(N_DOM * HALO).astype(jnp.int32)


def draw_right_atoms(key, part):
    perms, parents = topology(key)
    mains = BOND_DEV - HALO
    return perms[:, mains + 1:mains + 1 + HALO].reshape(N_DOM * HALO).astype(jnp.int32)


def bond_lengths(key, shape):
    return jnp.exp(jax.random.uniform(key, shape, jnp.float32, math.log(0.1), math.log(0.15)))


def random_steps(key, shape):
    keys = jax.random.split(key, 3)
    cosine = jax.random.uniform(keys[0], shape, jnp.float32, -1.0, 1.0)
    angle = jax.random.uniform(keys[1], shape, jnp.float32, 0.0, 2.0 * math.pi)
    sine = jnp.sqrt(jnp.maximum(1.0 - cosine * cosine, 0.0))
    lengths = bond_lengths(keys[2], shape)
    return jnp.stack([sine * jnp.cos(angle), sine * jnp.sin(angle), cosine], axis=1) * lengths[:, None, :]


def tetra_steps(key, index, sign):
    keys = jax.random.split(key, 2)
    table = jnp.array([[1.0, 1.0, 1.0], [1.0, -1.0, -1.0], [-1.0, 1.0, -1.0], [-1.0, -1.0, 1.0]], jnp.float32) / math.sqrt(3.0)
    pick = (index[..., None] == jnp.arange(4, dtype=jnp.int32)).astype(jnp.float32)
    direction = jnp.einsum('dnk,kc->dcn', pick, table) * sign[:, None, :]
    jitter = jnp.clip(jax.random.normal(keys[0], direction.shape, jnp.float32), -2.0, 2.0)
    direction = direction + 0.15 * jitter
    direction = direction / jnp.sqrt(jnp.sum(direction * direction, axis=1, keepdims=True))
    return direction * bond_lengths(keys[1], index.shape)[:, None, :]


def draw_protein_pos(key, part):
    perms, parents = topology(key)
    keys = jax.random.split(jax.random.fold_in(key, 21), 9)
    mains = BOND_DEV - HALO
    nodes = jnp.arange(mains + 1, dtype=jnp.int32)
    turns = jax.random.randint(keys[5], (N_DOM, mains + 1), 0, 3, dtype=jnp.int32)
    first_dir = jax.random.randint(keys[6], (N_DOM, 1), 0, 4, dtype=jnp.int32)
    slot = jnp.maximum(nodes - 1, 0) % 3
    index = jnp.broadcast_to(first_dir, (N_DOM, mains + 1)).astype(jnp.int32)
    depth = jnp.zeros((N_DOM, mains + 1), jnp.int32)
    for rounds in range(16):
        up_index = jnp.take_along_axis(index, parents, axis=1)
        up_turn = jnp.take_along_axis(turns, parents, axis=1)
        up_depth = jnp.take_along_axis(depth, parents, axis=1)
        index = jnp.where(nodes == 0, first_dir, (up_index + 1 + (slot + up_turn) % 3) % 4).astype(jnp.int32)
        depth = jnp.where(nodes == 0, 0, up_depth + 1).astype(jnp.int32)
    sign = jnp.where(depth % 2 == 1, 1.0, -1.0).astype(jnp.float32)
    steps = tetra_steps(keys[0], index, sign)
    steps = steps.at[:, :, 0].set(0.0)
    root = jax.random.uniform(keys[1], (N_DOM, 3), jnp.float32, -1.0, 1.0)
    total = steps
    pointer = parents
    for rounds in range(6):
        total = total + jnp.take_along_axis(total, jnp.broadcast_to(pointer[:, None, :], total.shape), axis=2)
        pointer = jnp.take_along_axis(pointer, pointer, axis=1)
    main_pos = total + root[:, :, None]
    anchor_pos = main_pos[:, :, mains + 1 - HALO:mains + 1]
    anchor_index = jnp.roll(index[:, mains + 1 - HALO:mains + 1], 1, axis=0)
    anchor_depth = jnp.roll(depth[:, mains + 1 - HALO:mains + 1], 1, axis=0)
    anchor_sign = jnp.where(anchor_depth % 2 == 0, 1.0, -1.0).astype(jnp.float32)
    cap_index = (anchor_index + 1 + jax.random.randint(keys[7], (N_DOM, HALO), 0, 3, dtype=jnp.int32)) % 4
    child_index = (cap_index + 1 + jax.random.randint(keys[8], (N_DOM, HALO), 0, 3, dtype=jnp.int32)) % 4
    cap_pos = jnp.roll(anchor_pos, 1, axis=0) + tetra_steps(keys[2], cap_index, anchor_sign)
    child_pos = cap_pos + tetra_steps(keys[3], child_index, -anchor_sign)
    lone_pos = root[:, :, None] + random_steps(keys[4], (N_DOM, HALO - 1))

    def place(perm, main_part, cap_part, child_part, lone_part):
        field = jnp.zeros((3, PROT_DEV), jnp.float32)
        field = field.at[:, perm[HALO:HALO + mains + 1]].set(main_part)
        field = field.at[:, perm[:HALO]].set(cap_part)
        field = field.at[:, perm[HALO + mains + 1:HALO + mains + 1 + HALO]].set(child_part)
        return field.at[:, perm[PROT_DEV - HALO + 1:]].set(lone_part)
    placed = jax.vmap(place)(perms, main_pos, cap_pos, child_pos, lone_pos)
    return jnp.transpose(placed, (1, 0, 2)).reshape(3, N_DOM * PROT_DEV)


def draw_water_pos(key, part):
    keys = jax.random.split(jax.random.fold_in(key, 31), 4)
    oxygen = jax.random.uniform(keys[0], (3, WATERS), jnp.float32, -3.0, 3.0)
    first_angle = jax.random.uniform(keys[1], (WATERS,), jnp.float32, -math.pi, math.pi)
    second_angle = jax.random.uniform(keys[2], (WATERS,), jnp.float32, -math.pi, math.pi)
    third_angle = jax.random.uniform(keys[3], (WATERS,), jnp.float32, -math.pi, math.pi)
    cos_a, sin_a = (jnp.cos(first_angle), jnp.sin(first_angle))
    cos_b, sin_b = (jnp.cos(second_angle), jnp.sin(second_angle))
    cos_c, sin_c = (jnp.cos(third_angle), jnp.sin(third_angle))
    column_one = jnp.stack([cos_a * cos_c - sin_a * cos_b * sin_c, sin_a * cos_c + cos_a * cos_b * sin_c, sin_b * sin_c])
    column_two = jnp.stack([-cos_a * sin_c - sin_a * cos_b * cos_c, -sin_a * sin_c + cos_a * cos_b * cos_c, sin_b * cos_c])
    half = 0.5 * hydrogen_pair
    height = math.sqrt(oxygen_hydrogen * oxygen_hydrogen - half * half)
    first = oxygen + half * column_one - height * column_two
    second = oxygen - half * column_one - height * column_two
    return jnp.concatenate([oxygen, first, second], axis=0)


def block_levels(own_key, shape, shards, least, high):
    gain = 1.0
    for axis_at, shards_of in shards:
        draws = jax.random.uniform(jax.random.fold_in(jax.random.fold_in(own_key, 6), axis_at), (shards_of,), jnp.float32, least / len(shards), high / len(shards))
        gain = gain * jnp.repeat(jnp.exp(draws), shape[axis_at] // shards_of).reshape((-1,) + (1,) * (len(shape) - 1 - axis_at))
    return gain


def gaussian(key, dims, spread, bound, cuts=(), kind=jnp.bfloat16):
    level = block_levels(key, dims, cuts, -0.22, 0.18) if cuts else 1.0
    entries = jax.random.normal(key, dims, jnp.float32) * spread * level
    return jnp.minimum(jnp.maximum(entries, -bound), bound).astype(kind)


def setup_inputs(seed: int = 0, part: int = 0) -> dict:
    seeds = jax.random.split(jax.random.key(seed), 9)
    part_splits = jax.random.split(jax.random.fold_in(seeds[8], part), 9)
    return {
        "protein_pos": draw_protein_pos(jax.random.fold_in(jax.random.fold_in(seeds[8], part), 71), part),
        "protein_vel": gaussian(part_splits[1], (3, PROTEIN), 1.0, 3.0, ((1, 8),), jnp.float32),
        "inv_mass": jnp.clip(jnp.exp(math.log(1.0) - 2.7725887 * jax.random.uniform(part_splits[2], (PROTEIN,), jnp.float32) ** block_levels(part_splits[2], (PROTEIN,), ((0, 8),), -0.2, 0.2)), 0.0625, 1.0),
        "bond_atoms": draw_bond_atoms(jax.random.fold_in(jax.random.fold_in(seeds[8], part), 71), part),
        "left_atoms": draw_left_atoms(jax.random.fold_in(jax.random.fold_in(seeds[8], part), 71), part),
        "right_atoms": draw_right_atoms(jax.random.fold_in(jax.random.fold_in(seeds[8], part), 71), part),
        "water_pos": draw_water_pos(jax.random.fold_in(jax.random.fold_in(seeds[8], part), 71), part),
        "water_vel": gaussian(part_splits[7], (9, WATERS), 1.0, 3.0, ((1, 8),), jnp.float32),
    }


time_step = 0.002
mass_oxygen = 15.9994
mass_hydrogen = 1.008
oxygen_hydrogen = 0.09572
hydrogen_pair = 0.15139
total_mass = mass_oxygen + 2.0 * mass_hydrogen
half_pair = 0.5 * hydrogen_pair
water_height = math.sqrt(oxygen_hydrogen * oxygen_hydrogen - half_pair * half_pair)
oxygen_reach = 2.0 * mass_hydrogen * water_height / total_mass
hydrogen_reach = water_height - oxygen_reach

def cross_product(left, right):
    return jnp.stack([left[1] * right[2] - left[2] * right[1], left[2] * right[0] - left[0] * right[2], left[0] * right[1] - left[1] * right[0]])

def inner(left, right):
    return lax.optimization_barrier(jnp.sum(left * right, axis=0))

def settle(before, after):
    old_oxygen, old_first, old_second = (before[0:3], before[3:6], before[6:9])
    new_oxygen, new_first, new_second = (after[0:3], after[3:6], after[6:9])
    center = (mass_oxygen * new_oxygen + mass_hydrogen * (new_first + new_second)) / total_mass
    old_b = old_first - old_oxygen
    old_c = old_second - old_oxygen
    rel_a = new_oxygen - center
    rel_b = new_first - center
    rel_c = new_second - center
    normal = cross_product(old_b, old_c)
    side = cross_product(rel_a, normal)
    upward = cross_product(normal, side)
    axis_z = normal / jnp.sqrt(inner(normal, normal))
    axis_x = side / jnp.sqrt(inner(side, side))
    axis_y = upward / jnp.sqrt(inner(upward, upward))
    oldb_x = inner(axis_x, old_b)
    oldb_y = inner(axis_y, old_b)
    oldc_x = inner(axis_x, old_c)
    oldc_y = inner(axis_y, old_c)
    newa_z = inner(axis_z, rel_a)
    newb_x = inner(axis_x, rel_b)
    newb_y = inner(axis_y, rel_b)
    newb_z = inner(axis_z, rel_b)
    newc_x = inner(axis_x, rel_c)
    newc_y = inner(axis_y, rel_c)
    newc_z = inner(axis_z, rel_c)
    sin_phi = newa_z / oxygen_reach
    cos_phi = jnp.sqrt(1.0 - sin_phi * sin_phi)
    sin_psi = (newb_z - newc_z) / (2.0 * half_pair * cos_phi)
    cos_psi = jnp.sqrt(1.0 - sin_psi * sin_psi)
    rest_ay = oxygen_reach * cos_phi
    rest_bx = -half_pair * cos_psi
    lowered = -hydrogen_reach * cos_phi
    tilted = half_pair * sin_psi * sin_phi
    rest_by = lowered - tilted
    rest_cy = lowered + tilted
    alpha = rest_bx * (oldb_x - oldc_x) + oldb_y * rest_by + oldc_y * rest_cy
    beta = rest_bx * (oldc_y - oldb_y) + oldb_x * rest_by + oldc_x * rest_cy
    gamma = oldb_x * newb_y - newb_x * oldb_y + oldc_x * newc_y - newc_x * oldc_y
    summed = alpha * alpha + beta * beta
    sin_theta = (alpha * gamma - beta * jnp.sqrt(summed - gamma * gamma)) / summed
    cos_theta = jnp.sqrt(1.0 - sin_theta * sin_theta)
    final_ax = -rest_ay * sin_theta
    final_ay = rest_ay * cos_theta
    final_bx = rest_bx * cos_theta - rest_by * sin_theta
    final_by = rest_bx * sin_theta + rest_by * cos_theta
    final_cx = -rest_bx * cos_theta - rest_cy * sin_theta
    final_cy = -rest_bx * sin_theta + rest_cy * cos_theta
    oxygen = center + axis_x * final_ax + axis_y * final_ay + axis_z * newa_z
    first = center + axis_x * final_bx + axis_y * final_by + axis_z * newb_z
    second = center + axis_x * final_cx + axis_y * final_cy + axis_z * newc_z
    return jnp.concatenate([oxygen, first, second], axis=0)

def reference(protein_pos, protein_vel, inv_mass, bond_atoms, left_atoms, right_atoms, water_pos, water_vel):
    bond_domain = jnp.arange(BONDS, dtype=jnp.int32) // BOND_DEV
    slot_domain = jnp.arange(CROSS, dtype=jnp.int32) // HALO
    next_domain = (slot_domain + 1) % N_DOM
    anchors = right_atoms + slot_domain * PROT_DEV
    capped = jnp.roll(left_atoms, -HALO) + next_domain * PROT_DEV
    first = jnp.concatenate([bond_atoms[0] + bond_domain * PROT_DEV, anchors]).astype(jnp.int32)
    second = jnp.concatenate([bond_atoms[1] + bond_domain * PROT_DEV, capped]).astype(jnp.int32)
    moved = protein_pos + time_step * protein_vel
    diff = protein_pos[:, first] - protein_pos[:, second]
    length = jnp.sqrt(inner(diff, diff))
    unit = diff / length
    scale = 1.0 / jnp.sqrt(inv_mass[first] + inv_mass[second])

    def atom_field(values):
        weighted = unit * (scale * values)
        force = jnp.zeros((3, PROTEIN), jnp.float32).at[:, first].add(weighted).at[:, second].add(-weighted)
        return inv_mass * force

    def expand(rhs):
        total = rhs
        current = rhs
        for order_index in range(ORDER):
            field = atom_field(current)
            current = current - scale * inner(unit, field[:, first] - field[:, second])
            total = total + current
        return total
    rhs = scale * (inner(unit, moved[:, first] - moved[:, second]) - length)
    delta = -atom_field(expand(rhs))
    for round_index in range(ITER):
        now = moved + delta
        gap = now[:, first] - now[:, second]
        target = jnp.sqrt(2.0 * length * length - inner(gap, gap))
        rhs = scale * (length - target)
        delta = delta - atom_field(expand(rhs))
    protein_velocity = protein_vel + delta / time_step
    water_moved = water_pos + time_step * water_vel
    settled = settle(water_pos, water_moved)
    water_velocity = water_vel + (settled - water_moved) / time_step
    return (protein_velocity, water_velocity)
```

```python
import functools
import math

import jax
import jax.numpy as jnp
from jax import lax
from jax.experimental import pallas as pl
from jax.experimental.pallas import tpu as pltpu
from jax.sharding import PartitionSpec as P

ORDER = 4
ITER = 2

time_step = 0.002
mass_oxygen = 15.9994
mass_hydrogen = 1.008
oxygen_hydrogen = 0.09572
hydrogen_pair = 0.15139
total_mass = mass_oxygen + 2.0 * mass_hydrogen
half_pair = 0.5 * hydrogen_pair
water_height = math.sqrt(oxygen_hydrogen * oxygen_hydrogen - half_pair * half_pair)
oxygen_reach = 2.0 * mass_hydrogen * water_height / total_mass
hydrogen_reach = water_height - oxygen_reach

LANES = 128
DOMAINS = 8
ATOM_ROWS = 16
BOND_ROWS = 10
SLOT_ROWS = 3
RIGHT = BOND_ROWS
LEFT = BOND_ROWS + SLOT_ROWS
CON_ROWS = BOND_ROWS + 2 * SLOT_ROWS
END_ROWS = CON_ROWS + BOND_ROWS
PLUS = LEFT * LANES

DIFF, VELO, SCAL = 0, 3 * CON_ROWS, 6 * CON_ROWS
ENDS = 7 * CON_ROWS
ATOM = ENDS + END_ROWS
POSN = ATOM + END_ROWS
MASS = POSN + END_ROWS
ROWS = MASS + END_ROWS


def lanes_of(table, index):
    dims = lax.GatherDimensionNumbers(
        offset_dims=(),
        collapsed_slice_dims=(1,),
        start_index_map=(1,),
        operand_batching_dims=(0,),
        start_indices_batching_dims=(0,),
    )
    return lax.gather(
        table, index[..., None], dims, (1, 1), mode=lax.GatherScatterMode.PROMISE_IN_BOUNDS
    )


def bits_of(row, count):
    return [(row & (1 << b)) != 0 for b in range(max(1, (count - 1).bit_length()))]


def pick(get, count, masks, low=0):
    if count == 1:
        return get(low)
    bit = (count - 1).bit_length() - 1
    half = 1 << bit
    left = pick(get, half, masks, low)
    right = pick(get, count - half, masks, low + half)
    return jnp.where(masks[bit], right, left)


def gather_rows(table, count, row, lane):
    masks = bits_of(row, count)
    return pick(lambda r: lanes_of(table(r), lane), count, masks)


def spread(ref, r):
    return jnp.broadcast_to(ref[r : r + 1, :], (8, LANES))


def place_of(position):
    lane = (position * 2521) >> 16
    return position - lane * END_ROWS, lane


def cross3(a, b):
    return [a[1] * b[2] - a[2] * b[1], a[2] * b[0] - a[0] * b[2], a[0] * b[1] - a[1] * b[0]]


def dot3(a, b):
    return a[0] * b[0] + a[1] * b[1] + a[2] * b[2]


def settle(before, after):
    old_o, old_1, old_2 = before[0:3], before[3:6], before[6:9]
    new_o, new_1, new_2 = after[0:3], after[3:6], after[6:9]
    every = range(3)
    center = [(mass_oxygen * new_o[c] + mass_hydrogen * (new_1[c] + new_2[c])) / total_mass for c in every]
    old_b = [old_1[c] - old_o[c] for c in every]
    old_c = [old_2[c] - old_o[c] for c in every]
    rel_a = [new_o[c] - center[c] for c in every]
    rel_b = [new_1[c] - center[c] for c in every]
    rel_c = [new_2[c] - center[c] for c in every]
    normal = cross3(old_b, old_c)
    side = cross3(rel_a, normal)
    upward = cross3(normal, side)

    def normed(v):
        size = jnp.sqrt(dot3(v, v))
        return [part / size for part in v]

    axis_z, axis_x, axis_y = normed(normal), normed(side), normed(upward)
    oldb_x, oldb_y = dot3(axis_x, old_b), dot3(axis_y, old_b)
    oldc_x, oldc_y = dot3(axis_x, old_c), dot3(axis_y, old_c)
    newa_z = dot3(axis_z, rel_a)
    newb_x, newb_y, newb_z = dot3(axis_x, rel_b), dot3(axis_y, rel_b), dot3(axis_z, rel_b)
    newc_x, newc_y, newc_z = dot3(axis_x, rel_c), dot3(axis_y, rel_c), dot3(axis_z, rel_c)
    sin_phi = newa_z / oxygen_reach
    cos_phi = jnp.sqrt(1.0 - sin_phi * sin_phi)
    sin_psi = (newb_z - newc_z) / (2.0 * half_pair * cos_phi)
    cos_psi = jnp.sqrt(1.0 - sin_psi * sin_psi)
    rest_ay = oxygen_reach * cos_phi
    rest_bx = -half_pair * cos_psi
    lowered = -hydrogen_reach * cos_phi
    tilted = half_pair * sin_psi * sin_phi
    rest_by = lowered - tilted
    rest_cy = lowered + tilted
    alpha = rest_bx * (oldb_x - oldc_x) + oldb_y * rest_by + oldc_y * rest_cy
    beta = rest_bx * (oldc_y - oldb_y) + oldb_x * rest_by + oldc_x * rest_cy
    gamma = oldb_x * newb_y - newb_x * oldb_y + oldc_x * newc_y - newc_x * oldc_y
    summed = alpha * alpha + beta * beta
    sin_theta = (alpha * gamma - beta * jnp.sqrt(summed - gamma * gamma)) / summed
    cos_theta = jnp.sqrt(1.0 - sin_theta * sin_theta)
    final_ax = -rest_ay * sin_theta
    final_ay = rest_ay * cos_theta
    final_bx = rest_bx * cos_theta - rest_by * sin_theta
    final_by = rest_bx * sin_theta + rest_by * cos_theta
    final_cx = -rest_bx * cos_theta - rest_cy * sin_theta
    final_cy = -rest_bx * sin_theta + rest_cy * cos_theta
    oxygen = [center[c] + axis_x[c] * final_ax + axis_y[c] * final_ay + axis_z[c] * newa_z for c in every]
    first = [center[c] + axis_x[c] * final_bx + axis_y[c] * final_by + axis_z[c] * newb_z for c in every]
    second = [center[c] + axis_x[c] * final_cx + axis_y[c] * final_cy + axis_z[c] * newc_z for c in every]
    return oxygen + first + second


def sort_keys(keys):
    lane = lax.broadcasted_iota(jnp.int32, (8, LANES), 1)
    sub = lax.broadcasted_iota(jnp.int32, (8, LANES), 0)
    base = lane * 32 + sub * 4

    def clear(bit, reg):
        if bit == 12:
            return None
        return (((base + reg) >> bit) & 1) == 0

    for size in range(1, 13):
        for bit in range(size - 1, -1, -1):
            if bit < 2:
                out = list(keys)
                for reg in range(4):
                    if reg & (1 << bit):
                        continue
                    other = reg | (1 << bit)
                    low = jnp.minimum(keys[reg], keys[other])
                    high = jnp.maximum(keys[reg], keys[other])
                    if size == 12:
                        out[reg], out[other] = low, high
                    elif size < 2:
                        up = not reg & (1 << size)
                        out[reg], out[other] = (low, high) if up else (high, low)
                    else:
                        up = clear(size, 0)
                        out[reg] = jnp.where(up, low, high)
                        out[other] = jnp.where(up, high, low)
                keys = out
                continue
            if size == 12:
                keep = ((base >> bit) & 1) == 0
            else:
                keep = (((base >> bit) ^ (base >> size)) & 1) == 0
            out = []
            for key in keys:
                if bit < 5:
                    step = 1 << (bit - 2)
                    if step == 4:
                        mate = pltpu.roll(key, 4, 0)
                    else:
                        upper = (sub & step) != 0
                        mate = jnp.where(upper, pltpu.roll(key, step, 0), pltpu.roll(key, 8 - step, 0))
                else:
                    mate = lanes_of(key, lane ^ (1 << (bit - 5)))
                out.append(jnp.where(keep, jnp.minimum(key, mate), jnp.maximum(key, mate)))
            keys = out
    return keys


def prepare(
    pos, vel, mass, bonds, left, right, water_pos, water_vel, pay, begin, water_out, atoms, ranked, ordered, wet
):
    lane = lax.broadcasted_iota(jnp.int32, (8, LANES), 1)
    sub = lax.broadcasted_iota(jnp.int32, (8, LANES), 0)

    for r in range(BOND_ROWS):
        cut = slice(r * LANES, (r + 1) * LANES)
        atoms[r : r + 1, :] = bonds[0:1, cut]
        atoms[CON_ROWS + r : CON_ROWS + r + 1, :] = bonds[1:2, cut]
    atoms[RIGHT:LEFT, :] = right[...]
    atoms[LEFT:CON_ROWS, :] = left[...]
    atoms[END_ROWS:32, :] = jnp.full((32 - END_ROWS, LANES), 2048, jnp.int32)
    ends = [atoms[8 * k : 8 * k + 8, :] for k in range(4)]
    keys = [(ends[k] * 4096 + (k * 8 + sub) * LANES + lane).astype(jnp.float32) for k in range(4)]

    done = sort_keys(keys)
    for k in range(4):
        ranked[8 * k : 8 * k + 8, :] = done[k]

    for k in range(4):
        rank = lane * END_ROWS + k * 8 + sub
        got = gather_rows(
            functools.partial(spread, ranked), 32, (rank & 3) * 8 + ((rank >> 2) & 7), rank >> 5
        ).astype(jnp.int32)
        ordered[8 * k : 8 * k + 8, :] = got
    for k in range(4):
        count = min(8, END_ROWS - 8 * k)
        got = ordered[8 * k : 8 * k + 8, :]
        end = (got & 4095).astype(jnp.float32)
        atom = jnp.minimum(got >> 12, 2047)
        weight = gather_rows(functools.partial(spread, mass), ATOM_ROWS, atom >> 7, atom & 127)
        pay[ENDS + 8 * k : ENDS + 8 * k + count, :] = end[:count]
        pay[ATOM + 8 * k : ATOM + 8 * k + count, :] = atom[:count].astype(jnp.float32)
        pay[MASS + 8 * k : MASS + 8 * k + count, :] = weight[:count]

    heads = ranked[0:1, :]
    marks = [jnp.broadcast_to(heads[:, 8 * i : 8 * i + 1], (8, LANES)) for i in range(1, 16)]
    queries = keys + [(((k * 8 + sub) * LANES + lane) * 4096).astype(jnp.float32) for k in range(2)]
    wide = jnp.broadcast_to(heads, (8, LANES))
    ranks = []
    for query in queries:
        group = jnp.zeros((8, LANES), jnp.int32)
        for mark in marks:
            group = group + jnp.where(mark <= query, 8, 0)
        column = group
        for i in range(1, 8):
            column = column + jnp.where(lanes_of(wide, group + i) <= query, 1, 0)
        rank = column * 32
        for r in range(32):
            rank = rank + jnp.where(lanes_of(spread(ranked, r), column) < query, 1, 0)
        ranks.append(rank)
    for k in range(4):
        count = min(8, END_ROWS - 8 * k)
        pay[POSN + 8 * k : POSN + 8 * k + count, :] = ranks[k][:count].astype(jnp.float32)
    for k in range(2):
        begin[8 * k : 8 * k + 8, :] = jnp.minimum(ranks[4 + k], END_ROWS * LANES - 1)

    where = [(jnp.minimum(e, 2047) >> 7, e & 127) for e in ends]

    def at_ends(table):
        return [gather_rows(table, ATOM_ROWS, row, col) for row, col in where]

    two = sub < BOND_ROWS - 8
    for base, source in ((DIFF, pos), (VELO, vel)):
        for c in range(3):
            a0, a1, b0, b1 = at_ends(
                lambda r: jnp.broadcast_to(source[c : c + 1, r * LANES : (r + 1) * LANES], (8, LANES))
            )
            pay[base + CON_ROWS * c : base + CON_ROWS * c + 8, :] = a0 - b0
            pay[base + CON_ROWS * c + 8 : base + CON_ROWS * c + 16, :] = jnp.where(two, a1 - b1, a1)
    a0, a1, b0, b1 = at_ends(functools.partial(spread, mass))
    pay[SCAL : SCAL + 8, :] = 1.0 / jnp.sqrt(a0 + b0)
    pay[SCAL + 8 : SCAL + 16, :] = jnp.where(two, 1.0 / jnp.sqrt(a1 + b1), a1)

    for j in range(8):
        cut = slice(j * LANES, (j + 1) * LANES)
        for c in range(9):
            wet[c, j : j + 1, :] = water_pos[c : c + 1, cut]
            wet[9 + c, j : j + 1, :] = water_vel[c : c + 1, cut]
    before = [wet[c] for c in range(9)]
    speed = [wet[9 + c] for c in range(9)]
    after = [before[c] + time_step * speed[c] for c in range(9)]
    settled = settle(before, after)
    for c in range(9):
        result = speed[c] + (settled[c] - after[c]) / time_step
        for j in range(8):
            water_out[c : c + 1, j * LANES : (j + 1) * LANES] = result[j : j + 1, :]


def solve(
    whole, begin, vel, out,
    con_row, con_col, end_row, end_col, atom, mass, first, second, push, unit, length, scale, diff, drift,
    now, total, field, ahead, behind, moved, more,
):
    def load(r):
        return whole[pl.ds(r, DOMAINS, stride=ROWS), :]

    def up(x):
        return pltpu.roll(x, DOMAINS - 1, 0)

    def down(x):
        return pltpu.roll(x, 1, 0)

    def before(get, v, step):
        return get(v - step) if v >= step else pltpu.roll(get(v - step + END_ROWS), 1, 1)

    def after(get, v, step):
        return get(v + step) if v + step < END_ROWS else pltpu.roll(get(v + step - END_ROWS), LANES - 1, 1)

    slots = [(RIGHT + k, LEFT + k) for k in range(SLOT_ROWS)]

    many = jnp.zeros((8, LANES), jnp.int32)
    for v in range(END_ROWS):
        end = load(ENDS + v).astype(jnp.int32)
        con = end & 2047
        con_row[v] = con >> 7
        con_col[v] = con & 127
        push[0, v] = jnp.where(end < PLUS, 1.0, -1.0)
        row, col = place_of(load(POSN + v).astype(jnp.int32))
        end_row[v] = row
        end_col[v] = col
        mass[v] = load(MASS + v)
        atom[v] = load(ATOM + v)
    for v in range(END_ROWS):
        here = atom[v]
        first[v] = jnp.where(here == before(lambda r: atom[r], v, 1), 1.0, 0.0)
        second[v] = jnp.where(here == before(lambda r: atom[r], v, 2), 1.0, 0.0)
        many = jnp.where(here == before(lambda r: atom[r], v, 4), 1, many)
    steps = jnp.where(jnp.max(many) > 0, 12, 2)

    for r in range(CON_ROWS):
        if r >= LEFT:
            continue
        d = [load(DIFF + CON_ROWS * c + r) for c in range(3)]
        g = [load(VELO + CON_ROWS * c + r) for c in range(3)]
        s = load(SCAL + r)
        if r >= RIGHT:
            other = r + SLOT_ROWS
            d = [d[c] - up(load(DIFF + CON_ROWS * c + other)) for c in range(3)]
            g = [g[c] - up(load(VELO + CON_ROWS * c + other)) for c in range(3)]
            s = 1.0 / jnp.sqrt(s + up(load(SCAL + other)))
        size = jnp.sqrt(dot3(d, d))
        part = s / size
        g = [time_step * x for x in g]
        rhs = part * dot3(d, g)
        length[r] = size
        scale[r] = s
        now[r] = rhs
        total[r] = rhs
        for c in range(3):
            diff[c, r] = d[c]
            drift[c, r] = g[c]
            unit[c, r] = part * d[c]
        if r >= RIGHT:
            now[other] = down(rhs)
            total[other] = down(rhs)
            for c in range(3):
                unit[c, other] = down(part * d[c])

    for v in range(END_ROWS):
        col = con_col[v]
        masks = bits_of(con_row[v], CON_ROWS)
        sign = push[0, v]
        parts = [pick(lambda r: lanes_of(unit[c, r], col), CON_ROWS, masks) for c in range(3)]
        for c in range(3):
            push[c, v] = sign * parts[c]
            moved[c, v] = jnp.zeros((8, LANES), jnp.float32)

    def same(ref, v):
        return ref[v] > 0.5

    def sums(source):
        for v in range(END_ROWS):
            masks = bits_of(con_row[v], CON_ROWS)
            col = con_col[v]
            x = pick(lambda r: lanes_of(source[r], col), CON_ROWS, masks)
            for c in range(3):
                field[c, v] = push[c, v] * x
        zero = jnp.zeros((8, LANES), jnp.float32)
        for c in range(3):
            one = [
                field[c, v] + jnp.where(same(first, v), before(lambda r: field[c, r], v, 1), zero)
                for v in range(END_ROWS)
            ]
            for v in range(END_ROWS):
                ahead[c, v] = one[v] + jnp.where(same(second, v), before(lambda r: one[r], v, 2), zero)
            one = [
                field[c, v]
                + jnp.where(after(lambda r: first[r], v, 1) > 0.5, after(lambda r: field[c, r], v, 1), zero)
                for v in range(END_ROWS)
            ]
            for v in range(END_ROWS):
                behind[c, v] = one[v] + jnp.where(
                    after(lambda r: second[r], v, 2) > 0.5, after(lambda r: one[r], v, 2), zero
                )

        def longer(k, carry):
            step = lax.shift_left(1, k)
            turns = step // END_ROWS
            rest = step - turns * END_ROWS

            def row(v, carry):
                here = atom[v]
                low = v - rest
                wrap = jnp.where(low < 0, 1, 0)
                low = low + wrap * END_ROWS
                shift = turns + wrap
                match = here == pltpu.roll(atom[low], shift, 1)
                high = v + rest
                wrap = jnp.where(high >= END_ROWS, 1, 0)
                high = high - wrap * END_ROWS
                back = LANES - turns - wrap
                match_back = here == pltpu.roll(atom[high], back, 1)
                for c in range(3):
                    more[c, v] = ahead[c, v] + jnp.where(match, pltpu.roll(ahead[c, low], shift, 1), 0.0)
                    more[3 + c, v] = behind[c, v] + jnp.where(
                        match_back, pltpu.roll(behind[c, high], back, 1), 0.0
                    )
                return carry

            lax.fori_loop(0, END_ROWS, row, 0)

            def keep(v, carry):
                for c in range(3):
                    ahead[c, v] = more[c, v]
                    behind[c, v] = more[3 + c, v]
                return carry

            return lax.fori_loop(0, END_ROWS, keep, carry)

        lax.fori_loop(2, steps, longer, 0)

    def apply(order, carry):
        sums(now)
        zero = jnp.zeros((8, LANES), jnp.float32)
        for v in range(END_ROWS):
            low = same(first, v)
            high = after(lambda r: first[r], v, 1) > 0.5
            rest = [
                jnp.where(low, before(lambda r: ahead[c, r], v, 1), zero)
                + jnp.where(high, after(lambda r: behind[c, r], v, 1), zero)
                for c in range(3)
            ]
            field[0, v] = mass[v] * dot3([push[c, v] for c in range(3)], rest)

        def end(v):
            masks = bits_of(end_row[v], END_ROWS)
            col = end_col[v]
            return pick(lambda r: lanes_of(field[0, r], col), END_ROWS, masks)

        for r in range(LEFT):
            if r < BOND_ROWS:
                fresh = -(end(r) + end(CON_ROWS + r))
            else:
                fresh = -(end(r) + up(end(r + SLOT_ROWS)))
                now[r + SLOT_ROWS] = down(fresh)
                total[r + SLOT_ROWS] = total[r + SLOT_ROWS] + down(fresh)
            now[r] = fresh
            total[r] = total[r] + fresh
        return carry

    def turn(index, carry):
        lax.fori_loop(0, ORDER, apply, 0)
        sums(total)
        for v in range(END_ROWS):
            for c in range(3):
                moved[c, v] = moved[c, v] + mass[v] * (ahead[c, v] + behind[c, v] - field[c, v])

        @pl.when(index < ITER)
        def _():
            def end(v):
                masks = bits_of(end_row[v], END_ROWS)
                col = end_col[v]
                return [pick(lambda r: lanes_of(moved[c, r], col), END_ROWS, masks) for c in range(3)]

            for r in range(LEFT):
                here = end(r)
                if r < BOND_ROWS:
                    there = end(CON_ROWS + r)
                else:
                    there = [up(x) for x in end(r + SLOT_ROWS)]
                g = [drift[c, r] - (here[c] - there[c]) for c in range(3)]
                excess = 2.0 * dot3([diff[c, r] for c in range(3)], g) + dot3(g, g)
                size = length[r]
                rhs = scale[r] * excess / (size + jnp.sqrt(size * size - excess))
                now[r] = rhs
                total[r] = rhs
                if r >= RIGHT:
                    now[r + SLOT_ROWS] = down(rhs)
                    total[r + SLOT_ROWS] = down(rhs)

        return carry

    lax.fori_loop(0, ITER + 1, turn, 0)

    me = lax.axis_index("dom")
    own = [
        [jnp.broadcast_to(moved[c, v, pl.ds(me, 1), :], (8, LANES)) for v in range(END_ROWS)] for c in range(3)
    ]
    names = [jnp.broadcast_to(atom[v, pl.ds(me, 1), :], (8, LANES)) for v in range(END_ROWS)]
    lane = lax.broadcasted_iota(jnp.int32, (8, LANES), 1)
    sub = lax.broadcasted_iota(jnp.int32, (8, LANES), 0)
    for k in range(2):
        row, col = place_of(begin[8 * k : 8 * k + 8, :])
        masks = bits_of(row, END_ROWS)
        name = pick(lambda r: lanes_of(names[r], col), END_ROWS, masks).astype(jnp.int32)
        bound = name == (k * 8 + sub) * LANES + lane
        for c in range(3):
            shift = pick(lambda r: lanes_of(own[c][r], col), END_ROWS, masks)
            shift = jnp.where(bound, shift, 0.0) / time_step
            for j in range(8):
                cut = slice((8 * k + j) * LANES, (8 * k + j + 1) * LANES)
                out[c : c + 1, cut] = vel[c : c + 1, cut] - shift[j : j + 1, :]


def on_device(
    protein_pos, protein_vel, inv_mass, bond_atoms, left_atoms, right_atoms, water_pos, water_vel
):
    f32, i32 = jnp.float32, jnp.int32
    mass = inv_mass.reshape(ATOM_ROWS, LANES)
    pay, begin, water_velocity = pl.pallas_call(
        prepare,
        out_shape=(
            jax.ShapeDtypeStruct((ROWS, LANES), f32),
            jax.ShapeDtypeStruct((ATOM_ROWS, LANES), i32),
            jax.ShapeDtypeStruct(water_pos.shape, f32),
        ),
        scratch_shapes=[
            pltpu.VMEM((32, LANES), i32),
            pltpu.VMEM((32, LANES), f32),
            pltpu.VMEM((32, LANES), i32),
            pltpu.VMEM((18, 8, LANES), f32),
        ],
        name="prepare",
    )(
        protein_pos,
        protein_vel,
        mass,
        bond_atoms,
        left_atoms.reshape(SLOT_ROWS, LANES),
        right_atoms.reshape(SLOT_ROWS, LANES),
        water_pos,
        water_vel,
    )
    whole = lax.all_gather(pay, "dom", axis=0, tiled=True)

    def block(*lead, dtype=f32):
        return pltpu.VMEM((*lead, 8, LANES), dtype)

    protein_velocity = pl.pallas_call(
        solve,
        out_shape=jax.ShapeDtypeStruct(protein_vel.shape, f32),
        scratch_shapes=[
            block(END_ROWS, dtype=i32),
            block(END_ROWS, dtype=i32),
            block(END_ROWS, dtype=i32),
            block(END_ROWS, dtype=i32),
            block(END_ROWS),
            block(END_ROWS),
            block(END_ROWS),
            block(END_ROWS),
            block(3, END_ROWS),
            block(3, CON_ROWS),
            block(CON_ROWS),
            block(CON_ROWS),
            block(3, CON_ROWS),
            block(3, CON_ROWS),
            block(CON_ROWS),
            block(CON_ROWS),
            block(3, END_ROWS),
            block(3, END_ROWS),
            block(3, END_ROWS),
            block(3, END_ROWS),
            block(6, END_ROWS),
        ],
        name="solve",
    )(whole, begin, protein_vel)
    return (protein_velocity, water_velocity)


def solution(mesh):
    in_specs = (
        P(None, ("rep", "dom")),
        P(None, ("rep", "dom")),
        P(("rep", "dom")),
        P(None, ("rep", "dom")),
        P(("rep", "dom")),
        P(("rep", "dom")),
        P(None, ("rep", "dom")),
        P(None, ("rep", "dom")),
    )
    out_specs = (P(None, ("rep", "dom")), P(None, ("rep", "dom")))
    return jax.shard_map(
        on_device, mesh=mesh, in_specs=in_specs, out_specs=out_specs, check_vma=False
    )
```

```python
import functools
import math

import jax
import jax.numpy as jnp
from jax import lax
from jax.experimental import pallas as pl
from jax.experimental.pallas import tpu as pltpu
from jax.sharding import PartitionSpec as P

ORDER = 4
ITER = 2

time_step = 0.002
mass_oxygen = 15.9994
mass_hydrogen = 1.008
oxygen_hydrogen = 0.09572
hydrogen_pair = 0.15139
total_mass = mass_oxygen + 2.0 * mass_hydrogen
half_pair = 0.5 * hydrogen_pair
water_height = math.sqrt(oxygen_hydrogen * oxygen_hydrogen - half_pair * half_pair)
oxygen_reach = 2.0 * mass_hydrogen * water_height / total_mass
hydrogen_reach = water_height - oxygen_reach

LANES = 128
DOMAINS = 8
ATOM_ROWS = 16
BOND_ROWS = 10
SLOT_ROWS = 3
END_ROWS = 2 * BOND_ROWS
CROSS_ROWS = 2 * SLOT_ROWS
HALF = BOND_ROWS * LANES
NEAR = 3
NONE = 4095

DIFF, VELO, SCAL = 0, 3 * END_ROWS, 6 * END_ROWS
MASS, ATOM, MATE, LINK = (k * END_ROWS for k in (7, 8, 9, 10))
CPOS = 11 * END_ROWS
CVEL, CMAS, HOST = CPOS + 3 * CROSS_ROWS, CPOS + 6 * CROSS_ROWS, CPOS + 7 * CROSS_ROWS
ROWS = -(-(CPOS + 8 * CROSS_ROWS) // 8) * 8


def lanes_of(table, index):
    dims = lax.GatherDimensionNumbers(
        offset_dims=(),
        collapsed_slice_dims=(1,),
        start_index_map=(1,),
        operand_batching_dims=(0,),
        start_indices_batching_dims=(0,),
    )
    return lax.gather(
        table, index[..., None], dims, (1, 1), mode=lax.GatherScatterMode.PROMISE_IN_BOUNDS
    )


def bits_of(row, count):
    return [(row & (1 << b)) != 0 for b in range(max(1, (count - 1).bit_length()))]


def pick(get, count, masks, low=0):
    if count == 1:
        return get(low)
    bit = (count - 1).bit_length() - 1
    half = 1 << bit
    left = pick(get, half, masks, low)
    right = pick(get, count - half, masks, low + half)
    return jnp.where(masks[bit], right, left)


def gather_rows(table, count, row, lane):
    masks = bits_of(row, count)
    return pick(lambda r: lanes_of(table(r), lane), count, masks)


def spread(ref, r):
    return jnp.broadcast_to(ref[r : r + 1, :], (8, LANES))


def place_of(position):
    lane = (position * 3277) >> 16
    return position - lane * END_ROWS, lane


def cross3(a, b):
    return [a[1] * b[2] - a[2] * b[1], a[2] * b[0] - a[0] * b[2], a[0] * b[1] - a[1] * b[0]]


def dot3(a, b):
    return a[0] * b[0] + a[1] * b[1] + a[2] * b[2]


def settle(before, after):
    old_o, old_1, old_2 = before[0:3], before[3:6], before[6:9]
    new_o, new_1, new_2 = after[0:3], after[3:6], after[6:9]
    every = range(3)
    center = [(mass_oxygen * new_o[c] + mass_hydrogen * (new_1[c] + new_2[c])) / total_mass for c in every]
    old_b = [old_1[c] - old_o[c] for c in every]
    old_c = [old_2[c] - old_o[c] for c in every]
    rel_a = [new_o[c] - center[c] for c in every]
    rel_b = [new_1[c] - center[c] for c in every]
    rel_c = [new_2[c] - center[c] for c in every]
    normal = cross3(old_b, old_c)
    side = cross3(rel_a, normal)
    upward = cross3(normal, side)

    def normed(v):
        size = jnp.sqrt(dot3(v, v))
        return [part / size for part in v]

    axis_z, axis_x, axis_y = normed(normal), normed(side), normed(upward)
    oldb_x, oldb_y = dot3(axis_x, old_b), dot3(axis_y, old_b)
    oldc_x, oldc_y = dot3(axis_x, old_c), dot3(axis_y, old_c)
    newa_z = dot3(axis_z, rel_a)
    newb_x, newb_y, newb_z = dot3(axis_x, rel_b), dot3(axis_y, rel_b), dot3(axis_z, rel_b)
    newc_x, newc_y, newc_z = dot3(axis_x, rel_c), dot3(axis_y, rel_c), dot3(axis_z, rel_c)
    sin_phi = newa_z / oxygen_reach
    cos_phi = jnp.sqrt(1.0 - sin_phi * sin_phi)
    sin_psi = (newb_z - newc_z) / (2.0 * half_pair * cos_phi)
    cos_psi = jnp.sqrt(1.0 - sin_psi * sin_psi)
    rest_ay = oxygen_reach * cos_phi
    rest_bx = -half_pair * cos_psi
    lowered = -hydrogen_reach * cos_phi
    tilted = half_pair * sin_psi * sin_phi
    rest_by = lowered - tilted
    rest_cy = lowered + tilted
    alpha = rest_bx * (oldb_x - oldc_x) + oldb_y * rest_by + oldc_y * rest_cy
    beta = rest_bx * (oldc_y - oldb_y) + oldb_x * rest_by + oldc_x * rest_cy
    gamma = oldb_x * newb_y - newb_x * oldb_y + oldc_x * newc_y - newc_x * oldc_y
    summed = alpha * alpha + beta * beta
    sin_theta = (alpha * gamma - beta * jnp.sqrt(summed - gamma * gamma)) / summed
    cos_theta = jnp.sqrt(1.0 - sin_theta * sin_theta)
    final_ax = -rest_ay * sin_theta
    final_ay = rest_ay * cos_theta
    final_bx = rest_bx * cos_theta - rest_by * sin_theta
    final_by = rest_bx * sin_theta + rest_by * cos_theta
    final_cx = -rest_bx * cos_theta - rest_cy * sin_theta
    final_cy = -rest_bx * sin_theta + rest_cy * cos_theta
    oxygen = [center[c] + axis_x[c] * final_ax + axis_y[c] * final_ay + axis_z[c] * newa_z for c in every]
    first = [center[c] + axis_x[c] * final_bx + axis_y[c] * final_by + axis_z[c] * newb_z for c in every]
    second = [center[c] + axis_x[c] * final_cx + axis_y[c] * final_cy + axis_z[c] * newc_z for c in every]
    return oxygen + first + second


def sort_keys(keys):
    lane = lax.broadcasted_iota(jnp.int32, (8, LANES), 1)
    sub = lax.broadcasted_iota(jnp.int32, (8, LANES), 0)
    reg_bits = (len(keys) - 1).bit_length()
    bits = reg_bits + 10
    base = (lane * 8 + sub) << reg_bits

    for size in range(1, bits + 1):
        for bit in range(size - 1, -1, -1):
            if bit < reg_bits:
                out = list(keys)
                for reg in range(len(keys)):
                    if reg & (1 << bit):
                        continue
                    other = reg | (1 << bit)
                    low = jnp.minimum(keys[reg], keys[other])
                    high = jnp.maximum(keys[reg], keys[other])
                    if size == bits:
                        out[reg], out[other] = low, high
                    elif size < reg_bits:
                        out[reg], out[other] = (high, low) if reg & (1 << size) else (low, high)
                    else:
                        rising = ((base >> size) & 1) == 0
                        out[reg] = jnp.where(rising, low, high)
                        out[other] = jnp.where(rising, high, low)
                keys = out
                continue
            turned = base >> bit if size == bits else (base >> bit) ^ (base >> size)
            keep = (turned & 1) == 0
            out = []
            for key in keys:
                step = 1 << (bit - reg_bits)
                if step == 4:
                    mate = pltpu.roll(key, 4, 0)
                elif step < 4:
                    upper = (sub & step) != 0
                    mate = jnp.where(upper, pltpu.roll(key, step, 0), pltpu.roll(key, 8 - step, 0))
                else:
                    mate = lanes_of(key, lane ^ (step // 8))
                out.append(jnp.where(keep, jnp.minimum(key, mate), jnp.maximum(key, mate)))
            keys = out
    return keys


def find(table, rows, queries):
    heads = table[0:1, :]
    marks = [jnp.broadcast_to(heads[:, 8 * i : 8 * i + 1], (8, LANES)) for i in range(1, 16)]
    wide = jnp.broadcast_to(heads, (8, LANES))
    found = []
    for query in queries:
        group = jnp.zeros((8, LANES), jnp.int32)
        for mark in marks:
            group = group + jnp.where(mark < query, 8, 0)
        column = group
        for i in range(1, 8):
            column = column + jnp.where(lanes_of(wide, group + i) < query, 1, 0)
        rank = column * rows
        best = jnp.full((8, LANES), -1.0, jnp.float32)
        for r in range(rows):
            key = lanes_of(spread(table, r), column)
            below = key < query
            rank = rank + jnp.where(below, 1, 0)
            best = jnp.maximum(best, jnp.where(below, key, -1.0))
        found.append((rank, best.astype(jnp.int32)))
    return found


def prepare(
    pos, vel, mass, bonds, left, right, water_pos, water_vel, pay, place, water_out, atoms, ranked, slots, wet
):
    lane = lax.broadcasted_iota(jnp.int32, (8, LANES), 1)
    sub = lax.broadcasted_iota(jnp.int32, (8, LANES), 0)
    f32, i32 = jnp.float32, jnp.int32

    def index(k):
        return (k * 8 + sub) * LANES + lane

    for r in range(BOND_ROWS):
        cut = slice(r * LANES, (r + 1) * LANES)
        atoms[r : r + 1, :] = bonds[0:1, cut]
        atoms[BOND_ROWS + r : BOND_ROWS + r + 1, :] = bonds[1:2, cut]
    atoms[END_ROWS:32, :] = jnp.full((32 - END_ROWS, LANES), 2048, i32)
    atoms[32 : 32 + SLOT_ROWS, :] = right[...]
    atoms[32 + SLOT_ROWS : 32 + CROSS_ROWS, :] = left[...]
    atoms[32 + CROSS_ROWS : 40, :] = jnp.full((8 - CROSS_ROWS, LANES), 4096, i32)
    crossed = atoms[32:40, :]

    keys = [(atoms[8 * k : 8 * k + 8, :] * 4096 + index(k)).astype(f32) for k in range(4)]
    keys = sort_keys(keys)
    for k in range(4):
        ranked[8 * k : 8 * k + 8, :] = keys[k]
    slots[...] = sort_keys([(crossed * 1024 + index(0)).astype(f32)])[0]

    own, far, mates = [], [], []
    for k in range(3):
        rank = lane * END_ROWS + k * 8 + sub
        key = gather_rows(
            functools.partial(spread, ranked), 32, (rank & 3) * 8 + ((rank >> 2) & 7), rank >> 5
        ).astype(i32)
        end = key & 4095
        mate = jnp.where(end < HALF, end + HALF, end - HALF)
        other = gather_rows(functools.partial(spread, atoms), END_ROWS, mate >> 7, mate & 127)
        own.append(jnp.minimum(key >> 12, 2047))
        far.append(jnp.minimum(other, 2047))
        mates.append((other * 4096 + mate).astype(f32))

    def put(block, k, value):
        count = min(8, END_ROWS - 8 * k)
        pay[block + 8 * k : block + 8 * k + count, :] = value[:count].astype(f32)

    inside = find(
        ranked,
        32,
        mates + [((crossed + 1) * 4096).astype(f32)] + [((index(k) + 1) * 4096).astype(f32) for k in range(2)],
    )
    outside = find(
        slots, 8, [((a + 1) * 1024).astype(f32) for a in own] + [((index(k) + 1) * 1024).astype(f32) for k in range(2)]
    )
    for k in range(3):
        put(ATOM, k, own[k])
        put(MATE, k, inside[k][0])
        best = outside[k][1]
        put(LINK, k, jnp.where(best >> 10 == own[k], best & 1023, NONE))
    rank, best = inside[3]
    host = jnp.where(best >> 12 == crossed, rank - 1, NONE)
    pay[HOST : HOST + CROSS_ROWS, :] = host[:CROSS_ROWS].astype(f32)
    for k in range(2):
        rank, best = inside[4 + k]
        slot = outside[3 + k][1]
        row, col = place_of(rank - 1)
        place[8 * k : 8 * k + 8, :] = jnp.where(
            best >> 12 == index(k),
            row * LANES + col,
            jnp.where(slot >> 10 == index(k), END_ROWS * LANES + (slot & 1023), -1),
        )

    edge = jnp.minimum(crossed, 2047)
    where = [(a >> 7, a & 127) for a in own + far + [edge]]

    def at_ends(table):
        return [gather_rows(table, ATOM_ROWS, row, col) for row, col in where]

    for block, cross, source in ((DIFF, CPOS, pos), (VELO, CVEL, vel)):
        for c in range(3):
            values = at_ends(
                lambda r: jnp.broadcast_to(source[c : c + 1, r * LANES : (r + 1) * LANES], (8, LANES))
            )
            for k in range(3):
                put(block + END_ROWS * c, k, values[k] - values[3 + k])
            pay[cross + CROSS_ROWS * c : cross + CROSS_ROWS * (c + 1), :] = values[6][:CROSS_ROWS]
    values = at_ends(functools.partial(spread, mass))
    for k in range(3):
        put(MASS, k, values[k])
        put(SCAL, k, 1.0 / jnp.sqrt(values[k] + values[3 + k]))
    pay[CMAS : CMAS + CROSS_ROWS, :] = values[6][:CROSS_ROWS]

    for j in range(8):
        cut = slice(j * LANES, (j + 1) * LANES)
        for c in range(9):
            wet[c, j : j + 1, :] = water_pos[c : c + 1, cut]
            wet[9 + c, j : j + 1, :] = water_vel[c : c + 1, cut]
    before = [wet[c] for c in range(9)]
    speed = [wet[9 + c] for c in range(9)]
    after = [before[c] + time_step * speed[c] for c in range(9)]
    settled = settle(before, after)
    for c in range(9):
        result = speed[c] + (settled[c] - after[c]) / time_step
        for j in range(8):
            water_out[c : c + 1, j * LANES : (j + 1) * LANES] = result[j : j + 1, :]


def solve(
    whole, place, vel, out,
    mate_row, mate_col, link_row, link_col, host_row, host_col, atom, mass, push, length, scale, diff, drift,
    below, above, near, hinge, edge, edge_mass, edge_length, edge_scale, edge_diff, edge_drift, anchor,
    now, total, now_edge, total_edge, part, ties, moved, moved_edge, run, more,
):
    zero = jnp.zeros((8, LANES), jnp.float32)
    every, ends, right = range(3), range(END_ROWS), range(SLOT_ROWS)

    def load(r):
        return whole[pl.ds(r, DOMAINS, stride=ROWS), :]

    def up(x):
        return pltpu.roll(x, DOMAINS - 1, 0)

    def down(x):
        return pltpu.roll(x, 1, 0)

    def around(rows):
        wide = {v: rows[v] for v in ends}
        for s in range(1, NEAR + 1):
            wide[-s] = pltpu.roll(rows[END_ROWS - s], 1, 1)
            wide[END_ROWS - 1 + s] = pltpu.roll(rows[s - 1], LANES - 1, 1)
        return wide

    def choose(rows, count, masks, col):
        return pick(lambda r: lanes_of(rows[r], col), count, masks)

    def both(values):
        return values + [down(x) for x in values]

    for v in ends:
        row, col = place_of(load(MATE + v).astype(jnp.int32))
        mate_row[v], mate_col[v] = row, col
        slot = load(LINK + v).astype(jnp.int32)
        link_row[v], link_col[v] = slot >> 7, slot & 127
        mass[v] = load(MASS + v)
        atom[v] = load(ATOM + v)
    for r in range(CROSS_ROWS):
        row, col = place_of(load(HOST + r).astype(jnp.int32))
        host_row[r], host_col[r] = row, jnp.minimum(col, LANES - 1)
        anchor[r] = jnp.where(col < LANES, 1.0, 0.0)

    for v in ends:
        d = [load(DIFF + END_ROWS * c + v) for c in every]
        g = [time_step * load(VELO + END_ROWS * c + v) for c in every]
        s = load(SCAL + v)
        size = jnp.sqrt(dot3(d, d))
        rate = s / size
        rhs = rate * dot3(d, g)
        length[v], scale[v], now[v], total[v] = size, s, rhs, rhs
        for c in every:
            diff[c, v], drift[c, v], push[c, v], moved[c, v] = d[c], g[c], rate * d[c], zero

    start = []
    for r in right:
        l = r + SLOT_ROWS
        d = [load(CPOS + CROSS_ROWS * c + r) - up(load(CPOS + CROSS_ROWS * c + l)) for c in every]
        g = [
            time_step * (load(CVEL + CROSS_ROWS * c + r) - up(load(CVEL + CROSS_ROWS * c + l))) for c in every
        ]
        edge_mass[r], edge_mass[l] = load(CMAS + r), load(CMAS + l)
        s = 1.0 / jnp.sqrt(edge_mass[r] + up(edge_mass[l]))
        size = jnp.sqrt(dot3(d, d))
        rate = s / size
        edge_length[r], edge_scale[r] = size, s
        start.append(rate * dot3(d, g))
        for c in every:
            edge_diff[c, r], edge_drift[c, r] = d[c], g[c]
            edge[c, r], edge[c, l] = rate * d[c], -down(rate * d[c])
            moved_edge[c, r], moved_edge[c, l] = zero, zero
    for r, x in enumerate(both(start)):
        now_edge[r], total_edge[r] = x, x

    names = around([atom[v] for v in ends])
    many = jnp.zeros((8, LANES), jnp.int32)
    fields = [around([push[c, v] for v in ends]) for c in every]
    for v in ends:
        here = [mass[v] * push[c, v] for c in every]
        for s in range(1, NEAR + 1):
            same = names[v] == names[v - s]
            near[s - 1, v] = jnp.where(same, 1.0, 0.0)
            below[s - 1, v] = jnp.where(same, dot3(here, [fields[c][v - s] for c in every]), 0.0)
            above[s - 1, v] = jnp.where(
                names[v] == names[v + s], dot3(here, [fields[c][v + s] for c in every]), 0.0
            )
        past = names[v - 4] if v >= 1 else pltpu.roll(atom[END_ROWS - 4], 1, 1)
        many = jnp.where(names[v] == past, 1, many)
        masks = bits_of(link_row[v], CROSS_ROWS)
        linked = link_row[v] < CROSS_ROWS
        across = [choose([edge[c, r] for r in range(CROSS_ROWS)], CROSS_ROWS, masks, link_col[v]) for c in every]
        for c in every:
            ties[c, v] = jnp.where(linked, mass[v] * across[c], 0.0)
        hinge[v] = jnp.where(linked, dot3(here, across), 0.0)
    crowded = jnp.max(many) > 0

    def gated(factor, value):
        return jnp.where(factor != 0.0, factor * value, 0.0)

    def scan(rows, forward):
        def double(k, carry):
            step = lax.shift_left(1, k)
            turns = step // END_ROWS
            rest = step - turns * END_ROWS

            def one(v, carry):
                source = v - rest if forward else v + rest
                wrap = jnp.where(source < 0, 1, 0) if forward else jnp.where(source >= END_ROWS, 1, 0)
                source = source + wrap * END_ROWS if forward else source - wrap * END_ROWS
                shift = turns + wrap if forward else (LANES - turns - wrap)
                match = atom[v] == pltpu.roll(atom[source], shift, 1)
                for r in rows:
                    more[r, v] = run[r, v] + jnp.where(match, pltpu.roll(run[r, source], shift, 1), 0.0)
                return carry

            lax.fori_loop(0, END_ROWS, one, 0)

            def keep(v, carry):
                for r in rows:
                    run[r, v] = more[r, v]
                return carry

            return lax.fori_loop(0, END_ROWS, keep, carry)

        lax.fori_loop(0, 12, double, 0)

    def scan_fields(source):
        def fill(v, carry):
            x = source[v]
            for c in every:
                run[c, v] = push[c, v] * x
                run[3 + c, v] = push[c, v] * x
            run[6, v] = gated(hinge[v], x)
            return carry

        lax.fori_loop(0, END_ROWS, fill, 0)
        scan((0, 1, 2, 6), True)
        scan((3, 4, 5), False)

    def at_edges(table):
        got = []
        for r in range(CROSS_ROWS):
            value = choose(table, END_ROWS, bits_of(host_row[r], END_ROWS), host_col[r])
            got.append(value)
        return got

    def apply(order, carry):
        x = around([now[v] for v in ends])
        bound = {v: gated(hinge[v], x[v]) for v in ends}
        wide = around([bound[v] for v in ends])
        for v in ends:
            sum_x, sum_bound = zero, bound[v]
            for s in range(1, NEAR + 1):
                sum_x = sum_x + gated(below[s - 1, v], x[v - s])
                sum_x = sum_x + gated(above[s - 1, v], x[v + s])
                sum_bound = sum_bound + jnp.where(near[s - 1, v] > 0.5, wide[v - s], 0.0)
            part[0, v] = sum_x
            part[1, v] = sum_bound

        @pl.when(crowded)
        def _():
            scan_fields(now)

            def fill(v, carry):
                here = [push[c, v] for c in every]
                both_sides = [run[c, v] + run[3 + c, v] - 2.0 * here[c] * now[v] for c in every]
                part[0, v] = mass[v] * dot3(here, both_sides)
                part[1, v] = run[6, v]
                return carry

            lax.fori_loop(0, END_ROWS, fill, 0)

        crossing = [now_edge[r] for r in range(CROSS_ROWS)]
        whole_part = []
        for v in ends:
            value = choose(crossing, CROSS_ROWS, bits_of(link_row[v], CROSS_ROWS), link_col[v])
            whole_part.append(part[0, v] + gated(hinge[v], value))
        pulled = at_edges([part[1, v] for v in ends])
        pulled = [jnp.where(anchor[r] > 0.5, pulled[r], 0.0) for r in range(CROSS_ROWS)]
        for r, value in enumerate(both([-(pulled[r] + up(pulled[r + SLOT_ROWS])) for r in right])):
            now_edge[r] = value
            total_edge[r] = total_edge[r] + value
        for v in ends:
            value = choose(whole_part, END_ROWS, bits_of(mate_row[v], END_ROWS), mate_col[v])
            value = -(whole_part[v] + value)
            now[v] = value
            total[v] = total[v] + value
        return carry

    def edges_moved():
        got = []
        for r in range(CROSS_ROWS):
            masks = bits_of(host_row[r], END_ROWS)
            fast = anchor[r] > 0.5
            got.append(
                [
                    jnp.where(fast, choose([moved[c, v] for v in ends], END_ROWS, masks, host_col[r]), moved_edge[c, r])
                    for c in every
                ]
            )
        return got

    def turn(index, carry):
        lax.fori_loop(0, ORDER, apply, 0)

        x = [total[v] for v in ends]
        for c in every:
            field = around([push[c, v] * x[v] for v in ends])
            for v in ends:
                value = field[v]
                for s in range(1, NEAR + 1):
                    value = value + jnp.where(names_equal(v, -s), field[v - s], 0.0)
                    value = value + jnp.where(names_equal(v, s), field[v + s], 0.0)
                run[c, v] = value

        @pl.when(crowded)
        def _():
            scan_fields(total)

            def fill(v, carry):
                for c in every:
                    run[c, v] = run[c, v] + run[3 + c, v] - push[c, v] * total[v]
                return carry

            lax.fori_loop(0, END_ROWS, fill, 0)

        crossing = [total_edge[r] for r in range(CROSS_ROWS)]
        for v in ends:
            value = choose(crossing, CROSS_ROWS, bits_of(link_row[v], CROSS_ROWS), link_col[v])
            linked = link_row[v] < CROSS_ROWS
            for c in every:
                moved[c, v] = moved[c, v] + mass[v] * run[c, v] + jnp.where(linked, ties[c, v] * value, 0.0)
        for r in range(CROSS_ROWS):
            for c in every:
                moved_edge[c, r] = moved_edge[c, r] + edge_mass[r] * edge[c, r] * crossing[r]

        def correct(d, g, size, s):
            excess = 2.0 * dot3(d, g) + dot3(g, g)
            return s * excess / (size + jnp.sqrt(size * size - excess))

        @pl.when(index < ITER)
        def _():
            here = edges_moved()
            start = []
            for r in right:
                g = [edge_drift[c, r] - (here[r][c] - up(here[r + SLOT_ROWS][c])) for c in every]
                start.append(correct([edge_diff[c, r] for c in every], g, edge_length[r], edge_scale[r]))
            for r, value in enumerate(both(start)):
                now_edge[r], total_edge[r] = value, value
            for v in ends:
                masks = bits_of(mate_row[v], END_ROWS)
                there = [choose([moved[c, w] for w in ends], END_ROWS, masks, mate_col[v]) for c in every]
                g = [drift[c, v] - (moved[c, v] - there[c]) for c in every]
                value = correct([diff[c, v] for c in every], g, length[v], scale[v])
                now[v], total[v] = value, value

        return carry

    def names_equal(v, s):
        flag = near[s - 1, v + s] if s > 0 and v + s < END_ROWS else None
        if s < 0:
            flag = near[-s - 1, v]
        elif flag is None:
            flag = pltpu.roll(near[s - 1, v + s - END_ROWS], LANES - 1, 1)
        return flag > 0.5

    lax.fori_loop(0, ITER + 1, turn, 0)

    me = lax.axis_index("dom")
    edges = edges_moved()
    for r in range(CROSS_ROWS):
        for c in every:
            moved_edge[c, r] = edges[r][c]
    own = [
        [jnp.broadcast_to(moved[c, v, pl.ds(me, 1), :], (8, LANES)) for v in ends]
        + [jnp.broadcast_to(moved_edge[c, r, pl.ds(me, 1), :], (8, LANES)) for r in range(CROSS_ROWS)]
        for c in every
    ]
    for k in range(2):
        code = place[8 * k : 8 * k + 8, :]
        bound = code >= 0
        code = jnp.maximum(code, 0)
        masks = bits_of(code >> 7, END_ROWS + CROSS_ROWS)
        for c in every:
            shift = choose(own[c], END_ROWS + CROSS_ROWS, masks, code & 127)
            shift = jnp.where(bound, shift, 0.0) / time_step
            for j in range(8):
                cut = slice((8 * k + j) * LANES, (8 * k + j + 1) * LANES)
                out[c : c + 1, cut] = vel[c : c + 1, cut] - shift[j : j + 1, :]


def on_device(
    protein_pos, protein_vel, inv_mass, bond_atoms, left_atoms, right_atoms, water_pos, water_vel
):
    f32, i32 = jnp.float32, jnp.int32
    mass = inv_mass.reshape(ATOM_ROWS, LANES)
    pay, place, water_velocity = pl.pallas_call(
        prepare,
        out_shape=(
            jax.ShapeDtypeStruct((ROWS, LANES), f32),
            jax.ShapeDtypeStruct((ATOM_ROWS, LANES), i32),
            jax.ShapeDtypeStruct(water_pos.shape, f32),
        ),
        scratch_shapes=[
            pltpu.VMEM((40, LANES), i32),
            pltpu.VMEM((32, LANES), f32),
            pltpu.VMEM((8, LANES), f32),
            pltpu.VMEM((18, 8, LANES), f32),
        ],
        name="prepare",
    )(
        protein_pos,
        protein_vel,
        mass,
        bond_atoms,
        left_atoms.reshape(SLOT_ROWS, LANES),
        right_atoms.reshape(SLOT_ROWS, LANES),
        water_pos,
        water_vel,
    )
    whole = lax.all_gather(pay, "dom", axis=0, tiled=True)

    def rows(*lead, dtype=f32):
        return pltpu.VMEM((*lead, 8, LANES), dtype)

    n, m = END_ROWS, CROSS_ROWS
    protein_velocity = pl.pallas_call(
        solve,
        out_shape=jax.ShapeDtypeStruct(protein_vel.shape, f32),
        scratch_shapes=[
            *(rows(n, dtype=i32) for _ in range(4)),
            *(rows(m, dtype=i32) for _ in range(2)),
            *(rows(n) for _ in range(2)),
            rows(3, n),
            *(rows(n) for _ in range(2)),
            *(rows(3, n) for _ in range(2)),
            *(rows(NEAR, n) for _ in range(3)),
            rows(n),
            rows(3, m),
            *(rows(m) for _ in range(3)),
            *(rows(3, m) for _ in range(2)),
            rows(m),
            *(rows(n) for _ in range(2)),
            *(rows(m) for _ in range(2)),
            rows(2, n),
            *(rows(3, n) for _ in range(2)),
            rows(3, m),
            *(rows(7, n) for _ in range(2)),
        ],
        name="solve",
    )(whole, place, protein_vel)
    return (protein_velocity, water_velocity)


def solution(mesh):
    in_specs = (
        P(None, ("rep", "dom")),
        P(None, ("rep", "dom")),
        P(("rep", "dom")),
        P(None, ("rep", "dom")),
        P(("rep", "dom")),
        P(("rep", "dom")),
        P(None, ("rep", "dom")),
        P(None, ("rep", "dom")),
    )
    out_specs = (P(None, ("rep", "dom")), P(None, ("rep", "dom")))
    return jax.shard_map(
        on_device, mesh=mesh, in_specs=in_specs, out_specs=out_specs, check_vma=False
    )
```

```python
import functools
import math

import jax
import jax.numpy as jnp
from jax import lax
from jax.experimental import pallas as pl
from jax.experimental.pallas import tpu as pltpu
from jax.sharding import PartitionSpec as P

ORDER = 4
ITER = 2

time_step = 0.002
mass_oxygen = 15.9994
mass_hydrogen = 1.008
oxygen_hydrogen = 0.09572
hydrogen_pair = 0.15139
total_mass = mass_oxygen + 2.0 * mass_hydrogen
half_pair = 0.5 * hydrogen_pair
water_height = math.sqrt(oxygen_hydrogen * oxygen_hydrogen - half_pair * half_pair)
oxygen_reach = 2.0 * mass_hydrogen * water_height / total_mass
hydrogen_reach = water_height - oxygen_reach

LANES = 128
DOMAINS = 8
ATOM_ROWS = 16
BOND_ROWS = 10
SLOT_ROWS = 3
END_ROWS = 2 * BOND_ROWS
HALF = BOND_ROWS * LANES
CROSS_ROWS = 2 * SLOT_ROWS
NEAR = 3
NONE = 4095
UNROLLED = True

DIFF, VELO, SCAL = 0, 3 * END_ROWS, 6 * END_ROWS
MASS, MATE, NAME = (k * END_ROWS for k in (7, 8, 9))
CPOS = 10 * END_ROWS
CVEL, CMAS, HOST = CPOS + 3 * CROSS_ROWS, CPOS + 6 * CROSS_ROWS, CPOS + 7 * CROSS_ROWS
ROWS = -(-(CPOS + 8 * CROSS_ROWS) // 8) * 8


def lanes_of(table, index):
    dims = lax.GatherDimensionNumbers(
        offset_dims=(),
        collapsed_slice_dims=(1,),
        start_index_map=(1,),
        operand_batching_dims=(0,),
        start_indices_batching_dims=(0,),
    )
    return lax.gather(
        table, index[..., None], dims, (1, 1), mode=lax.GatherScatterMode.PROMISE_IN_BOUNDS
    )


def bits_of(row, count):
    return [(row & (1 << b)) != 0 for b in range(max(1, (count - 1).bit_length()))]


def pick(get, count, masks, low=0):
    if count == 1:
        return get(low)
    bit = (count - 1).bit_length() - 1
    half = 1 << bit
    left = pick(get, half, masks, low)
    right = pick(get, count - half, masks, low + half)
    return jnp.where(masks[bit], right, left)


def gather_rows(table, count, row, lane):
    masks = bits_of(row, count)
    return pick(lambda r: lanes_of(table(r), lane), count, masks)


def spread(ref, r):
    return jnp.broadcast_to(ref[r : r + 1, :], (8, LANES))


def place_of(position):
    lane = (position * 3277) >> 16
    return position - lane * END_ROWS, lane


def cross3(a, b):
    return [a[1] * b[2] - a[2] * b[1], a[2] * b[0] - a[0] * b[2], a[0] * b[1] - a[1] * b[0]]


def dot3(a, b):
    return a[0] * b[0] + a[1] * b[1] + a[2] * b[2]


def settle(before, after):
    old_o, old_1, old_2 = before[0:3], before[3:6], before[6:9]
    new_o, new_1, new_2 = after[0:3], after[3:6], after[6:9]
    every = range(3)
    center = [(mass_oxygen * new_o[c] + mass_hydrogen * (new_1[c] + new_2[c])) / total_mass for c in every]
    old_b = [old_1[c] - old_o[c] for c in every]
    old_c = [old_2[c] - old_o[c] for c in every]
    rel_a = [new_o[c] - center[c] for c in every]
    rel_b = [new_1[c] - center[c] for c in every]
    rel_c = [new_2[c] - center[c] for c in every]
    normal = cross3(old_b, old_c)
    side = cross3(rel_a, normal)
    upward = cross3(normal, side)

    def normed(v):
        size = jnp.sqrt(dot3(v, v))
        return [part / size for part in v]

    axis_z, axis_x, axis_y = normed(normal), normed(side), normed(upward)
    oldb_x, oldb_y = dot3(axis_x, old_b), dot3(axis_y, old_b)
    oldc_x, oldc_y = dot3(axis_x, old_c), dot3(axis_y, old_c)
    newa_z = dot3(axis_z, rel_a)
    newb_x, newb_y, newb_z = dot3(axis_x, rel_b), dot3(axis_y, rel_b), dot3(axis_z, rel_b)
    newc_x, newc_y, newc_z = dot3(axis_x, rel_c), dot3(axis_y, rel_c), dot3(axis_z, rel_c)
    sin_phi = newa_z / oxygen_reach
    cos_phi = jnp.sqrt(1.0 - sin_phi * sin_phi)
    sin_psi = (newb_z - newc_z) / (2.0 * half_pair * cos_phi)
    cos_psi = jnp.sqrt(1.0 - sin_psi * sin_psi)
    rest_ay = oxygen_reach * cos_phi
    rest_bx = -half_pair * cos_psi
    lowered = -hydrogen_reach * cos_phi
    tilted = half_pair * sin_psi * sin_phi
    rest_by = lowered - tilted
    rest_cy = lowered + tilted
    alpha = rest_bx * (oldb_x - oldc_x) + oldb_y * rest_by + oldc_y * rest_cy
    beta = rest_bx * (oldc_y - oldb_y) + oldb_x * rest_by + oldc_x * rest_cy
    gamma = oldb_x * newb_y - newb_x * oldb_y + oldc_x * newc_y - newc_x * oldc_y
    summed = alpha * alpha + beta * beta
    sin_theta = (alpha * gamma - beta * jnp.sqrt(summed - gamma * gamma)) / summed
    cos_theta = jnp.sqrt(1.0 - sin_theta * sin_theta)
    final_ax = -rest_ay * sin_theta
    final_ay = rest_ay * cos_theta
    final_bx = rest_bx * cos_theta - rest_by * sin_theta
    final_by = rest_bx * sin_theta + rest_by * cos_theta
    final_cx = -rest_bx * cos_theta - rest_cy * sin_theta
    final_cy = -rest_bx * sin_theta + rest_cy * cos_theta
    oxygen = [center[c] + axis_x[c] * final_ax + axis_y[c] * final_ay + axis_z[c] * newa_z for c in every]
    first = [center[c] + axis_x[c] * final_bx + axis_y[c] * final_by + axis_z[c] * newb_z for c in every]
    second = [center[c] + axis_x[c] * final_cx + axis_y[c] * final_cy + axis_z[c] * newc_z for c in every]
    return oxygen + first + second


def sort_keys(keys):
    lane = lax.broadcasted_iota(jnp.int32, (8, LANES), 1)
    sub = lax.broadcasted_iota(jnp.int32, (8, LANES), 0)
    reg_bits = (len(keys) - 1).bit_length()
    bits = reg_bits + 10
    base = (lane * 8 + sub) << reg_bits

    def ordered(bit, size, here, there):
        turned = base >> bit if size == bits else (base >> bit) ^ (base >> size)
        return jnp.where((turned & 1) == 0, jnp.minimum(here, there), jnp.maximum(here, there))

    def registers(keys, bit, size):
        out = list(keys)
        for reg in range(len(keys)):
            if reg & (1 << bit):
                continue
            other = reg | (1 << bit)
            low = jnp.minimum(keys[reg], keys[other])
            high = jnp.maximum(keys[reg], keys[other])
            if size == bits:
                out[reg], out[other] = low, high
            elif size < reg_bits:
                out[reg], out[other] = (high, low) if reg & (1 << size) else (low, high)
            else:
                rising = ((base >> size) & 1) == 0
                out[reg] = jnp.where(rising, low, high)
                out[other] = jnp.where(rising, high, low)
        return out

    def sublanes(key, bit, size):
        step = 1 << (bit - reg_bits)
        if step == 4:
            mate = pltpu.roll(key, 4, 0)
        else:
            mate = jnp.where((sub & step) != 0, pltpu.roll(key, step, 0), pltpu.roll(key, 8 - step, 0))
        return ordered(bit, size, key, mate)

    def lanes(key, group, size):
        steps = [1 << (bit - reg_bits - 3) for bit in group]
        reach = [0]
        for step in steps:
            reach = reach + [far ^ step for far in reach]
        values = {far: lanes_of(key, lane ^ far) if far else key for far in reach}
        for bit, step in zip(group, steps):
            values = {
                far: ordered(bit, size, values[far], values[far ^ step])
                for far in values
                if far < step
            }
        return values[0]

    for size in range(1, bits + 1):
        crossing = [bit for bit in range(size - 1, reg_bits + 2, -1)]
        while crossing:
            width = {4: 2, 2: 2, 1: 1}.get(len(crossing), 3)
            group, crossing = crossing[:width], crossing[width:]
            keys = [lanes(key, group, size) for key in keys]
        for bit in range(min(size - 1, reg_bits + 2), -1, -1):
            if bit < reg_bits:
                keys = registers(keys, bit, size)
            else:
                keys = [sublanes(key, bit, size) for key in keys]
    return keys


def find(table, rows, queries):
    heads = table[0:1, :]
    marks = [jnp.broadcast_to(heads[:, 8 * i : 8 * i + 1], (8, LANES)) for i in range(1, 16)]
    wide = jnp.broadcast_to(heads, (8, LANES))
    found = []
    for query in queries:
        group = jnp.zeros((8, LANES), jnp.int32)
        for mark in marks:
            group = group + jnp.where(mark < query, 8, 0)
        column = group
        for i in range(1, 8):
            column = column + jnp.where(lanes_of(wide, group + i) < query, 1, 0)
        rank = column * rows
        best = jnp.full((8, LANES), -1.0, jnp.float32)
        for r in range(rows):
            key = lanes_of(spread(table, r), column)
            below = key < query
            rank = rank + jnp.where(below, 1, 0)
            best = jnp.maximum(best, jnp.where(below, key, -1.0))
        found.append((rank, best.astype(jnp.int32)))
    return found


def prepare(
    bonds_in, right_in, left_in, pos_in, vel_in, mass_in, water_pos_in, water_vel_in, pay, place, water_out,
    bonds, right, left, pos, vel, mass, water_pos, water_vel, atoms, ranked, slots, wet, arrived,
):
    lane = lax.broadcasted_iota(jnp.int32, (8, LANES), 1)
    sub = lax.broadcasted_iota(jnp.int32, (8, LANES), 0)
    f32, i32 = jnp.float32, jnp.int32

    sources = (bonds_in, right_in, left_in, pos_in, vel_in, mass_in, water_pos_in, water_vel_in)
    targets = (bonds, right, left, pos, vel, mass, water_pos, water_vel)
    copies = [
        pltpu.make_async_copy(source, target, arrived.at[k])
        for k, (source, target) in enumerate(zip(sources, targets))
    ]
    for copy in copies:
        copy.start()
    for copy in copies:
        copy.wait()

    def index(k):
        return (k * 8 + sub) * LANES + lane

    for r in range(BOND_ROWS):
        cut = slice(r * LANES, (r + 1) * LANES)
        atoms[r : r + 1, :] = bonds[0:1, cut]
        atoms[BOND_ROWS + r : BOND_ROWS + r + 1, :] = bonds[1:2, cut]
    atoms[END_ROWS:32, :] = jnp.full((32 - END_ROWS, LANES), 2048, i32)
    atoms[32 : 32 + SLOT_ROWS, :] = right[...]
    atoms[32 + SLOT_ROWS : 32 + CROSS_ROWS, :] = left[...]
    atoms[32 + CROSS_ROWS : 40, :] = jnp.full((8 - CROSS_ROWS, LANES), 4096, i32)
    crossed = atoms[32:40, :]

    keys = [(atoms[8 * k : 8 * k + 8, :] * 4096 + index(k)).astype(f32) for k in range(4)]
    keys = sort_keys(keys)
    for k in range(4):
        ranked[pl.ds(k, 8, stride=4), :] = keys[k]
    slots[...] = sort_keys([(crossed * 1024 + index(0)).astype(f32)])[0]

    own, far, mates = [], [], []
    quads = []
    for j in range(8):
        quad = ranked[4 * j : 4 * j + 4, :]
        quads.append(jnp.concatenate([quad, quad], axis=0))
    for k in range(3):
        rank = lane * END_ROWS + k * 8 + sub
        masks = bits_of((rank >> 2) & 7, 8)
        key = pick(lambda j: lanes_of(quads[j], rank >> 5), 8, masks).astype(i32)
        end = key & 4095
        mate = jnp.where(end < HALF, end + HALF, end - HALF)
        other = gather_rows(functools.partial(spread, atoms), END_ROWS, mate >> 7, mate & 127)
        own.append(jnp.minimum(key >> 12, 2047))
        far.append(jnp.minimum(other, 2047))
        mates.append((other * 4096 + mate).astype(f32))

    def put(block, k, value):
        count = min(8, END_ROWS - 8 * k)
        pay[block + 8 * k : block + 8 * k + count, :] = value[:count].astype(f32)

    inside = find(
        ranked,
        32,
        mates + [((crossed + 1) * 4096).astype(f32)] + [((index(k) + 1) * 4096).astype(f32) for k in range(2)],
    )
    outside = find(
        slots, 8, [((a + 1) * 1024).astype(f32) for a in own] + [((index(k) + 1) * 1024).astype(f32) for k in range(2)]
    )
    for k in range(3):
        put(MATE, k, inside[k][0])
        best = outside[k][1]
        put(NAME, k, jnp.where(best >> 10 == own[k], best & 1023, own[k] + 1024))
    rank, best = inside[3]
    host = jnp.where(best >> 12 == crossed, rank - 1, NONE)
    pay[HOST : HOST + CROSS_ROWS, :] = host[:CROSS_ROWS].astype(f32)
    for k in range(2):
        rank, best = inside[4 + k]
        slot = outside[3 + k][1]
        row, col = place_of(rank - 1)
        place[8 * k : 8 * k + 8, :] = jnp.where(
            best >> 12 == index(k),
            row * LANES + col,
            jnp.where(slot >> 10 == index(k), END_ROWS * LANES + (slot & 1023), -1),
        )

    edge = jnp.minimum(crossed, 2047)
    where = [(a >> 7, a & 127) for a in own + far + [edge]]

    def at_ends(table):
        return [gather_rows(table, ATOM_ROWS, row, col) for row, col in where]

    for block, cross, source in ((DIFF, CPOS, pos), (VELO, CVEL, vel)):
        for c in range(3):
            values = at_ends(
                lambda r: jnp.broadcast_to(source[c : c + 1, r * LANES : (r + 1) * LANES], (8, LANES))
            )
            for k in range(3):
                put(block + END_ROWS * c, k, values[k] - values[3 + k])
            pay[cross + CROSS_ROWS * c : cross + CROSS_ROWS * (c + 1), :] = values[6][:CROSS_ROWS]
    values = at_ends(functools.partial(spread, mass))
    for k in range(3):
        put(MASS, k, values[k])
        put(SCAL, k, 1.0 / jnp.sqrt(values[k] + values[3 + k]))
    pay[CMAS : CMAS + CROSS_ROWS, :] = values[6][:CROSS_ROWS]

    for j in range(8):
        cut = slice(j * LANES, (j + 1) * LANES)
        for c in range(9):
            wet[c, j : j + 1, :] = water_pos[c : c + 1, cut]
            wet[9 + c, j : j + 1, :] = water_vel[c : c + 1, cut]
    before = [wet[c] for c in range(9)]
    speed = [wet[9 + c] for c in range(9)]
    after = [before[c] + time_step * speed[c] for c in range(9)]
    settled = settle(before, after)
    for c in range(9):
        result = speed[c] + (settled[c] - after[c]) / time_step
        for j in range(8):
            water_out[c : c + 1, j * LANES : (j + 1) * LANES] = result[j : j + 1, :]


def solve(
    whole, place, vel, out,
    mate_row, mate_col, link_row, link_col, host_row, host_col, name, mass, push, length, scale, diff, drift,
    below, above, near, hinge, hinges, edge, edge_mass, edge_length, edge_scale, edge_diff, edge_drift, anchor,
    now, total, now_edge, total_edge, part, ties, moved, moved_edge, run, more,
):
    zero = jnp.zeros((8, LANES), jnp.float32)
    every, ends, right = range(3), range(END_ROWS), range(SLOT_ROWS)

    def load(r):
        return whole[pl.ds(r, DOMAINS, stride=ROWS), :]

    def up(x):
        return pltpu.roll(x, DOMAINS - 1, 0)

    def down(x):
        return pltpu.roll(x, 1, 0)

    def around(rows):
        wide = {v: rows[v] for v in ends}
        for s in range(1, NEAR + 1):
            wide[-s] = pltpu.roll(rows[END_ROWS - s], 1, 1)
            wide[END_ROWS - 1 + s] = pltpu.roll(rows[s - 1], LANES - 1, 1)
        return wide

    def choose(rows, count, masks, col):
        return pick(lambda r: lanes_of(rows[r], col), count, masks)

    def both(values):
        return values + [down(x) for x in values]

    for v in ends:
        row, col = place_of(load(MATE + v).astype(jnp.int32))
        mate_row[v], mate_col[v] = row, col
        mass[v] = load(MASS + v)
        name[v] = load(NAME + v)
        slot = name[v].astype(jnp.int32)
        link_row[v], link_col[v] = slot >> 7, slot & 127
    for r in range(CROSS_ROWS):
        row, col = place_of(load(HOST + r).astype(jnp.int32))
        host_row[r], host_col[r] = row, jnp.minimum(col, LANES - 1)
        anchor[r] = jnp.where(col < LANES, 1.0, 0.0)

    for v in ends:
        d = [load(DIFF + END_ROWS * c + v) for c in every]
        g = [time_step * load(VELO + END_ROWS * c + v) for c in every]
        s = load(SCAL + v)
        size = jnp.sqrt(dot3(d, d))
        rate = s / size
        rhs = rate * dot3(d, g)
        length[v], scale[v], now[v], total[v] = size, s, rhs, rhs
        for c in every:
            diff[c, v], drift[c, v], push[c, v], moved[c, v] = d[c], g[c], rate * d[c], zero

    start = []
    for r in right:
        l = r + SLOT_ROWS
        d = [load(CPOS + CROSS_ROWS * c + r) - up(load(CPOS + CROSS_ROWS * c + l)) for c in every]
        g = [
            time_step * (load(CVEL + CROSS_ROWS * c + r) - up(load(CVEL + CROSS_ROWS * c + l))) for c in every
        ]
        edge_mass[r], edge_mass[l] = load(CMAS + r), load(CMAS + l)
        s = 1.0 / jnp.sqrt(edge_mass[r] + up(edge_mass[l]))
        size = jnp.sqrt(dot3(d, d))
        rate = s / size
        edge_length[r], edge_scale[r] = size, s
        start.append(rate * dot3(d, g))
        for c in every:
            edge_diff[c, r], edge_drift[c, r] = d[c], g[c]
            edge[c, r], edge[c, l] = rate * d[c], -down(rate * d[c])
            moved_edge[c, r], moved_edge[c, l] = zero, zero
    for r, x in enumerate(both(start)):
        now_edge[r], total_edge[r] = x, x

    names = around([name[v] for v in ends])
    many = jnp.zeros((8, LANES), jnp.int32)
    fields = [around([push[c, v] for v in ends]) for c in every]
    for v in ends:
        here = [mass[v] * push[c, v] for c in every]
        for s in range(1, NEAR + 1):
            same = names[v] == names[v - s]
            near[s - 1, v] = jnp.where(same, 1.0, 0.0)
            below[s - 1, v] = jnp.where(same, dot3(here, [fields[c][v - s] for c in every]), 0.0)
            above[s - 1, v] = jnp.where(
                names[v] == names[v + s], dot3(here, [fields[c][v + s] for c in every]), 0.0
            )
        past = names[v - 4] if v >= 1 else pltpu.roll(name[END_ROWS - 4], 1, 1)
        many = jnp.where(names[v] == past, 1, many)
        masks = bits_of(link_row[v], CROSS_ROWS)
        linked = link_row[v] < CROSS_ROWS
        across = [choose([edge[c, r] for r in range(CROSS_ROWS)], CROSS_ROWS, masks, link_col[v]) for c in every]
        for c in every:
            ties[c, v] = jnp.where(linked, mass[v] * across[c], 0.0)
        hinge[v] = jnp.where(linked, dot3(here, across), 0.0)
    crowded = jnp.max(many) > 0
    bound = around([hinge[v] for v in ends])
    for v in ends:
        for s in range(1, NEAR + 1):
            hinges[s - 1, v] = jnp.where(near[s - 1, v] > 0.5, bound[v - s], 0.0)

    def gated(factor, value):
        return jnp.where(factor != 0.0, factor * value, 0.0)

    def scan(rows, forward):
        def double(k, carry):
            step = lax.shift_left(1, k)
            turns = step // END_ROWS
            rest = step - turns * END_ROWS

            def one(v, carry):
                source = v - rest if forward else v + rest
                wrap = jnp.where(source < 0, 1, 0) if forward else jnp.where(source >= END_ROWS, 1, 0)
                source = source + wrap * END_ROWS if forward else source - wrap * END_ROWS
                shift = turns + wrap if forward else (LANES - turns - wrap)
                match = name[v] == pltpu.roll(name[source], shift, 1)
                for r in rows:
                    more[r, v] = run[r, v] + jnp.where(match, pltpu.roll(run[r, source], shift, 1), 0.0)
                return carry

            lax.fori_loop(0, END_ROWS, one, 0)

            def keep(v, carry):
                for r in rows:
                    run[r, v] = more[r, v]
                return carry

            return lax.fori_loop(0, END_ROWS, keep, carry)

        lax.fori_loop(0, 12, double, 0)

    def scan_fields(source):
        def fill(v, carry):
            x = source[v]
            for c in every:
                run[c, v] = push[c, v] * x
                run[3 + c, v] = push[c, v] * x
            run[6, v] = gated(hinge[v], x)
            return carry

        lax.fori_loop(0, END_ROWS, fill, 0)
        scan((0, 1, 2, 6), True)
        scan((3, 4, 5), False)

    def at_edges(table):
        got = []
        for r in range(CROSS_ROWS):
            value = choose(table, END_ROWS, bits_of(host_row[r], END_ROWS), host_col[r])
            got.append(value)
        return got

    def apply(slow):
        x = around([now[v] for v in ends])
        crossing = [now_edge[r] for r in range(CROSS_ROWS)]
        if slow:
            scan_fields(now)

            def fill(v, carry):
                here = [push[c, v] for c in every]
                both_sides = [run[c, v] + run[3 + c, v] - 2.0 * here[c] * now[v] for c in every]
                part[0, v] = mass[v] * dot3(here, both_sides)
                part[1, v] = run[6, v]
                return carry

            lax.fori_loop(0, END_ROWS, fill, 0)
        sums, bounds = [], []
        for v in ends:
            if slow:
                sum_x, sum_bound = part[0, v], part[1, v]
            else:
                sum_x, sum_bound = zero, gated(hinge[v], x[v])
                for s in range(1, NEAR + 1):
                    sum_x = sum_x + gated(below[s - 1, v], x[v - s])
                    sum_x = sum_x + gated(above[s - 1, v], x[v + s])
                    sum_bound = sum_bound + gated(hinges[s - 1, v], x[v - s])
            value = choose(crossing, CROSS_ROWS, bits_of(link_row[v], CROSS_ROWS), link_col[v])
            sums.append(sum_x + gated(hinge[v], value))
            bounds.append(sum_bound)
        pulled = at_edges(bounds)
        pulled = [jnp.where(anchor[r] > 0.5, pulled[r], 0.0) for r in range(CROSS_ROWS)]
        for r, value in enumerate(both([-(pulled[r] + up(pulled[r + SLOT_ROWS])) for r in right])):
            now_edge[r] = value
            total_edge[r] = total_edge[r] + value
        for v in ends:
            value = choose(sums, END_ROWS, bits_of(mate_row[v], END_ROWS), mate_col[v])
            value = -(sums[v] + value)
            now[v] = value
            total[v] = total[v] + value

    def edges_moved():
        got = []
        for r in range(CROSS_ROWS):
            masks = bits_of(host_row[r], END_ROWS)
            fast = anchor[r] > 0.5
            got.append(
                [
                    jnp.where(fast, choose([moved[c, v] for v in ends], END_ROWS, masks, host_col[r]), moved_edge[c, r])
                    for c in every
                ]
            )
        return got

    def same(v, s):
        if s < 0:
            return near[-s - 1, v] > 0.5
        if v + s < END_ROWS:
            return near[s - 1, v + s] > 0.5
        return pltpu.roll(near[s - 1, v + s - END_ROWS], LANES - 1, 1) > 0.5

    def move(slow):
        if slow:
            scan_fields(total)

            def fill(v, carry):
                for c in every:
                    run[c, v] = run[c, v] + run[3 + c, v] - push[c, v] * total[v]
                return carry

            lax.fori_loop(0, END_ROWS, fill, 0)
        else:
            x = [total[v] for v in ends]
            for c in every:
                field = around([push[c, v] * x[v] for v in ends])
                for v in ends:
                    value = field[v]
                    for s in range(1, NEAR + 1):
                        value = value + jnp.where(same(v, -s), field[v - s], 0.0)
                        value = value + jnp.where(same(v, s), field[v + s], 0.0)
                    run[c, v] = value
        crossing = [total_edge[r] for r in range(CROSS_ROWS)]
        for v in ends:
            value = choose(crossing, CROSS_ROWS, bits_of(link_row[v], CROSS_ROWS), link_col[v])
            linked = link_row[v] < CROSS_ROWS
            for c in every:
                moved[c, v] = moved[c, v] + mass[v] * run[c, v] + jnp.where(linked, ties[c, v] * value, 0.0)
        for r in range(CROSS_ROWS):
            for c in every:
                moved_edge[c, r] = moved_edge[c, r] + edge_mass[r] * edge[c, r] * crossing[r]

    def correct():
        def rate(d, g, size, s):
            excess = 2.0 * dot3(d, g) + dot3(g, g)
            return s * excess / (size + jnp.sqrt(size * size - excess))

        here = edges_moved()
        start = []
        for r in right:
            g = [edge_drift[c, r] - (here[r][c] - up(here[r + SLOT_ROWS][c])) for c in every]
            start.append(rate([edge_diff[c, r] for c in every], g, edge_length[r], edge_scale[r]))
        for r, value in enumerate(both(start)):
            now_edge[r], total_edge[r] = value, value
        for v in ends:
            masks = bits_of(mate_row[v], END_ROWS)
            there = [choose([moved[c, w] for w in ends], END_ROWS, masks, mate_col[v]) for c in every]
            g = [drift[c, v] - (moved[c, v] - there[c]) for c in every]
            value = rate([diff[c, v] for c in every], g, length[v], scale[v])
            now[v], total[v] = value, value

    def rounds(slow):
        def one(order, carry):
            apply(slow)
            return carry

        def turn(index, carry):
            if slow or not UNROLLED:
                lax.fori_loop(0, ORDER, one, 0)
            else:
                for order in range(ORDER):
                    apply(slow)
            move(slow)

            @pl.when(index < ITER)
            def _():
                correct()

            return carry

        lax.fori_loop(0, ITER + 1, turn, 0)

    @pl.when(crowded)
    def _():
        rounds(True)

    @pl.when(jnp.logical_not(crowded))
    def _():
        rounds(False)

    me = lax.axis_index("dom")
    own = [
        [jnp.broadcast_to(moved[c, v, pl.ds(me, 1), :], (8, LANES)) for v in ends]
        + [jnp.broadcast_to(moved_edge[c, r, pl.ds(me, 1), :], (8, LANES)) for r in range(CROSS_ROWS)]
        for c in every
    ]
    for k in range(2):
        code = place[8 * k : 8 * k + 8, :]
        bound = code >= 0
        code = jnp.maximum(code, 0)
        masks = bits_of(code >> 7, END_ROWS + CROSS_ROWS)
        for c in every:
            shift = choose(own[c], END_ROWS + CROSS_ROWS, masks, code & 127)
            shift = jnp.where(bound, shift, 0.0) / time_step
            for j in range(8):
                cut = slice((8 * k + j) * LANES, (8 * k + j + 1) * LANES)
                out[c : c + 1, cut] = vel[c : c + 1, cut] - shift[j : j + 1, :]


def on_device(
    protein_pos, protein_vel, inv_mass, bond_atoms, left_atoms, right_atoms, water_pos, water_vel
):
    f32, i32 = jnp.float32, jnp.int32
    inputs = (
        bond_atoms,
        right_atoms.reshape(SLOT_ROWS, LANES),
        left_atoms.reshape(SLOT_ROWS, LANES),
        protein_pos,
        protein_vel,
        inv_mass.reshape(ATOM_ROWS, LANES),
        water_pos,
        water_vel,
    )
    inputs = [pltpu.with_memory_space_constraint(x, pltpu.HBM) for x in inputs]
    pay, place, water_velocity = pl.pallas_call(
        prepare,
        in_specs=[pl.BlockSpec(memory_space=pltpu.HBM)] * len(inputs),
        out_shape=(
            jax.ShapeDtypeStruct((ROWS, LANES), f32),
            jax.ShapeDtypeStruct((ATOM_ROWS, LANES), i32),
            jax.ShapeDtypeStruct(water_pos.shape, f32),
        ),
        scratch_shapes=[
            *(pltpu.VMEM(x.shape, x.dtype) for x in inputs),
            pltpu.VMEM((40, LANES), i32),
            pltpu.VMEM((32, LANES), f32),
            pltpu.VMEM((8, LANES), f32),
            pltpu.VMEM((18, 8, LANES), f32),
            pltpu.SemaphoreType.DMA((len(inputs),)),
        ],
        compiler_params=pltpu.CompilerParams(vmem_limit_bytes=8 << 20),
        name="prepare",
    )(*inputs)
    whole = lax.all_gather(pay, "dom", axis=0, tiled=True)

    def rows(*lead, dtype=f32):
        return pltpu.VMEM((*lead, 8, LANES), dtype)

    n, m = END_ROWS, CROSS_ROWS
    protein_velocity = pl.pallas_call(
        solve,
        out_shape=jax.ShapeDtypeStruct(protein_vel.shape, f32),
        scratch_shapes=[
            *(rows(n, dtype=i32) for _ in range(4)),
            *(rows(m, dtype=i32) for _ in range(2)),
            *(rows(n) for _ in range(2)),
            rows(3, n),
            *(rows(n) for _ in range(2)),
            *(rows(3, n) for _ in range(2)),
            *(rows(NEAR, n) for _ in range(3)),
            rows(n),
            rows(NEAR, n),
            rows(3, m),
            *(rows(m) for _ in range(3)),
            *(rows(3, m) for _ in range(2)),
            rows(m),
            *(rows(n) for _ in range(2)),
            *(rows(m) for _ in range(2)),
            rows(2, n),
            *(rows(3, n) for _ in range(2)),
            rows(3, m),
            *(rows(7, n) for _ in range(2)),
        ],
        compiler_params=pltpu.CompilerParams(vmem_limit_bytes=16 << 20),
        name="solve",
    )(whole, place, protein_vel)
    return (protein_velocity, water_velocity)


def solution(mesh):
    in_specs = (
        P(None, ("rep", "dom")),
        P(None, ("rep", "dom")),
        P(("rep", "dom")),
        P(None, ("rep", "dom")),
        P(("rep", "dom")),
        P(("rep", "dom")),
        P(None, ("rep", "dom")),
        P(None, ("rep", "dom")),
    )
    out_specs = (P(None, ("rep", "dom")), P(None, ("rep", "dom")))
    return jax.shard_map(
        on_device, mesh=mesh, in_specs=in_specs, out_specs=out_specs, check_vma=False
    )
```

```python
import functools
import math

import jax
import jax.numpy as jnp
from jax import lax
from jax.experimental import pallas as pl
from jax.experimental.pallas import tpu as pltpu
from jax.sharding import PartitionSpec as P

ORDER = 4
ITER = 2

time_step = 0.002
mass_oxygen = 15.9994
mass_hydrogen = 1.008
oxygen_hydrogen = 0.09572
hydrogen_pair = 0.15139
total_mass = mass_oxygen + 2.0 * mass_hydrogen
half_pair = 0.5 * hydrogen_pair
water_height = math.sqrt(oxygen_hydrogen * oxygen_hydrogen - half_pair * half_pair)
oxygen_reach = 2.0 * mass_hydrogen * water_height / total_mass
hydrogen_reach = water_height - oxygen_reach

LANES = 128
DOMAINS = 8
ATOM_ROWS = 16
BOND_ROWS = 10
SLOT_ROWS = 3
END_ROWS = 2 * BOND_ROWS
HALF = BOND_ROWS * LANES
CROSS_ROWS = 2 * SLOT_ROWS
NEAR = 3
NONE = 4095

DIFF, VELO, SCAL = 0, 3 * END_ROWS, 6 * END_ROWS
MASS, MATE, NAME = (k * END_ROWS for k in (7, 8, 9))
CPOS = 10 * END_ROWS
CVEL, CMAS, HOST = CPOS + 3 * CROSS_ROWS, CPOS + 6 * CROSS_ROWS, CPOS + 7 * CROSS_ROWS
ROWS = -(-(CPOS + 8 * CROSS_ROWS) // 8) * 8


def lanes_of(table, index):
    dims = lax.GatherDimensionNumbers(
        offset_dims=(),
        collapsed_slice_dims=(1,),
        start_index_map=(1,),
        operand_batching_dims=(0,),
        start_indices_batching_dims=(0,),
    )
    return lax.gather(
        table, index[..., None], dims, (1, 1), mode=lax.GatherScatterMode.PROMISE_IN_BOUNDS
    )


def bits_of(row, count):
    return [(row & (1 << b)) != 0 for b in range(max(1, (count - 1).bit_length()))]


def pick(get, count, masks, low=0):
    if count == 1:
        return get(low)
    bit = (count - 1).bit_length() - 1
    half = 1 << bit
    left = pick(get, half, masks, low)
    right = pick(get, count - half, masks, low + half)
    return jnp.where(masks[bit], right, left)


def gather_rows(table, count, row, lane):
    masks = bits_of(row, count)
    return pick(lambda r: lanes_of(table(r), lane), count, masks)


def spread(ref, r):
    return jnp.broadcast_to(ref[r : r + 1, :], (8, LANES))


def place_of(position):
    lane = (position * 3277) >> 16
    return position - lane * END_ROWS, lane


def cross3(a, b):
    return [a[1] * b[2] - a[2] * b[1], a[2] * b[0] - a[0] * b[2], a[0] * b[1] - a[1] * b[0]]


def dot3(a, b):
    return a[0] * b[0] + a[1] * b[1] + a[2] * b[2]


def settle(before, after):
    old_o, old_1, old_2 = before[0:3], before[3:6], before[6:9]
    new_o, new_1, new_2 = after[0:3], after[3:6], after[6:9]
    every = range(3)
    center = [(mass_oxygen * new_o[c] + mass_hydrogen * (new_1[c] + new_2[c])) / total_mass for c in every]
    old_b = [old_1[c] - old_o[c] for c in every]
    old_c = [old_2[c] - old_o[c] for c in every]
    rel_a = [new_o[c] - center[c] for c in every]
    rel_b = [new_1[c] - center[c] for c in every]
    rel_c = [new_2[c] - center[c] for c in every]
    normal = cross3(old_b, old_c)
    side = cross3(rel_a, normal)
    upward = cross3(normal, side)

    def normed(v):
        size = jnp.sqrt(dot3(v, v))
        return [part / size for part in v]

    axis_z, axis_x, axis_y = normed(normal), normed(side), normed(upward)
    oldb_x, oldb_y = dot3(axis_x, old_b), dot3(axis_y, old_b)
    oldc_x, oldc_y = dot3(axis_x, old_c), dot3(axis_y, old_c)
    newa_z = dot3(axis_z, rel_a)
    newb_x, newb_y, newb_z = dot3(axis_x, rel_b), dot3(axis_y, rel_b), dot3(axis_z, rel_b)
    newc_x, newc_y, newc_z = dot3(axis_x, rel_c), dot3(axis_y, rel_c), dot3(axis_z, rel_c)
    sin_phi = newa_z / oxygen_reach
    cos_phi = jnp.sqrt(1.0 - sin_phi * sin_phi)
    sin_psi = (newb_z - newc_z) / (2.0 * half_pair * cos_phi)
    cos_psi = jnp.sqrt(1.0 - sin_psi * sin_psi)
    rest_ay = oxygen_reach * cos_phi
    rest_bx = -half_pair * cos_psi
    lowered = -hydrogen_reach * cos_phi
    tilted = half_pair * sin_psi * sin_phi
    rest_by = lowered - tilted
    rest_cy = lowered + tilted
    alpha = rest_bx * (oldb_x - oldc_x) + oldb_y * rest_by + oldc_y * rest_cy
    beta = rest_bx * (oldc_y - oldb_y) + oldb_x * rest_by + oldc_x * rest_cy
    gamma = oldb_x * newb_y - newb_x * oldb_y + oldc_x * newc_y - newc_x * oldc_y
    summed = alpha * alpha + beta * beta
    sin_theta = (alpha * gamma - beta * jnp.sqrt(summed - gamma * gamma)) / summed
    cos_theta = jnp.sqrt(1.0 - sin_theta * sin_theta)
    final_ax = -rest_ay * sin_theta
    final_ay = rest_ay * cos_theta
    final_bx = rest_bx * cos_theta - rest_by * sin_theta
    final_by = rest_bx * sin_theta + rest_by * cos_theta
    final_cx = -rest_bx * cos_theta - rest_cy * sin_theta
    final_cy = -rest_bx * sin_theta + rest_cy * cos_theta
    oxygen = [center[c] + axis_x[c] * final_ax + axis_y[c] * final_ay + axis_z[c] * newa_z for c in every]
    first = [center[c] + axis_x[c] * final_bx + axis_y[c] * final_by + axis_z[c] * newb_z for c in every]
    second = [center[c] + axis_x[c] * final_cx + axis_y[c] * final_cy + axis_z[c] * newc_z for c in every]
    return oxygen + first + second


def sort_keys(keys):
    lane = lax.broadcasted_iota(jnp.int32, (8, LANES), 1)
    sub = lax.broadcasted_iota(jnp.int32, (8, LANES), 0)
    reg_bits = (len(keys) - 1).bit_length()
    bits = reg_bits + 10
    base = (lane * 8 + sub) << reg_bits

    def ordered(bit, size, here, there):
        turned = base >> bit if size == bits else (base >> bit) ^ (base >> size)
        return jnp.where((turned & 1) == 0, jnp.minimum(here, there), jnp.maximum(here, there))

    def registers(keys, bit, size):
        out = list(keys)
        for reg in range(len(keys)):
            if reg & (1 << bit):
                continue
            other = reg | (1 << bit)
            low = jnp.minimum(keys[reg], keys[other])
            high = jnp.maximum(keys[reg], keys[other])
            if size == bits:
                out[reg], out[other] = low, high
            elif size < reg_bits:
                out[reg], out[other] = (high, low) if reg & (1 << size) else (low, high)
            else:
                rising = ((base >> size) & 1) == 0
                out[reg] = jnp.where(rising, low, high)
                out[other] = jnp.where(rising, high, low)
        return out

    def sublanes(key, bit, size):
        step = 1 << (bit - reg_bits)
        if step == 4:
            mate = pltpu.roll(key, 4, 0)
        else:
            mate = jnp.where((sub & step) != 0, pltpu.roll(key, step, 0), pltpu.roll(key, 8 - step, 0))
        return ordered(bit, size, key, mate)

    def lanes(key, group, size):
        steps = [1 << (bit - reg_bits - 3) for bit in group]
        reach = [0]
        for step in steps:
            reach = reach + [far ^ step for far in reach]
        values = {far: lanes_of(key, lane ^ far) if far else key for far in reach}
        for bit, step in zip(group, steps):
            values = {
                far: ordered(bit, size, values[far], values[far ^ step])
                for far in values
                if far < step
            }
        return values[0]

    for size in range(1, bits + 1):
        crossing = [bit for bit in range(size - 1, reg_bits + 2, -1)]
        while crossing:
            width = {4: 2, 2: 2, 1: 1}.get(len(crossing), 3)
            group, crossing = crossing[:width], crossing[width:]
            keys = [lanes(key, group, size) for key in keys]
        for bit in range(min(size - 1, reg_bits + 2), -1, -1):
            if bit < reg_bits:
                keys = registers(keys, bit, size)
            else:
                keys = [sublanes(key, bit, size) for key in keys]
    return keys


def find(table, rows, queries):
    heads = table[0:1, :]
    marks = [jnp.broadcast_to(heads[:, 8 * i : 8 * i + 1], (8, LANES)) for i in range(1, 16)]
    wide = jnp.broadcast_to(heads, (8, LANES))
    found = []
    for query in queries:
        group = jnp.zeros((8, LANES), jnp.int32)
        for mark in marks:
            group = group + jnp.where(mark < query, 8, 0)
        column = group
        for i in range(1, 8):
            column = column + jnp.where(lanes_of(wide, group + i) < query, 1, 0)
        rank = column * rows
        best = jnp.full((8, LANES), -1.0, jnp.float32)
        for r in range(rows):
            key = lanes_of(spread(table, r), column)
            below = key < query
            rank = rank + jnp.where(below, 1, 0)
            best = jnp.maximum(best, jnp.where(below, key, -1.0))
        found.append((rank, best.astype(jnp.int32)))
    return found


def prepare(
    bonds_in, right_in, left_in, pos_in, vel_in, mass_in, pay, place,
    bonds, right, left, pos, vel, mass, atoms, ranked, slots, arrived,
):
    lane = lax.broadcasted_iota(jnp.int32, (8, LANES), 1)
    sub = lax.broadcasted_iota(jnp.int32, (8, LANES), 0)
    f32, i32 = jnp.float32, jnp.int32

    sources = (bonds_in, right_in, left_in, pos_in, vel_in, mass_in)
    targets = (bonds, right, left, pos, vel, mass)
    copies = [
        pltpu.make_async_copy(source, target, arrived.at[k])
        for k, (source, target) in enumerate(zip(sources, targets))
    ]
    for copy in copies:
        copy.start()
    for copy in copies:
        copy.wait()

    def index(k):
        return (k * 8 + sub) * LANES + lane

    for r in range(BOND_ROWS):
        cut = slice(r * LANES, (r + 1) * LANES)
        atoms[r : r + 1, :] = bonds[0:1, cut]
        atoms[BOND_ROWS + r : BOND_ROWS + r + 1, :] = bonds[1:2, cut]
    atoms[END_ROWS:32, :] = jnp.full((32 - END_ROWS, LANES), 2048, i32)
    atoms[32 : 32 + SLOT_ROWS, :] = right[...]
    atoms[32 + SLOT_ROWS : 32 + CROSS_ROWS, :] = left[...]
    atoms[32 + CROSS_ROWS : 40, :] = jnp.full((8 - CROSS_ROWS, LANES), 4096, i32)
    crossed = atoms[32:40, :]

    keys = [(atoms[8 * k : 8 * k + 8, :] * 4096 + index(k)).astype(f32) for k in range(4)]
    keys = sort_keys(keys)
    for k in range(4):
        ranked[pl.ds(k, 8, stride=4), :] = keys[k]
    slots[...] = sort_keys([(crossed * 1024 + index(0)).astype(f32)])[0]

    own, far, mates = [], [], []
    quads = []
    for j in range(8):
        quad = ranked[4 * j : 4 * j + 4, :]
        quads.append(jnp.concatenate([quad, quad], axis=0))
    for k in range(3):
        rank = lane * END_ROWS + k * 8 + sub
        masks = bits_of((rank >> 2) & 7, 8)
        key = pick(lambda j: lanes_of(quads[j], rank >> 5), 8, masks).astype(i32)
        end = key & 4095
        mate = jnp.where(end < HALF, end + HALF, end - HALF)
        other = gather_rows(functools.partial(spread, atoms), END_ROWS, mate >> 7, mate & 127)
        own.append(jnp.minimum(key >> 12, 2047))
        far.append(jnp.minimum(other, 2047))
        mates.append((other * 4096 + mate).astype(f32))

    def put(block, k, value):
        count = min(8, END_ROWS - 8 * k)
        pay[block + 8 * k : block + 8 * k + count, :] = value[:count].astype(f32)

    inside = find(
        ranked,
        32,
        mates + [((crossed + 1) * 4096).astype(f32)] + [((index(k) + 1) * 4096).astype(f32) for k in range(2)],
    )
    outside = find(
        slots, 8, [((a + 1) * 1024).astype(f32) for a in own] + [((index(k) + 1) * 1024).astype(f32) for k in range(2)]
    )
    for k in range(3):
        put(MATE, k, inside[k][0])
        best = outside[k][1]
        put(NAME, k, jnp.where(best >> 10 == own[k], best & 1023, own[k] + 1024))
    rank, best = inside[3]
    host = jnp.where(best >> 12 == crossed, rank - 1, NONE)
    pay[HOST : HOST + CROSS_ROWS, :] = host[:CROSS_ROWS].astype(f32)
    for k in range(2):
        rank, best = inside[4 + k]
        slot = outside[3 + k][1]
        row, col = place_of(rank - 1)
        place[8 * k : 8 * k + 8, :] = jnp.where(
            best >> 12 == index(k),
            row * LANES + col,
            jnp.where(slot >> 10 == index(k), END_ROWS * LANES + (slot & 1023), -1),
        )

    edge = jnp.minimum(crossed, 2047)
    where = [(a >> 7, a & 127) for a in own + far + [edge]]

    def at_ends(table):
        return [gather_rows(table, ATOM_ROWS, row, col) for row, col in where]

    for block, cross, source in ((DIFF, CPOS, pos), (VELO, CVEL, vel)):
        for c in range(3):
            values = at_ends(
                lambda r: jnp.broadcast_to(source[c : c + 1, r * LANES : (r + 1) * LANES], (8, LANES))
            )
            for k in range(3):
                put(block + END_ROWS * c, k, values[k] - values[3 + k])
            pay[cross + CROSS_ROWS * c : cross + CROSS_ROWS * (c + 1), :] = values[6][:CROSS_ROWS]
    values = at_ends(functools.partial(spread, mass))
    for k in range(3):
        put(MASS, k, values[k])
        put(SCAL, k, 1.0 / jnp.sqrt(values[k] + values[3 + k]))
    pay[CMAS : CMAS + CROSS_ROWS, :] = values[6][:CROSS_ROWS]


def solve(
    whole, place, vel, water_pos, water_vel, out, water_home,
    mate_row, mate_col, link_row, link_col, host_row, host_col, name, mass, push, length, scale, diff, drift,
    below, above, near, hinge, hinges, edge, edge_mass, edge_length, edge_scale, edge_diff, edge_drift, anchor,
    now, total, now_edge, total_edge, part, ties, moved, moved_edge, run, more, mine, index, shown,
    wet, water_out, leaving,
):
    zero = jnp.zeros((8, LANES), jnp.float32)
    every, ends, right = range(3), range(END_ROWS), range(SLOT_ROWS)

    def load(r):
        return whole[pl.ds(r, DOMAINS, stride=ROWS), :]

    def up(x):
        return pltpu.roll(x, DOMAINS - 1, 0)

    def down(x):
        return pltpu.roll(x, 1, 0)

    def around(rows):
        wide = {v: rows[v] for v in ends}
        for s in range(1, NEAR + 1):
            wide[-s] = pltpu.roll(rows[END_ROWS - s], 1, 1)
            wide[END_ROWS - 1 + s] = pltpu.roll(rows[s - 1], LANES - 1, 1)
        return wide

    def choose(rows, count, masks, col):
        return pick(lambda r: lanes_of(rows[r], col), count, masks)

    def both(values):
        return values + [down(x) for x in values]

    for j in range(8):
        cut = slice(j * LANES, (j + 1) * LANES)
        for c in range(9):
            wet[c, j : j + 1, :] = water_pos[c : c + 1, cut]
            wet[9 + c, j : j + 1, :] = water_vel[c : c + 1, cut]
    here = [wet[c] for c in range(9)]
    speed = [wet[9 + c] for c in range(9)]
    there = [here[c] + time_step * speed[c] for c in range(9)]
    settled = settle(here, there)
    for c in range(9):
        result = speed[c] + (settled[c] - there[c]) / time_step
        for j in range(8):
            water_out[c : c + 1, j * LANES : (j + 1) * LANES] = result[j : j + 1, :]
    drained = pltpu.make_async_copy(water_out, water_home, leaving)
    drained.start()

    for v in ends:
        row, col = place_of(load(MATE + v).astype(jnp.int32))
        mate_row[v], mate_col[v] = row, col
        mass[v] = load(MASS + v)
        name[v] = load(NAME + v)
        slot = name[v].astype(jnp.int32)
        link_row[v], link_col[v] = slot >> 7, slot & 127
    for r in range(CROSS_ROWS):
        row, col = place_of(load(HOST + r).astype(jnp.int32))
        host_row[r], host_col[r] = row, jnp.minimum(col, LANES - 1)
        anchor[r] = jnp.where(col < LANES, 1.0, 0.0)

    for v in ends:
        d = [load(DIFF + END_ROWS * c + v) for c in every]
        g = [time_step * load(VELO + END_ROWS * c + v) for c in every]
        s = load(SCAL + v)
        size = jnp.sqrt(dot3(d, d))
        rate = s / size
        rhs = rate * dot3(d, g)
        length[v], scale[v], now[v], total[v] = size, s, rhs, rhs
        for c in every:
            diff[c, v], drift[c, v], push[c, v], moved[c, v] = d[c], g[c], rate * d[c], zero

    start = []
    for r in right:
        l = r + SLOT_ROWS
        d = [load(CPOS + CROSS_ROWS * c + r) - up(load(CPOS + CROSS_ROWS * c + l)) for c in every]
        g = [
            time_step * (load(CVEL + CROSS_ROWS * c + r) - up(load(CVEL + CROSS_ROWS * c + l))) for c in every
        ]
        edge_mass[r], edge_mass[l] = load(CMAS + r), load(CMAS + l)
        s = 1.0 / jnp.sqrt(edge_mass[r] + up(edge_mass[l]))
        size = jnp.sqrt(dot3(d, d))
        rate = s / size
        edge_length[r], edge_scale[r] = size, s
        start.append(rate * dot3(d, g))
        for c in every:
            edge_diff[c, r], edge_drift[c, r] = d[c], g[c]
            edge[c, r], edge[c, l] = rate * d[c], -down(rate * d[c])
            moved_edge[c, r], moved_edge[c, l] = zero, zero
    for r, x in enumerate(both(start)):
        now_edge[r], total_edge[r] = x, x

    names = around([name[v] for v in ends])
    many = jnp.zeros((8, LANES), jnp.int32)
    fields = [around([push[c, v] for v in ends]) for c in every]
    for v in ends:
        here = [mass[v] * push[c, v] for c in every]
        for s in range(1, NEAR + 1):
            same = names[v] == names[v - s]
            near[s - 1, v] = jnp.where(same, 1.0, 0.0)
            below[s - 1, v] = jnp.where(same, dot3(here, [fields[c][v - s] for c in every]), 0.0)
            above[s - 1, v] = jnp.where(
                names[v] == names[v + s], dot3(here, [fields[c][v + s] for c in every]), 0.0
            )
        past = names[v - 4] if v >= 1 else pltpu.roll(name[END_ROWS - 4], 1, 1)
        many = jnp.where(names[v] == past, 1, many)
        masks = bits_of(link_row[v], CROSS_ROWS)
        linked = link_row[v] < CROSS_ROWS
        across = [choose([edge[c, r] for r in range(CROSS_ROWS)], CROSS_ROWS, masks, link_col[v]) for c in every]
        for c in every:
            ties[c, v] = jnp.where(linked, mass[v] * across[c], 0.0)
        hinge[v] = jnp.where(linked, dot3(here, across), 0.0)
    crowded = jnp.max(many) > 0
    bound = around([hinge[v] for v in ends])
    for v in ends:
        for s in range(1, NEAR + 1):
            hinges[s - 1, v] = jnp.where(near[s - 1, v] > 0.5, bound[v - s], 0.0)

    def gated(factor, value):
        return jnp.where(factor != 0.0, factor * value, 0.0)

    def scan(rows, forward):
        def double(k, carry):
            step = lax.shift_left(1, k)
            turns = step // END_ROWS
            rest = step - turns * END_ROWS

            def one(v, carry):
                source = v - rest if forward else v + rest
                wrap = jnp.where(source < 0, 1, 0) if forward else jnp.where(source >= END_ROWS, 1, 0)
                source = source + wrap * END_ROWS if forward else source - wrap * END_ROWS
                shift = turns + wrap if forward else (LANES - turns - wrap)
                match = name[v] == pltpu.roll(name[source], shift, 1)
                for r in rows:
                    more[r, v] = run[r, v] + jnp.where(match, pltpu.roll(run[r, source], shift, 1), 0.0)
                return carry

            lax.fori_loop(0, END_ROWS, one, 0)

            def keep(v, carry):
                for r in rows:
                    run[r, v] = more[r, v]
                return carry

            return lax.fori_loop(0, END_ROWS, keep, carry)

        lax.fori_loop(0, 12, double, 0)

    def scan_fields(source):
        def fill(v, carry):
            x = source[v]
            for c in every:
                run[c, v] = push[c, v] * x
                run[3 + c, v] = push[c, v] * x
            run[6, v] = gated(hinge[v], x)
            return carry

        lax.fori_loop(0, END_ROWS, fill, 0)
        scan((0, 1, 2, 6), True)
        scan((3, 4, 5), False)

    def at_edges(table):
        got = []
        for r in range(CROSS_ROWS):
            value = choose(table, END_ROWS, bits_of(host_row[r], END_ROWS), host_col[r])
            got.append(value)
        return got

    def apply(slow, last=False):
        x = around([now[v] for v in ends])
        crossing = [now_edge[r] for r in range(CROSS_ROWS)]
        if slow:
            scan_fields(now)

            def fill(v, carry):
                here = [push[c, v] for c in every]
                both_sides = [run[c, v] + run[3 + c, v] - 2.0 * here[c] * now[v] for c in every]
                part[0, v] = mass[v] * dot3(here, both_sides)
                part[1, v] = run[6, v]
                return carry

            lax.fori_loop(0, END_ROWS, fill, 0)
        sums, bounds = [], []
        for v in ends:
            if slow:
                sum_x, sum_bound = part[0, v], part[1, v]
            else:
                sum_x, sum_bound = zero, gated(hinge[v], x[v])
                for s in range(1, NEAR + 1):
                    sum_x = sum_x + gated(below[s - 1, v], x[v - s])
                    sum_x = sum_x + gated(above[s - 1, v], x[v + s])
                    sum_bound = sum_bound + gated(hinges[s - 1, v], x[v - s])
            value = choose(crossing, CROSS_ROWS, bits_of(link_row[v], CROSS_ROWS), link_col[v])
            sums.append(sum_x + gated(hinge[v], value))
            bounds.append(sum_bound)
        pulled = at_edges(bounds)
        pulled = [jnp.where(anchor[r] > 0.5, pulled[r], 0.0) for r in range(CROSS_ROWS)]
        for r, value in enumerate(both([-(pulled[r] + up(pulled[r + SLOT_ROWS])) for r in right])):
            now_edge[r] = value
            total_edge[r] = total_edge[r] + value
        if last:
            for v in ends:
                part[0, v] = sums[v]
            return
        for v in ends:
            value = choose(sums, END_ROWS, bits_of(mate_row[v], END_ROWS), mate_col[v])
            value = -(sums[v] + value)
            now[v] = value
            total[v] = total[v] + value

    def edges_moved():
        got = []
        for r in range(CROSS_ROWS):
            masks = bits_of(host_row[r], END_ROWS)
            fast = anchor[r] > 0.5
            got.append(
                [
                    jnp.where(fast, choose([moved[c, v] for v in ends], END_ROWS, masks, host_col[r]), moved_edge[c, r])
                    for c in every
                ]
            )
        return got

    def same(v, s):
        if s < 0:
            return near[-s - 1, v] > 0.5
        if v + s < END_ROWS:
            return near[s - 1, v + s] > 0.5
        return pltpu.roll(near[s - 1, v + s - END_ROWS], LANES - 1, 1) > 0.5

    def move(slow):
        if slow:
            scan_fields(total)

            def fill(v, carry):
                for c in every:
                    run[c, v] = run[c, v] + run[3 + c, v] - push[c, v] * total[v]
                return carry

            lax.fori_loop(0, END_ROWS, fill, 0)
        else:
            x = [total[v] for v in ends]
            for c in every:
                field = around([push[c, v] * x[v] for v in ends])
                for v in ends:
                    value = field[v]
                    for s in range(1, NEAR + 1):
                        value = value + jnp.where(same(v, -s), field[v - s], 0.0)
                        value = value + jnp.where(same(v, s), field[v + s], 0.0)
                    run[c, v] = value
        crossing = [total_edge[r] for r in range(CROSS_ROWS)]
        for v in ends:
            value = choose(crossing, CROSS_ROWS, bits_of(link_row[v], CROSS_ROWS), link_col[v])
            linked = link_row[v] < CROSS_ROWS
            for c in every:
                moved[c, v] = moved[c, v] + mass[v] * run[c, v] + jnp.where(linked, ties[c, v] * value, 0.0)
        edge_sums()

    def correct():
        def rate(d, g, size, s):
            excess = 2.0 * dot3(d, g) + dot3(g, g)
            return s * excess / (size + jnp.sqrt(size * size - excess))

        here = edges_moved()
        start = []
        for r in right:
            g = [edge_drift[c, r] - (here[r][c] - up(here[r + SLOT_ROWS][c])) for c in every]
            start.append(rate([edge_diff[c, r] for c in every], g, edge_length[r], edge_scale[r]))
        for r, value in enumerate(both(start)):
            now_edge[r], total_edge[r] = value, value
        for v in ends:
            masks = bits_of(mate_row[v], END_ROWS)
            there = [choose([moved[c, w] for w in ends], END_ROWS, masks, mate_col[v]) for c in every]
            g = [drift[c, v] - (moved[c, v] - there[c]) for c in every]
            value = rate([diff[c, v] for c in every], g, length[v], scale[v])
            now[v], total[v] = value, value

    me = lax.axis_index("dom")
    bands = range(3)

    def take(target, place, source):
        for v in ends:
            target[place, v : v + 1, :] = source(v)[pl.ds(me, 1), :]

    def band(ref, place, k):
        return ref[place, 8 * k : 8 * k + 8, :]

    def spots(place, k):
        return band(index, place, k) & (LANES - 1)

    def show(place, values):
        for k in bands:
            shown[place, 4 + 8 * k : min(12 + 8 * k, 24), :] = values[k][: min(8, END_ROWS - 8 * k)]
        shown[place, 0:4, :] = pltpu.roll(values[2], 1, 1)[0:4]
        shown[place, 24:28, :] = pltpu.roll(values[0], LANES - 1, 1)[0:4]

    def shifted(place, k, step):
        return shown[place, 4 + 8 * k + step : 12 + 8 * k + step, :]

    def edge_sums():
        for r in range(CROSS_ROWS):
            for c in every:
                moved_edge[c, r] = moved_edge[c, r] + edge_mass[r] * edge[c, r] * total_edge[r]

    def finish():
        take(mine, 3, lambda v: part.at[0, v])
        take(mine, 4, lambda v: total.at[v])
        for c in every:
            take(mine, c, lambda v: moved.at[c, v])
        crossing = [jnp.broadcast_to(total_edge[r, pl.ds(me, 1), :], (8, LANES)) for r in range(CROSS_ROWS)]
        x, links = [], []
        for k in bands:
            masks = bits_of(band(index, 0, k), END_ROWS)
            value = pick(
                lambda r: lanes_of(jnp.broadcast_to(mine[3, r : r + 1, :], (8, LANES)), spots(1, k)),
                END_ROWS,
                masks,
            )
            x.append(band(mine, 4, k) - (band(mine, 3, k) + value))
            masks = bits_of(band(index, 2, k), CROSS_ROWS)
            links.append(choose(crossing, CROSS_ROWS, masks, spots(3, k)))
        show(3, [band(mine, 5, k) for k in bands])
        for c in every:
            show(c, [band(mine, 6 + c, k) * x[k] for k in bands])
        for k in bands:
            linked = band(index, 2, k) < CROSS_ROWS
            value = [shifted(c, k, 0) for c in every]
            for step in (-3, -2, -1, 1, 2, 3):
                same = shifted(3, k, step) == band(mine, 5, k)
                value = [value[c] + jnp.where(same, shifted(c, k, step), 0.0) for c in every]
            for c in every:
                mine[c, 8 * k : 8 * k + 8, :] = (
                    band(mine, c, k)
                    + band(mine, 12, k) * value[c]
                    + jnp.where(linked, band(mine, 9 + c, k) * links[k], 0.0)
                )

    def rounds(slow):
        if slow:

            def one(order, carry):
                apply(True)
                return carry

            def turn(turns, carry):
                lax.fori_loop(0, ORDER, one, 0)
                move(True)

                @pl.when(turns < ITER)
                def _():
                    correct()

                return carry

            lax.fori_loop(0, ITER + 1, turn, 0)
            for c in every:
                take(mine, c, lambda v: moved.at[c, v])
            return

        take(mine, 5, lambda v: name.at[v])
        take(mine, 12, lambda v: mass.at[v])
        for c in every:
            take(mine, 6 + c, lambda v: push.at[c, v])
            take(mine, 9 + c, lambda v: ties.at[c, v])
        for place_in, source in enumerate((mate_row, mate_col, link_row, link_col)):
            take(index, place_in, lambda v: source.at[v])

        def turn(turns, carry):
            for order in range(ORDER):
                apply(False)
            move(False)
            correct()
            return carry

        lax.fori_loop(0, ITER, turn, 0)
        for order in range(ORDER):
            apply(False, order == ORDER - 1)
        edge_sums()
        finish()

    @pl.when(crowded)
    def _():
        rounds(True)

    @pl.when(jnp.logical_not(crowded))
    def _():
        rounds(False)

    own = [
        [jnp.broadcast_to(mine[c, v : v + 1, :], (8, LANES)) for v in ends]
        + [jnp.broadcast_to(moved_edge[c, r, pl.ds(me, 1), :], (8, LANES)) for r in range(CROSS_ROWS)]
        for c in every
    ]
    for k in range(2):
        code = place[8 * k : 8 * k + 8, :]
        bound = code >= 0
        code = jnp.maximum(code, 0)
        masks = bits_of(code >> 7, END_ROWS + CROSS_ROWS)
        for c in every:
            shift = choose(own[c], END_ROWS + CROSS_ROWS, masks, code & 127)
            shift = jnp.where(bound, shift, 0.0) / time_step
            for j in range(8):
                cut = slice((8 * k + j) * LANES, (8 * k + j + 1) * LANES)
                out[c : c + 1, cut] = vel[c : c + 1, cut] - shift[j : j + 1, :]
    drained.wait()


def on_device(
    protein_pos, protein_vel, inv_mass, bond_atoms, left_atoms, right_atoms, water_pos, water_vel
):
    f32, i32 = jnp.float32, jnp.int32
    inputs = (
        bond_atoms,
        right_atoms.reshape(SLOT_ROWS, LANES),
        left_atoms.reshape(SLOT_ROWS, LANES),
        protein_pos,
        protein_vel,
        inv_mass.reshape(ATOM_ROWS, LANES),
    )
    inputs = [pltpu.with_memory_space_constraint(x, pltpu.HBM) for x in inputs]
    pay, place = pl.pallas_call(
        prepare,
        in_specs=[pl.BlockSpec(memory_space=pltpu.HBM)] * len(inputs),
        out_shape=(
            jax.ShapeDtypeStruct((ROWS, LANES), f32),
            jax.ShapeDtypeStruct((ATOM_ROWS, LANES), i32),
        ),
        scratch_shapes=[
            *(pltpu.VMEM(x.shape, x.dtype) for x in inputs),
            pltpu.VMEM((40, LANES), i32),
            pltpu.VMEM((32, LANES), f32),
            pltpu.VMEM((8, LANES), f32),
            pltpu.SemaphoreType.DMA((len(inputs),)),
        ],
        compiler_params=pltpu.CompilerParams(vmem_limit_bytes=8 << 20),
        name="prepare",
    )(*inputs)
    whole = lax.all_gather(pay, "dom", axis=0, tiled=True)

    def rows(*lead, dtype=f32):
        return pltpu.VMEM((*lead, 8, LANES), dtype)

    n, m = END_ROWS, CROSS_ROWS
    return pl.pallas_call(
        solve,
        out_specs=(pl.BlockSpec(memory_space=pltpu.VMEM), pl.BlockSpec(memory_space=pltpu.HBM)),
        out_shape=(
            jax.ShapeDtypeStruct(protein_vel.shape, f32),
            jax.ShapeDtypeStruct(water_pos.shape, f32),
        ),
        scratch_shapes=[
            *(rows(n, dtype=i32) for _ in range(4)),
            *(rows(m, dtype=i32) for _ in range(2)),
            *(rows(n) for _ in range(2)),
            rows(3, n),
            *(rows(n) for _ in range(2)),
            *(rows(3, n) for _ in range(2)),
            *(rows(NEAR, n) for _ in range(3)),
            rows(n),
            rows(NEAR, n),
            rows(3, m),
            *(rows(m) for _ in range(3)),
            *(rows(3, m) for _ in range(2)),
            rows(m),
            *(rows(n) for _ in range(2)),
            *(rows(m) for _ in range(2)),
            rows(2, n),
            *(rows(3, n) for _ in range(2)),
            rows(3, m),
            *(rows(7, n) for _ in range(2)),
            pltpu.VMEM((14, 24, LANES), f32),
            pltpu.VMEM((4, 24, LANES), i32),
            pltpu.VMEM((4, 32, LANES), f32),
            pltpu.VMEM((18, 8, LANES), f32),
            pltpu.VMEM(water_pos.shape, f32),
            pltpu.SemaphoreType.DMA,
        ],
        compiler_params=pltpu.CompilerParams(vmem_limit_bytes=16 << 20),
        name="solve",
    )(whole, place, protein_vel, water_pos, water_vel)


def solution(mesh):
    in_specs = (
        P(None, ("rep", "dom")),
        P(None, ("rep", "dom")),
        P(("rep", "dom")),
        P(None, ("rep", "dom")),
        P(("rep", "dom")),
        P(("rep", "dom")),
        P(None, ("rep", "dom")),
        P(None, ("rep", "dom")),
    )
    out_specs = (P(None, ("rep", "dom")), P(None, ("rep", "dom")))
    return jax.shard_map(
        on_device, mesh=mesh, in_specs=in_specs, out_specs=out_specs, check_vma=False
    )
```

```python
import functools
import math

import jax
import jax.numpy as jnp
from jax import lax
from jax.experimental import pallas as pl
from jax.experimental.pallas import tpu as pltpu
from jax.sharding import PartitionSpec as P

ORDER = 4
ITER = 2

time_step = 0.002
mass_oxygen = 15.9994
mass_hydrogen = 1.008
oxygen_hydrogen = 0.09572
hydrogen_pair = 0.15139
total_mass = mass_oxygen + 2.0 * mass_hydrogen
half_pair = 0.5 * hydrogen_pair
water_height = math.sqrt(oxygen_hydrogen * oxygen_hydrogen - half_pair * half_pair)
oxygen_reach = 2.0 * mass_hydrogen * water_height / total_mass
hydrogen_reach = water_height - oxygen_reach

LANES = 128
DOMAINS = 8
ATOM_ROWS = 16
BOND_ROWS = 10
SLOT_ROWS = 3
END_ROWS = 2 * BOND_ROWS
HALF = BOND_ROWS * LANES
CROSS_ROWS = 2 * SLOT_ROWS
NEAR = 3
NONE = 4095

DIFF, VELO, SCAL = 0, 3 * END_ROWS, 6 * END_ROWS
MASS, MATE, NAME = (k * END_ROWS for k in (7, 8, 9))
CPOS = 10 * END_ROWS
CVEL, CMAS, HOST = CPOS + 3 * CROSS_ROWS, CPOS + 6 * CROSS_ROWS, CPOS + 7 * CROSS_ROWS
ROWS = -(-(CPOS + 8 * CROSS_ROWS) // 8) * 8


def lanes_of(table, index):
    dims = lax.GatherDimensionNumbers(
        offset_dims=(),
        collapsed_slice_dims=(1,),
        start_index_map=(1,),
        operand_batching_dims=(0,),
        start_indices_batching_dims=(0,),
    )
    return lax.gather(
        table, index[..., None], dims, (1, 1), mode=lax.GatherScatterMode.PROMISE_IN_BOUNDS
    )


def bits_of(row, count):
    return [(row & (1 << b)) != 0 for b in range(max(1, (count - 1).bit_length()))]


def pick(get, count, masks, low=0):
    if count == 1:
        return get(low)
    bit = (count - 1).bit_length() - 1
    half = 1 << bit
    left = pick(get, half, masks, low)
    right = pick(get, count - half, masks, low + half)
    return jnp.where(masks[bit], right, left)


def gather_rows(table, count, row, lane):
    masks = bits_of(row, count)
    return pick(lambda r: lanes_of(table(r), lane), count, masks)


def spread(ref, r):
    return jnp.broadcast_to(ref[r : r + 1, :], (8, LANES))


def place_of(position):
    lane = (position * 3277) >> 16
    return position - lane * END_ROWS, lane


def cross3(a, b):
    return [a[1] * b[2] - a[2] * b[1], a[2] * b[0] - a[0] * b[2], a[0] * b[1] - a[1] * b[0]]


def dot3(a, b):
    return a[0] * b[0] + a[1] * b[1] + a[2] * b[2]


def settle(before, after):
    old_o, old_1, old_2 = before[0:3], before[3:6], before[6:9]
    new_o, new_1, new_2 = after[0:3], after[3:6], after[6:9]
    every = range(3)
    center = [(mass_oxygen * new_o[c] + mass_hydrogen * (new_1[c] + new_2[c])) / total_mass for c in every]
    old_b = [old_1[c] - old_o[c] for c in every]
    old_c = [old_2[c] - old_o[c] for c in every]
    rel_a = [new_o[c] - center[c] for c in every]
    rel_b = [new_1[c] - center[c] for c in every]
    rel_c = [new_2[c] - center[c] for c in every]
    normal = cross3(old_b, old_c)
    side = cross3(rel_a, normal)
    upward = cross3(normal, side)

    def normed(v):
        size = jnp.sqrt(dot3(v, v))
        return [part / size for part in v]

    axis_z, axis_x, axis_y = normed(normal), normed(side), normed(upward)
    oldb_x, oldb_y = dot3(axis_x, old_b), dot3(axis_y, old_b)
    oldc_x, oldc_y = dot3(axis_x, old_c), dot3(axis_y, old_c)
    newa_z = dot3(axis_z, rel_a)
    newb_x, newb_y, newb_z = dot3(axis_x, rel_b), dot3(axis_y, rel_b), dot3(axis_z, rel_b)
    newc_x, newc_y, newc_z = dot3(axis_x, rel_c), dot3(axis_y, rel_c), dot3(axis_z, rel_c)
    sin_phi = newa_z / oxygen_reach
    cos_phi = jnp.sqrt(1.0 - sin_phi * sin_phi)
    sin_psi = (newb_z - newc_z) / (2.0 * half_pair * cos_phi)
    cos_psi = jnp.sqrt(1.0 - sin_psi * sin_psi)
    rest_ay = oxygen_reach * cos_phi
    rest_bx = -half_pair * cos_psi
    lowered = -hydrogen_reach * cos_phi
    tilted = half_pair * sin_psi * sin_phi
    rest_by = lowered - tilted
    rest_cy = lowered + tilted
    alpha = rest_bx * (oldb_x - oldc_x) + oldb_y * rest_by + oldc_y * rest_cy
    beta = rest_bx * (oldc_y - oldb_y) + oldb_x * rest_by + oldc_x * rest_cy
    gamma = oldb_x * newb_y - newb_x * oldb_y + oldc_x * newc_y - newc_x * oldc_y
    summed = alpha * alpha + beta * beta
    sin_theta = (alpha * gamma - beta * jnp.sqrt(summed - gamma * gamma)) / summed
    cos_theta = jnp.sqrt(1.0 - sin_theta * sin_theta)
    final_ax = -rest_ay * sin_theta
    final_ay = rest_ay * cos_theta
    final_bx = rest_bx * cos_theta - rest_by * sin_theta
    final_by = rest_bx * sin_theta + rest_by * cos_theta
    final_cx = -rest_bx * cos_theta - rest_cy * sin_theta
    final_cy = -rest_bx * sin_theta + rest_cy * cos_theta
    oxygen = [center[c] + axis_x[c] * final_ax + axis_y[c] * final_ay + axis_z[c] * newa_z for c in every]
    first = [center[c] + axis_x[c] * final_bx + axis_y[c] * final_by + axis_z[c] * newb_z for c in every]
    second = [center[c] + axis_x[c] * final_cx + axis_y[c] * final_cy + axis_z[c] * newc_z for c in every]
    return oxygen + first + second


def sort_keys(keys):
    lane = lax.broadcasted_iota(jnp.int32, (8, LANES), 1)
    sub = lax.broadcasted_iota(jnp.int32, (8, LANES), 0)
    reg_bits = (len(keys) - 1).bit_length()
    bits = reg_bits + 10
    base = (lane * 8 + sub) << reg_bits

    def ordered(bit, size, here, there):
        turned = base >> bit if size == bits else (base >> bit) ^ (base >> size)
        return jnp.where((turned & 1) == 0, jnp.minimum(here, there), jnp.maximum(here, there))

    def registers(keys, bit, size):
        out = list(keys)
        for reg in range(len(keys)):
            if reg & (1 << bit):
                continue
            other = reg | (1 << bit)
            low = jnp.minimum(keys[reg], keys[other])
            high = jnp.maximum(keys[reg], keys[other])
            if size == bits:
                out[reg], out[other] = low, high
            elif size < reg_bits:
                out[reg], out[other] = (high, low) if reg & (1 << size) else (low, high)
            else:
                rising = ((base >> size) & 1) == 0
                out[reg] = jnp.where(rising, low, high)
                out[other] = jnp.where(rising, high, low)
        return out

    def sublanes(key, bit, size):
        step = 1 << (bit - reg_bits)
        if step == 4:
            mate = pltpu.roll(key, 4, 0)
        else:
            mate = jnp.where((sub & step) != 0, pltpu.roll(key, step, 0), pltpu.roll(key, 8 - step, 0))
        return ordered(bit, size, key, mate)

    def lanes(keys, group, size):
        steps = [1 << (bit - reg_bits - 3) for bit in group]
        reach = [0]
        for step in steps:
            reach = reach + [far ^ step for far in reach]
        values = {far: [lanes_of(key, lane ^ far) if far else key for key in keys] for far in reach}
        for bit, step in zip(group, steps):
            values = {
                far: [ordered(bit, size, here, there) for here, there in zip(values[far], values[far ^ step])]
                for far in values
                if far < step
            }
        return values[0]

    for size in range(1, bits + 1):
        crossing = [bit for bit in range(size - 1, reg_bits + 2, -1)]
        while crossing:
            width = {4: 2, 2: 2, 1: 1}.get(len(crossing), 3)
            group, crossing = crossing[:width], crossing[width:]
            keys = lanes(keys, group, size)
        for bit in range(min(size - 1, reg_bits + 2), -1, -1):
            if bit < reg_bits:
                keys = registers(keys, bit, size)
            else:
                keys = [sublanes(key, bit, size) for key in keys]
    return keys


def find(table, rows, queries):
    heads = table[0:1, :]
    marks = [jnp.broadcast_to(heads[:, 8 * i : 8 * i + 1], (8, LANES)) for i in range(1, 16)]
    wide = jnp.broadcast_to(heads, (8, LANES))
    rolled = [pltpu.roll(wide, LANES - i, 1) for i in range(1, 8)]
    found = []
    for query in queries:
        group = jnp.zeros((8, LANES), jnp.int32)
        for mark in marks:
            group = group + jnp.where(mark < query, 8, 0)
        column = group
        for turned in rolled:
            column = column + jnp.where(lanes_of(turned, group) < query, 1, 0)
        rank = column * rows
        best = jnp.full((8, LANES), -1.0, jnp.float32)
        for r in range(rows):
            key = lanes_of(spread(table, r), column)
            below = key < query
            rank = rank + jnp.where(below, 1, 0)
            best = jnp.maximum(best, jnp.where(below, key, -1.0))
        found.append((rank, best.astype(jnp.int32)))
    return found


def prepare(
    bonds_in, right_in, left_in, pos_in, vel_in, mass_in, pay, place,
    bonds, right, left, pos, vel, mass, atoms, ranked, listed, slots, arrived,
):
    lane = lax.broadcasted_iota(jnp.int32, (8, LANES), 1)
    sub = lax.broadcasted_iota(jnp.int32, (8, LANES), 0)
    f32, i32 = jnp.float32, jnp.int32

    sources = (bonds_in, right_in, left_in, pos_in, vel_in, mass_in)
    targets = (bonds, right, left, pos, vel, mass)
    copies = [
        pltpu.make_async_copy(source, target, arrived.at[k])
        for k, (source, target) in enumerate(zip(sources, targets))
    ]
    for copy in copies:
        copy.start()
    for copy in copies:
        copy.wait()

    def index(k):
        return (k * 8 + sub) * LANES + lane

    for r in range(BOND_ROWS):
        cut = slice(r * LANES, (r + 1) * LANES)
        atoms[r : r + 1, :] = bonds[0:1, cut]
        atoms[BOND_ROWS + r : BOND_ROWS + r + 1, :] = bonds[1:2, cut]
    atoms[END_ROWS:32, :] = jnp.full((32 - END_ROWS, LANES), 2048, i32)
    atoms[32 : 32 + SLOT_ROWS, :] = right[...]
    atoms[32 + SLOT_ROWS : 32 + CROSS_ROWS, :] = left[...]
    atoms[32 + CROSS_ROWS : 40, :] = jnp.full((8 - CROSS_ROWS, LANES), 4096, i32)
    crossed = atoms[32:40, :]

    keys = [(atoms[8 * k : 8 * k + 8, :] * 4096 + index(k)).astype(f32) for k in range(4)]
    keys = sort_keys(keys)
    for k in range(4):
        ranked[pl.ds(k, 8, stride=4), :] = keys[k]
    slots[...] = sort_keys([(crossed * 1024 + index(0)).astype(f32)])[0]

    own, far, mates = [], [], []
    quads = []
    for j in range(8):
        quad = ranked[4 * j : 4 * j + 4, :]
        quads.append(jnp.concatenate([quad, quad], axis=0))
    for k in range(3):
        rank = lane * END_ROWS + k * 8 + sub
        masks = bits_of((rank >> 2) & 7, 8)
        key = pick(lambda j: lanes_of(quads[j], rank >> 5), 8, masks)
        listed[8 * k : 8 * k + 8, :] = key
        key = key.astype(i32)
        end = key & 4095
        mate = jnp.where(end < HALF, end + HALF, end - HALF)
        other = gather_rows(functools.partial(spread, atoms), END_ROWS, mate >> 7, mate & 127)
        own.append(jnp.minimum(key >> 12, 2047))
        far.append(jnp.minimum(other, 2047))
        mates.append((other * 4096 + mate).astype(f32))

    def put(block, k, value):
        count = min(8, END_ROWS - 8 * k)
        pay[block + 8 * k : block + 8 * k + count, :] = value[:count].astype(f32)

    inside = find(
        listed,
        END_ROWS,
        mates + [((crossed + 1) * 4096).astype(f32)] + [((index(k) + 1) * 4096).astype(f32) for k in range(2)],
    )
    outside = find(
        slots, 8, [((a + 1) * 1024).astype(f32) for a in own] + [((index(k) + 1) * 1024).astype(f32) for k in range(2)]
    )
    for k in range(3):
        put(MATE, k, inside[k][0])
        best = outside[k][1]
        put(NAME, k, jnp.where(best >> 10 == own[k], best & 1023, own[k] + 1024))
    rank, best = inside[3]
    host = jnp.where(best >> 12 == crossed, rank - 1, NONE)
    pay[HOST : HOST + CROSS_ROWS, :] = host[:CROSS_ROWS].astype(f32)
    for k in range(2):
        rank, best = inside[4 + k]
        slot = outside[3 + k][1]
        row, col = place_of(rank - 1)
        place[8 * k : 8 * k + 8, :] = jnp.where(
            best >> 12 == index(k),
            row * LANES + col,
            jnp.where(slot >> 10 == index(k), END_ROWS * LANES + (slot & 1023), -1),
        )

    edge = jnp.minimum(crossed, 2047)
    where = [(a >> 7, a & 127) for a in own + far + [edge]]

    def wide(source, c, r):
        return jnp.broadcast_to(source[c : c + 1, r * LANES : (r + 1) * LANES], (8, LANES))

    tables = [functools.partial(wide, source, c) for source in (pos, vel) for c in range(3)]
    tables.append(functools.partial(spread, mass))

    def at(k):
        row, col = where[k]
        return [gather_rows(table, ATOM_ROWS, row, col) for table in tables]

    for k in range(3):
        near, away = at(k), at(3 + k)
        for c in range(6):
            put(END_ROWS * c, k, near[c] - away[c])
        put(MASS, k, near[6])
        put(SCAL, k, 1.0 / jnp.sqrt(near[6] + away[6]))
    for c, value in enumerate(at(6)):
        pay[CPOS + CROSS_ROWS * c : CPOS + CROSS_ROWS * (c + 1), :] = value[:CROSS_ROWS]


def solve(
    whole, place, vel, water_pos, water_vel, out, water_home,
    mate_row, mate_col, link_row, link_col, host_row, host_col, name, mass, push, length, scale, diff, drift,
    below, above, near, hinge, hinges, edge, edge_mass, edge_length, edge_scale, edge_diff, edge_drift, anchor,
    now, total, now_edge, total_edge, part, ties, moved, moved_edge, run, more, mine, index, shown,
    wet, water_out, leaving,
):
    zero = jnp.zeros((8, LANES), jnp.float32)
    every, ends, right = range(3), range(END_ROWS), range(SLOT_ROWS)

    def load(r):
        return whole[pl.ds(r, DOMAINS, stride=ROWS), :]

    def up(x):
        return pltpu.roll(x, DOMAINS - 1, 0)

    def down(x):
        return pltpu.roll(x, 1, 0)

    def around(rows):
        wide = {v: rows[v] for v in ends}
        for s in range(1, NEAR + 1):
            wide[-s] = pltpu.roll(rows[END_ROWS - s], 1, 1)
            wide[END_ROWS - 1 + s] = pltpu.roll(rows[s - 1], LANES - 1, 1)
        return wide

    def choose(rows, count, masks, col):
        return pick(lambda r: lanes_of(rows[r], col), count, masks)

    def both(values):
        return values + [down(x) for x in values]

    for j in range(8):
        cut = slice(j * LANES, (j + 1) * LANES)
        for c in range(9):
            wet[c, j : j + 1, :] = water_pos[c : c + 1, cut]
            wet[9 + c, j : j + 1, :] = water_vel[c : c + 1, cut]
    here = [wet[c] for c in range(9)]
    speed = [wet[9 + c] for c in range(9)]
    there = [here[c] + time_step * speed[c] for c in range(9)]
    settled = settle(here, there)
    for c in range(9):
        result = speed[c] + (settled[c] - there[c]) / time_step
        for j in range(8):
            water_out[c : c + 1, j * LANES : (j + 1) * LANES] = result[j : j + 1, :]
    drained = pltpu.make_async_copy(water_out, water_home, leaving)
    drained.start()

    for v in ends:
        row, col = place_of(load(MATE + v).astype(jnp.int32))
        mate_row[v], mate_col[v] = row, col
        mass[v] = load(MASS + v)
        name[v] = load(NAME + v)
        slot = name[v].astype(jnp.int32)
        link_row[v], link_col[v] = slot >> 7, slot & 127
    for r in range(CROSS_ROWS):
        row, col = place_of(load(HOST + r).astype(jnp.int32))
        host_row[r], host_col[r] = row, jnp.minimum(col, LANES - 1)
        anchor[r] = jnp.where(col < LANES, 1.0, 0.0)

    for v in ends:
        d = [load(DIFF + END_ROWS * c + v) for c in every]
        g = [time_step * load(VELO + END_ROWS * c + v) for c in every]
        s = load(SCAL + v)
        size = jnp.sqrt(dot3(d, d))
        rate = s / size
        rhs = rate * dot3(d, g)
        length[v], scale[v], now[v], total[v] = size, s, rhs, rhs
        for c in every:
            diff[c, v], drift[c, v], push[c, v], moved[c, v] = d[c], g[c], rate * d[c], zero

    start = []
    for r in right:
        l = r + SLOT_ROWS
        d = [load(CPOS + CROSS_ROWS * c + r) - up(load(CPOS + CROSS_ROWS * c + l)) for c in every]
        g = [
            time_step * (load(CVEL + CROSS_ROWS * c + r) - up(load(CVEL + CROSS_ROWS * c + l))) for c in every
        ]
        edge_mass[r], edge_mass[l] = load(CMAS + r), load(CMAS + l)
        s = 1.0 / jnp.sqrt(edge_mass[r] + up(edge_mass[l]))
        size = jnp.sqrt(dot3(d, d))
        rate = s / size
        edge_length[r], edge_scale[r] = size, s
        start.append(rate * dot3(d, g))
        for c in every:
            edge_diff[c, r], edge_drift[c, r] = d[c], g[c]
            edge[c, r], edge[c, l] = rate * d[c], -down(rate * d[c])
            moved_edge[c, r], moved_edge[c, l] = zero, zero
    for r, x in enumerate(both(start)):
        now_edge[r], total_edge[r] = x, x

    names = around([name[v] for v in ends])
    many = jnp.zeros((8, LANES), jnp.int32)
    fields = [around([push[c, v] for v in ends]) for c in every]
    for v in ends:
        here = [mass[v] * push[c, v] for c in every]
        for s in range(1, NEAR + 1):
            same = names[v] == names[v - s]
            near[s - 1, v] = jnp.where(same, 1.0, 0.0)
            below[s - 1, v] = jnp.where(same, dot3(here, [fields[c][v - s] for c in every]), 0.0)
            above[s - 1, v] = jnp.where(
                names[v] == names[v + s], dot3(here, [fields[c][v + s] for c in every]), 0.0
            )
        past = names[v - 4] if v >= 1 else pltpu.roll(name[END_ROWS - 4], 1, 1)
        many = jnp.where(names[v] == past, 1, many)
        masks = bits_of(link_row[v], CROSS_ROWS)
        linked = link_row[v] < CROSS_ROWS
        across = [choose([edge[c, r] for r in range(CROSS_ROWS)], CROSS_ROWS, masks, link_col[v]) for c in every]
        for c in every:
            ties[c, v] = jnp.where(linked, mass[v] * across[c], 0.0)
        hinge[v] = jnp.where(linked, dot3(here, across), 0.0)
    crowded = jnp.max(many) > 0
    bound = around([hinge[v] for v in ends])
    for v in ends:
        for s in range(1, NEAR + 1):
            hinges[s - 1, v] = jnp.where(near[s - 1, v] > 0.5, bound[v - s], 0.0)

    def gated(factor, value):
        return jnp.where(factor != 0.0, factor * value, 0.0)

    def scan(rows, forward):
        def double(k, carry):
            step = lax.shift_left(1, k)
            turns = step // END_ROWS
            rest = step - turns * END_ROWS

            def one(v, carry):
                source = v - rest if forward else v + rest
                wrap = jnp.where(source < 0, 1, 0) if forward else jnp.where(source >= END_ROWS, 1, 0)
                source = source + wrap * END_ROWS if forward else source - wrap * END_ROWS
                shift = turns + wrap if forward else (LANES - turns - wrap)
                match = name[v] == pltpu.roll(name[source], shift, 1)
                for r in rows:
                    more[r, v] = run[r, v] + jnp.where(match, pltpu.roll(run[r, source], shift, 1), 0.0)
                return carry

            lax.fori_loop(0, END_ROWS, one, 0)

            def keep(v, carry):
                for r in rows:
                    run[r, v] = more[r, v]
                return carry

            return lax.fori_loop(0, END_ROWS, keep, carry)

        lax.fori_loop(0, 12, double, 0)

    def scan_fields(source):
        def fill(v, carry):
            x = source[v]
            for c in every:
                run[c, v] = push[c, v] * x
                run[3 + c, v] = push[c, v] * x
            run[6, v] = gated(hinge[v], x)
            return carry

        lax.fori_loop(0, END_ROWS, fill, 0)
        scan((0, 1, 2, 6), True)
        scan((3, 4, 5), False)

    def at_edges(table):
        got = []
        for r in range(CROSS_ROWS):
            value = choose(table, END_ROWS, bits_of(host_row[r], END_ROWS), host_col[r])
            got.append(value)
        return got

    def apply(slow, last=False):
        x = around([now[v] for v in ends])
        crossing = [now_edge[r] for r in range(CROSS_ROWS)]
        if slow:
            scan_fields(now)

            def fill(v, carry):
                here = [push[c, v] for c in every]
                both_sides = [run[c, v] + run[3 + c, v] - 2.0 * here[c] * now[v] for c in every]
                part[0, v] = mass[v] * dot3(here, both_sides)
                part[1, v] = run[6, v]
                return carry

            lax.fori_loop(0, END_ROWS, fill, 0)
        sums, bounds = [], []
        for v in ends:
            if slow:
                sum_x, sum_bound = part[0, v], part[1, v]
            else:
                sum_x, sum_bound = zero, gated(hinge[v], x[v])
                for s in range(1, NEAR + 1):
                    sum_x = sum_x + gated(below[s - 1, v], x[v - s])
                    sum_x = sum_x + gated(above[s - 1, v], x[v + s])
                    sum_bound = sum_bound + gated(hinges[s - 1, v], x[v - s])
            value = choose(crossing, CROSS_ROWS, bits_of(link_row[v], CROSS_ROWS), link_col[v])
            sums.append(sum_x + gated(hinge[v], value))
            bounds.append(sum_bound)
        pulled = at_edges(bounds)
        pulled = [jnp.where(anchor[r] > 0.5, pulled[r], 0.0) for r in range(CROSS_ROWS)]
        for r, value in enumerate(both([-(pulled[r] + up(pulled[r + SLOT_ROWS])) for r in right])):
            now_edge[r] = value
            total_edge[r] = total_edge[r] + value
        if last:
            for v in ends:
                part[0, v] = sums[v]
            return
        for v in ends:
            value = choose(sums, END_ROWS, bits_of(mate_row[v], END_ROWS), mate_col[v])
            value = -(sums[v] + value)
            now[v] = value
            total[v] = total[v] + value

    def edges_moved():
        got = []
        for r in range(CROSS_ROWS):
            masks = bits_of(host_row[r], END_ROWS)
            fast = anchor[r] > 0.5
            got.append(
                [
                    jnp.where(fast, choose([moved[c, v] for v in ends], END_ROWS, masks, host_col[r]), moved_edge[c, r])
                    for c in every
                ]
            )
        return got

    def same(v, s):
        if s < 0:
            return near[-s - 1, v] > 0.5
        if v + s < END_ROWS:
            return near[s - 1, v + s] > 0.5
        return pltpu.roll(near[s - 1, v + s - END_ROWS], LANES - 1, 1) > 0.5

    def move(slow):
        if slow:
            scan_fields(total)

            def fill(v, carry):
                for c in every:
                    run[c, v] = run[c, v] + run[3 + c, v] - push[c, v] * total[v]
                return carry

            lax.fori_loop(0, END_ROWS, fill, 0)
        else:
            x = [total[v] for v in ends]
            for c in every:
                field = around([push[c, v] * x[v] for v in ends])
                for v in ends:
                    value = field[v]
                    for s in range(1, NEAR + 1):
                        value = value + jnp.where(same(v, -s), field[v - s], 0.0)
                        value = value + jnp.where(same(v, s), field[v + s], 0.0)
                    run[c, v] = value
        crossing = [total_edge[r] for r in range(CROSS_ROWS)]
        for v in ends:
            value = choose(crossing, CROSS_ROWS, bits_of(link_row[v], CROSS_ROWS), link_col[v])
            linked = link_row[v] < CROSS_ROWS
            for c in every:
                moved[c, v] = moved[c, v] + mass[v] * run[c, v] + jnp.where(linked, ties[c, v] * value, 0.0)
        edge_sums()

    def correct():
        def rate(d, g, size, s):
            excess = 2.0 * dot3(d, g) + dot3(g, g)
            return s * excess / (size + jnp.sqrt(size * size - excess))

        here = edges_moved()
        start = []
        for r in right:
            g = [edge_drift[c, r] - (here[r][c] - up(here[r + SLOT_ROWS][c])) for c in every]
            start.append(rate([edge_diff[c, r] for c in every], g, edge_length[r], edge_scale[r]))
        for r, value in enumerate(both(start)):
            now_edge[r], total_edge[r] = value, value
        for v in ends:
            masks = bits_of(mate_row[v], END_ROWS)
            there = [choose([moved[c, w] for w in ends], END_ROWS, masks, mate_col[v]) for c in every]
            g = [drift[c, v] - (moved[c, v] - there[c]) for c in every]
            value = rate([diff[c, v] for c in every], g, length[v], scale[v])
            now[v], total[v] = value, value

    me = lax.axis_index("dom")
    bands = range(3)

    def take(target, place, source):
        for v in ends:
            target[place, v : v + 1, :] = source(v)[pl.ds(me, 1), :]

    def band(ref, place, k):
        return ref[place, 8 * k : 8 * k + 8, :]

    def spots(place, k):
        return band(index, place, k) & (LANES - 1)

    def show(place, values):
        for k in bands:
            shown[place, 4 + 8 * k : min(12 + 8 * k, 24), :] = values[k][: min(8, END_ROWS - 8 * k)]
        shown[place, 0:4, :] = pltpu.roll(values[2], 1, 1)[0:4]
        shown[place, 24:28, :] = pltpu.roll(values[0], LANES - 1, 1)[0:4]

    def shifted(place, k, step):
        return shown[place, 4 + 8 * k + step : 12 + 8 * k + step, :]

    def edge_sums():
        for r in range(CROSS_ROWS):
            for c in every:
                moved_edge[c, r] = moved_edge[c, r] + edge_mass[r] * edge[c, r] * total_edge[r]

    def finish():
        take(mine, 3, lambda v: part.at[0, v])
        take(mine, 4, lambda v: total.at[v])
        for c in every:
            take(mine, c, lambda v: moved.at[c, v])
        crossing = [jnp.broadcast_to(total_edge[r, pl.ds(me, 1), :], (8, LANES)) for r in range(CROSS_ROWS)]
        x, links = [], []
        for k in bands:
            masks = bits_of(band(index, 0, k), END_ROWS)
            value = pick(
                lambda r: lanes_of(jnp.broadcast_to(mine[3, r : r + 1, :], (8, LANES)), spots(1, k)),
                END_ROWS,
                masks,
            )
            x.append(band(mine, 4, k) - (band(mine, 3, k) + value))
            masks = bits_of(band(index, 2, k), CROSS_ROWS)
            links.append(choose(crossing, CROSS_ROWS, masks, spots(3, k)))
        show(3, [band(mine, 5, k) for k in bands])
        for c in every:
            show(c, [band(mine, 6 + c, k) * x[k] for k in bands])
        for k in bands:
            linked = band(index, 2, k) < CROSS_ROWS
            value = [shifted(c, k, 0) for c in every]
            for step in (-3, -2, -1, 1, 2, 3):
                same = shifted(3, k, step) == band(mine, 5, k)
                value = [value[c] + jnp.where(same, shifted(c, k, step), 0.0) for c in every]
            for c in every:
                mine[c, 8 * k : 8 * k + 8, :] = (
                    band(mine, c, k)
                    + band(mine, 12, k) * value[c]
                    + jnp.where(linked, band(mine, 9 + c, k) * links[k], 0.0)
                )

    def rounds(slow):
        if slow:

            def one(order, carry):
                apply(True)
                return carry

            def turn(turns, carry):
                lax.fori_loop(0, ORDER, one, 0)
                move(True)

                @pl.when(turns < ITER)
                def _():
                    correct()

                return carry

            lax.fori_loop(0, ITER + 1, turn, 0)
            for c in every:
                take(mine, c, lambda v: moved.at[c, v])
            return

        take(mine, 5, lambda v: name.at[v])
        take(mine, 12, lambda v: mass.at[v])
        for c in every:
            take(mine, 6 + c, lambda v: push.at[c, v])
            take(mine, 9 + c, lambda v: ties.at[c, v])
        for place_in, source in enumerate((mate_row, mate_col, link_row, link_col)):
            take(index, place_in, lambda v: source.at[v])

        def turn(turns, carry):
            for order in range(ORDER):
                apply(False)
            move(False)
            correct()
            return carry

        lax.fori_loop(0, ITER, turn, 0)
        for order in range(ORDER):
            apply(False, order == ORDER - 1)
        edge_sums()
        finish()

    @pl.when(crowded)
    def _():
        rounds(True)

    @pl.when(jnp.logical_not(crowded))
    def _():
        rounds(False)

    own = [
        [jnp.broadcast_to(mine[c, v : v + 1, :], (8, LANES)) for v in ends]
        + [jnp.broadcast_to(moved_edge[c, r, pl.ds(me, 1), :], (8, LANES)) for r in range(CROSS_ROWS)]
        for c in every
    ]
    for k in range(2):
        code = place[8 * k : 8 * k + 8, :]
        bound = code >= 0
        code = jnp.maximum(code, 0)
        masks = bits_of(code >> 7, END_ROWS + CROSS_ROWS)
        for c in every:
            shift = choose(own[c], END_ROWS + CROSS_ROWS, masks, code & 127)
            shift = jnp.where(bound, shift, 0.0) / time_step
            for j in range(8):
                cut = slice((8 * k + j) * LANES, (8 * k + j + 1) * LANES)
                out[c : c + 1, cut] = vel[c : c + 1, cut] - shift[j : j + 1, :]
    drained.wait()


def on_device(
    protein_pos, protein_vel, inv_mass, bond_atoms, left_atoms, right_atoms, water_pos, water_vel
):
    f32, i32 = jnp.float32, jnp.int32
    inputs = (
        bond_atoms,
        right_atoms.reshape(SLOT_ROWS, LANES),
        left_atoms.reshape(SLOT_ROWS, LANES),
        protein_pos,
        protein_vel,
        inv_mass.reshape(ATOM_ROWS, LANES),
    )
    inputs = [pltpu.with_memory_space_constraint(x, pltpu.HBM) for x in inputs]
    pay, place = pl.pallas_call(
        prepare,
        in_specs=[pl.BlockSpec(memory_space=pltpu.HBM)] * len(inputs),
        out_shape=(
            jax.ShapeDtypeStruct((ROWS, LANES), f32),
            jax.ShapeDtypeStruct((ATOM_ROWS, LANES), i32),
        ),
        scratch_shapes=[
            *(pltpu.VMEM(x.shape, x.dtype) for x in inputs),
            pltpu.VMEM((40, LANES), i32),
            pltpu.VMEM((32, LANES), f32),
            pltpu.VMEM((24, LANES), f32),
            pltpu.VMEM((8, LANES), f32),
            pltpu.SemaphoreType.DMA((len(inputs),)),
        ],
        compiler_params=pltpu.CompilerParams(vmem_limit_bytes=8 << 20),
        name="prepare",
    )(*inputs)
    whole = lax.all_gather(pay, "dom", axis=0, tiled=True)

    def rows(*lead, dtype=f32):
        return pltpu.VMEM((*lead, 8, LANES), dtype)

    n, m = END_ROWS, CROSS_ROWS
    return pl.pallas_call(
        solve,
        out_specs=(pl.BlockSpec(memory_space=pltpu.VMEM), pl.BlockSpec(memory_space=pltpu.HBM)),
        out_shape=(
            jax.ShapeDtypeStruct(protein_vel.shape, f32),
            jax.ShapeDtypeStruct(water_pos.shape, f32),
        ),
        scratch_shapes=[
            *(rows(n, dtype=i32) for _ in range(4)),
            *(rows(m, dtype=i32) for _ in range(2)),
            *(rows(n) for _ in range(2)),
            rows(3, n),
            *(rows(n) for _ in range(2)),
            *(rows(3, n) for _ in range(2)),
            *(rows(NEAR, n) for _ in range(3)),
            rows(n),
            rows(NEAR, n),
            rows(3, m),
            *(rows(m) for _ in range(3)),
            *(rows(3, m) for _ in range(2)),
            rows(m),
            *(rows(n) for _ in range(2)),
            *(rows(m) for _ in range(2)),
            rows(2, n),
            *(rows(3, n) for _ in range(2)),
            rows(3, m),
            *(rows(7, n) for _ in range(2)),
            pltpu.VMEM((14, 24, LANES), f32),
            pltpu.VMEM((4, 24, LANES), i32),
            pltpu.VMEM((4, 32, LANES), f32),
            pltpu.VMEM((18, 8, LANES), f32),
            pltpu.VMEM(water_pos.shape, f32),
            pltpu.SemaphoreType.DMA,
        ],
        compiler_params=pltpu.CompilerParams(vmem_limit_bytes=16 << 20),
        name="solve",
    )(whole, place, protein_vel, water_pos, water_vel)


def solution(mesh):
    in_specs = (
        P(None, ("rep", "dom")),
        P(None, ("rep", "dom")),
        P(("rep", "dom")),
        P(None, ("rep", "dom")),
        P(("rep", "dom")),
        P(("rep", "dom")),
        P(None, ("rep", "dom")),
        P(None, ("rep", "dom")),
    )
    out_specs = (P(None, ("rep", "dom")), P(None, ("rep", "dom")))
    return jax.shard_map(
        on_device, mesh=mesh, in_specs=in_specs, out_specs=out_specs, check_vma=False
    )
```

```python
import functools
import math

import jax
import jax.numpy as jnp
from jax import lax
from jax.experimental import pallas as pl
from jax.experimental.pallas import tpu as pltpu
from jax.sharding import PartitionSpec as P

ORDER = 4
ITER = 2

time_step = 0.002
mass_oxygen = 15.9994
mass_hydrogen = 1.008
oxygen_hydrogen = 0.09572
hydrogen_pair = 0.15139
total_mass = mass_oxygen + 2.0 * mass_hydrogen
half_pair = 0.5 * hydrogen_pair
water_height = math.sqrt(oxygen_hydrogen * oxygen_hydrogen - half_pair * half_pair)
oxygen_reach = 2.0 * mass_hydrogen * water_height / total_mass
hydrogen_reach = water_height - oxygen_reach

LANES = 128
DOMAINS = 8
ATOM_ROWS = 16
BOND_ROWS = 10
SLOT_ROWS = 3
END_ROWS = 2 * BOND_ROWS
HALF = BOND_ROWS * LANES
CROSS_ROWS = 2 * SLOT_ROWS
NEAR = 3
NONE = 4095

DIFF, VELO, SCAL = 0, 3 * END_ROWS, 6 * END_ROWS
MASS, MATE, NAME = (k * END_ROWS for k in (7, 8, 9))
CPOS = 10 * END_ROWS
CVEL, CMAS, HOST = CPOS + 3 * CROSS_ROWS, CPOS + 6 * CROSS_ROWS, CPOS + 7 * CROSS_ROWS
ROWS = -(-(CPOS + 8 * CROSS_ROWS) // 8) * 8


def lanes_of(table, index):
    dims = lax.GatherDimensionNumbers(
        offset_dims=(),
        collapsed_slice_dims=(1,),
        start_index_map=(1,),
        operand_batching_dims=(0,),
        start_indices_batching_dims=(0,),
    )
    return lax.gather(
        table, index[..., None], dims, (1, 1), mode=lax.GatherScatterMode.PROMISE_IN_BOUNDS
    )


def bits_of(row, count):
    return [(row & (1 << b)) != 0 for b in range(max(1, (count - 1).bit_length()))]


def pick(get, count, masks, low=0):
    if count == 1:
        return get(low)
    bit = (count - 1).bit_length() - 1
    half = 1 << bit
    left = pick(get, half, masks, low)
    right = pick(get, count - half, masks, low + half)
    return jnp.where(masks[bit], right, left)


def gather_rows(table, count, row, lane):
    masks = bits_of(row, count)
    return pick(lambda r: lanes_of(table(r), lane), count, masks)


def spread(ref, r):
    return jnp.broadcast_to(ref[r : r + 1, :], (8, LANES))


def place_of(position):
    lane = (position * 3277) >> 16
    return position - lane * END_ROWS, lane


def cross3(a, b):
    return [a[1] * b[2] - a[2] * b[1], a[2] * b[0] - a[0] * b[2], a[0] * b[1] - a[1] * b[0]]


def dot3(a, b):
    return a[0] * b[0] + a[1] * b[1] + a[2] * b[2]


def settle(before, after):
    old_o, old_1, old_2 = before[0:3], before[3:6], before[6:9]
    new_o, new_1, new_2 = after[0:3], after[3:6], after[6:9]
    every = range(3)
    center = [(mass_oxygen * new_o[c] + mass_hydrogen * (new_1[c] + new_2[c])) / total_mass for c in every]
    old_b = [old_1[c] - old_o[c] for c in every]
    old_c = [old_2[c] - old_o[c] for c in every]
    rel_a = [new_o[c] - center[c] for c in every]
    rel_b = [new_1[c] - center[c] for c in every]
    rel_c = [new_2[c] - center[c] for c in every]
    normal = cross3(old_b, old_c)
    side = cross3(rel_a, normal)
    upward = cross3(normal, side)

    def normed(v):
        size = jnp.sqrt(dot3(v, v))
        return [part / size for part in v]

    axis_z, axis_x, axis_y = normed(normal), normed(side), normed(upward)
    oldb_x, oldb_y = dot3(axis_x, old_b), dot3(axis_y, old_b)
    oldc_x, oldc_y = dot3(axis_x, old_c), dot3(axis_y, old_c)
    newa_z = dot3(axis_z, rel_a)
    newb_x, newb_y, newb_z = dot3(axis_x, rel_b), dot3(axis_y, rel_b), dot3(axis_z, rel_b)
    newc_x, newc_y, newc_z = dot3(axis_x, rel_c), dot3(axis_y, rel_c), dot3(axis_z, rel_c)
    sin_phi = newa_z / oxygen_reach
    cos_phi = jnp.sqrt(1.0 - sin_phi * sin_phi)
    sin_psi = (newb_z - newc_z) / (2.0 * half_pair * cos_phi)
    cos_psi = jnp.sqrt(1.0 - sin_psi * sin_psi)
    rest_ay = oxygen_reach * cos_phi
    rest_bx = -half_pair * cos_psi
    lowered = -hydrogen_reach * cos_phi
    tilted = half_pair * sin_psi * sin_phi
    rest_by = lowered - tilted
    rest_cy = lowered + tilted
    alpha = rest_bx * (oldb_x - oldc_x) + oldb_y * rest_by + oldc_y * rest_cy
    beta = rest_bx * (oldc_y - oldb_y) + oldb_x * rest_by + oldc_x * rest_cy
    gamma = oldb_x * newb_y - newb_x * oldb_y + oldc_x * newc_y - newc_x * oldc_y
    summed = alpha * alpha + beta * beta
    sin_theta = (alpha * gamma - beta * jnp.sqrt(summed - gamma * gamma)) / summed
    cos_theta = jnp.sqrt(1.0 - sin_theta * sin_theta)
    final_ax = -rest_ay * sin_theta
    final_ay = rest_ay * cos_theta
    final_bx = rest_bx * cos_theta - rest_by * sin_theta
    final_by = rest_bx * sin_theta + rest_by * cos_theta
    final_cx = -rest_bx * cos_theta - rest_cy * sin_theta
    final_cy = -rest_bx * sin_theta + rest_cy * cos_theta
    oxygen = [center[c] + axis_x[c] * final_ax + axis_y[c] * final_ay + axis_z[c] * newa_z for c in every]
    first = [center[c] + axis_x[c] * final_bx + axis_y[c] * final_by + axis_z[c] * newb_z for c in every]
    second = [center[c] + axis_x[c] * final_cx + axis_y[c] * final_cy + axis_z[c] * newc_z for c in every]
    return oxygen + first + second


def sort_keys(keys):
    lane = lax.broadcasted_iota(jnp.int32, (8, LANES), 1)
    sub = lax.broadcasted_iota(jnp.int32, (8, LANES), 0)
    reg_bits = (len(keys) - 1).bit_length()
    bits = reg_bits + 10
    base = (lane * 8 + sub) << reg_bits

    def ordered(bit, size, here, there):
        turned = base >> bit if size == bits else (base >> bit) ^ (base >> size)
        return jnp.where((turned & 1) == 0, jnp.minimum(here, there), jnp.maximum(here, there))

    def registers(keys, bit, size):
        out = list(keys)
        for reg in range(len(keys)):
            if reg & (1 << bit):
                continue
            other = reg | (1 << bit)
            low = jnp.minimum(keys[reg], keys[other])
            high = jnp.maximum(keys[reg], keys[other])
            if size == bits:
                out[reg], out[other] = low, high
            elif size < reg_bits:
                out[reg], out[other] = (high, low) if reg & (1 << size) else (low, high)
            else:
                rising = ((base >> size) & 1) == 0
                out[reg] = jnp.where(rising, low, high)
                out[other] = jnp.where(rising, high, low)
        return out

    def sublanes(key, bit, size):
        step = 1 << (bit - reg_bits)
        if step == 4:
            mate = pltpu.roll(key, 4, 0)
        else:
            mate = jnp.where((sub & step) != 0, pltpu.roll(key, step, 0), pltpu.roll(key, 8 - step, 0))
        return ordered(bit, size, key, mate)

    def lanes(keys, group, size):
        steps = [1 << (bit - reg_bits - 3) for bit in group]
        reach = [0]
        for step in steps:
            reach = reach + [far ^ step for far in reach]
        values = {far: [lanes_of(key, lane ^ far) if far else key for key in keys] for far in reach}
        for bit, step in zip(group, steps):
            values = {
                far: [ordered(bit, size, here, there) for here, there in zip(values[far], values[far ^ step])]
                for far in values
                if far < step
            }
        return values[0]

    for size in range(1, bits + 1):
        crossing = [bit for bit in range(size - 1, reg_bits + 2, -1)]
        while crossing:
            width = {4: 2, 2: 2, 1: 1}.get(len(crossing), 3)
            group, crossing = crossing[:width], crossing[width:]
            keys = lanes(keys, group, size)
        for bit in range(min(size - 1, reg_bits + 2), -1, -1):
            if bit < reg_bits:
                keys = registers(keys, bit, size)
            else:
                keys = [sublanes(key, bit, size) for key in keys]
    return keys


def find(table, rows, queries):
    heads = table[0:1, :]
    marks = [jnp.broadcast_to(heads[:, 8 * i : 8 * i + 1], (8, LANES)) for i in range(1, 16)]
    wide = jnp.broadcast_to(heads, (8, LANES))
    rolled = [pltpu.roll(wide, LANES - i, 1) for i in range(1, 8)]
    found = []
    for query in queries:
        group = jnp.zeros((8, LANES), jnp.int32)
        for mark in marks:
            group = group + jnp.where(mark < query, 8, 0)
        column = group
        for turned in rolled:
            column = column + jnp.where(lanes_of(turned, group) < query, 1, 0)
        rank = column * rows
        best = jnp.full((8, LANES), -1.0, jnp.float32)
        for r in range(rows):
            key = lanes_of(spread(table, r), column)
            below = key < query
            rank = rank + jnp.where(below, 1, 0)
            best = jnp.maximum(best, jnp.where(below, key, -1.0))
        found.append((rank, best.astype(jnp.int32)))
    return found


def prepare(
    bonds_in, right_in, left_in, pos_in, vel_in, mass_in, pay, place,
    bonds, right, left, pos, vel, mass, atoms, ranked, listed, slots, arrived,
):
    lane = lax.broadcasted_iota(jnp.int32, (8, LANES), 1)
    sub = lax.broadcasted_iota(jnp.int32, (8, LANES), 0)
    f32, i32 = jnp.float32, jnp.int32

    sources = (bonds_in, right_in, left_in, pos_in, vel_in, mass_in)
    targets = (bonds, right, left, pos, vel, mass)
    copies = [
        pltpu.make_async_copy(source, target, arrived.at[k])
        for k, (source, target) in enumerate(zip(sources, targets))
    ]
    for copy in copies:
        copy.start()
    for copy in copies:
        copy.wait()

    def index(k):
        return (k * 8 + sub) * LANES + lane

    for r in range(BOND_ROWS):
        cut = slice(r * LANES, (r + 1) * LANES)
        atoms[r : r + 1, :] = bonds[0:1, cut]
        atoms[BOND_ROWS + r : BOND_ROWS + r + 1, :] = bonds[1:2, cut]
    atoms[END_ROWS:32, :] = jnp.full((32 - END_ROWS, LANES), 2048, i32)
    atoms[32 : 32 + SLOT_ROWS, :] = right[...]
    atoms[32 + SLOT_ROWS : 32 + CROSS_ROWS, :] = left[...]
    atoms[32 + CROSS_ROWS : 40, :] = jnp.full((8 - CROSS_ROWS, LANES), 4096, i32)
    crossed = atoms[32:40, :]

    keys = [(atoms[8 * k : 8 * k + 8, :] * 4096 + index(k)).astype(f32) for k in range(4)]
    keys = sort_keys(keys)
    for k in range(4):
        ranked[pl.ds(k, 8, stride=4), :] = keys[k]
    slots[...] = sort_keys([(crossed * 1024 + index(0)).astype(f32)])[0]

    own, far, mates = [], [], []
    quads = []
    for j in range(8):
        quad = ranked[4 * j : 4 * j + 4, :]
        quads.append(jnp.concatenate([quad, quad], axis=0))
    for k in range(3):
        rank = lane * END_ROWS + k * 8 + sub
        masks = bits_of((rank >> 2) & 7, 8)
        key = pick(lambda j: lanes_of(quads[j], rank >> 5), 8, masks)
        listed[8 * k : 8 * k + 8, :] = key
        key = key.astype(i32)
        end = key & 4095
        mate = jnp.where(end < HALF, end + HALF, end - HALF)
        other = gather_rows(functools.partial(spread, atoms), END_ROWS, mate >> 7, mate & 127)
        own.append(jnp.minimum(key >> 12, 2047))
        far.append(jnp.minimum(other, 2047))
        mates.append((other * 4096 + mate).astype(f32))

    def put(block, k, value):
        count = min(8, END_ROWS - 8 * k)
        pay[block + 8 * k : block + 8 * k + count, :] = value[:count].astype(f32)

    inside = find(
        listed,
        END_ROWS,
        mates + [((crossed + 1) * 4096).astype(f32)] + [((index(k) + 1) * 4096).astype(f32) for k in range(2)],
    )
    outside = find(
        slots, 8, [((a + 1) * 1024).astype(f32) for a in own] + [((index(k) + 1) * 1024).astype(f32) for k in range(2)]
    )
    for k in range(3):
        put(MATE, k, inside[k][0])
        best = outside[k][1]
        put(NAME, k, jnp.where(best >> 10 == own[k], best & 1023, own[k] + 1024))
    rank, best = inside[3]
    host = jnp.where(best >> 12 == crossed, rank - 1, NONE)
    pay[HOST : HOST + CROSS_ROWS, :] = host[:CROSS_ROWS].astype(f32)
    for k in range(2):
        rank, best = inside[4 + k]
        slot = outside[3 + k][1]
        row, col = place_of(rank - 1)
        place[8 * k : 8 * k + 8, :] = jnp.where(
            best >> 12 == index(k),
            row * LANES + col,
            jnp.where(slot >> 10 == index(k), END_ROWS * LANES + (slot & 1023), -1),
        )

    edge = jnp.minimum(crossed, 2047)
    where = [(a >> 7, a & 127) for a in own + far + [edge]]

    def wide(source, c, r):
        return jnp.broadcast_to(source[c : c + 1, r * LANES : (r + 1) * LANES], (8, LANES))

    tables = [functools.partial(wide, source, c) for source in (pos, vel) for c in range(3)]
    tables.append(functools.partial(spread, mass))

    def at(k):
        row, col = where[k]
        return [gather_rows(table, ATOM_ROWS, row, col) for table in tables]

    for k in range(3):
        near, away = at(k), at(3 + k)
        for c in range(6):
            put(END_ROWS * c, k, near[c] - away[c])
        put(MASS, k, near[6])
        put(SCAL, k, 1.0 / jnp.sqrt(near[6] + away[6]))
    for c, value in enumerate(at(6)):
        pay[CPOS + CROSS_ROWS * c : CPOS + CROSS_ROWS * (c + 1), :] = value[:CROSS_ROWS]


def solve(
    whole, place, vel, water_pos, water_vel, out, water_home,
    mate_row, mate_col, link_row, link_col, host_row, host_col, name, mass, push, length, scale, diff, drift,
    below, above, near, hinge, hinges, edge, edge_mass, edge_length, edge_scale, edge_diff, edge_drift, anchor,
    now, total, now_edge, total_edge, part, ties, moved, moved_edge, run, more, mine, index, shown,
    wet, water_out, leaving,
):
    zero = jnp.zeros((8, LANES), jnp.float32)
    every, ends, right = range(3), range(END_ROWS), range(SLOT_ROWS)

    def load(r):
        return whole[pl.ds(r, DOMAINS, stride=ROWS), :]

    def up(x):
        return pltpu.roll(x, DOMAINS - 1, 0)

    def down(x):
        return pltpu.roll(x, 1, 0)

    def around(rows):
        wide = {v: rows[v] for v in ends}
        for s in range(1, NEAR + 1):
            wide[-s] = pltpu.roll(rows[END_ROWS - s], 1, 1)
            wide[END_ROWS - 1 + s] = pltpu.roll(rows[s - 1], LANES - 1, 1)
        return wide

    def choose(rows, count, masks, col):
        return pick(lambda r: lanes_of(rows[r], col), count, masks)

    def both(values):
        return values + [down(x) for x in values]

    for j in range(8):
        cut = slice(j * LANES, (j + 1) * LANES)
        for c in range(9):
            wet[c, j : j + 1, :] = water_pos[c : c + 1, cut]
            wet[9 + c, j : j + 1, :] = water_vel[c : c + 1, cut]
    here = [wet[c] for c in range(9)]
    speed = [wet[9 + c] for c in range(9)]
    there = [here[c] + time_step * speed[c] for c in range(9)]
    settled = settle(here, there)
    for c in range(9):
        result = speed[c] + (settled[c] - there[c]) / time_step
        for j in range(8):
            water_out[c : c + 1, j * LANES : (j + 1) * LANES] = result[j : j + 1, :]
    drained = pltpu.make_async_copy(water_out, water_home, leaving)
    drained.start()

    for v in ends:
        row, col = place_of(load(MATE + v).astype(jnp.int32))
        mate_row[v], mate_col[v] = row, col
        mass[v] = load(MASS + v)
        name[v] = load(NAME + v)
        slot = name[v].astype(jnp.int32)
        link_row[v], link_col[v] = slot >> 7, slot & 127
    for r in range(CROSS_ROWS):
        row, col = place_of(load(HOST + r).astype(jnp.int32))
        host_row[r], host_col[r] = row, jnp.minimum(col, LANES - 1)
        anchor[r] = jnp.where(col < LANES, 1.0, 0.0)

    for v in ends:
        d = [load(DIFF + END_ROWS * c + v) for c in every]
        g = [time_step * load(VELO + END_ROWS * c + v) for c in every]
        s = load(SCAL + v)
        size = jnp.sqrt(dot3(d, d))
        rate = s / size
        rhs = rate * dot3(d, g)
        length[v], scale[v], now[v], total[v] = size, s, rhs, rhs
        for c in every:
            diff[c, v], drift[c, v], push[c, v], moved[c, v] = d[c], g[c], rate * d[c], zero

    start = []
    for r in right:
        l = r + SLOT_ROWS
        d = [load(CPOS + CROSS_ROWS * c + r) - up(load(CPOS + CROSS_ROWS * c + l)) for c in every]
        g = [
            time_step * (load(CVEL + CROSS_ROWS * c + r) - up(load(CVEL + CROSS_ROWS * c + l))) for c in every
        ]
        edge_mass[r], edge_mass[l] = load(CMAS + r), load(CMAS + l)
        s = 1.0 / jnp.sqrt(edge_mass[r] + up(edge_mass[l]))
        size = jnp.sqrt(dot3(d, d))
        rate = s / size
        edge_length[r], edge_scale[r] = size, s
        start.append(rate * dot3(d, g))
        for c in every:
            edge_diff[c, r], edge_drift[c, r] = d[c], g[c]
            edge[c, r], edge[c, l] = rate * d[c], -down(rate * d[c])
            moved_edge[c, r], moved_edge[c, l] = zero, zero
    for r, x in enumerate(both(start)):
        now_edge[r], total_edge[r] = x, x

    names = around([name[v] for v in ends])
    many = jnp.zeros((8, LANES), jnp.int32)
    fields = [around([push[c, v] for v in ends]) for c in every]
    for v in ends:
        here = [mass[v] * push[c, v] for c in every]
        for s in range(1, NEAR + 1):
            same = names[v] == names[v - s]
            near[s - 1, v] = jnp.where(same, 1.0, 0.0)
            below[s - 1, v] = jnp.where(same, dot3(here, [fields[c][v - s] for c in every]), 0.0)
            above[s - 1, v] = jnp.where(
                names[v] == names[v + s], dot3(here, [fields[c][v + s] for c in every]), 0.0
            )
        past = names[v - 4] if v >= 1 else pltpu.roll(name[END_ROWS - 4], 1, 1)
        many = jnp.where(names[v] == past, 1, many)
        masks = bits_of(link_row[v], CROSS_ROWS)
        linked = link_row[v] < CROSS_ROWS
        across = [choose([edge[c, r] for r in range(CROSS_ROWS)], CROSS_ROWS, masks, link_col[v]) for c in every]
        for c in every:
            ties[c, v] = jnp.where(linked, mass[v] * across[c], 0.0)
        hinge[v] = jnp.where(linked, dot3(here, across), 0.0)
    crowded = jnp.max(many) > 0
    bound = around([hinge[v] for v in ends])
    for v in ends:
        for s in range(1, NEAR + 1):
            hinges[s - 1, v] = jnp.where(near[s - 1, v] > 0.5, bound[v - s], 0.0)

    def gated(factor, value):
        return jnp.where(factor != 0.0, factor * value, 0.0)

    def scan(rows, forward):
        def double(k, carry):
            step = lax.shift_left(1, k)
            turns = step // END_ROWS
            rest = step - turns * END_ROWS

            def one(v, carry):
                source = v - rest if forward else v + rest
                wrap = jnp.where(source < 0, 1, 0) if forward else jnp.where(source >= END_ROWS, 1, 0)
                source = source + wrap * END_ROWS if forward else source - wrap * END_ROWS
                shift = turns + wrap if forward else (LANES - turns - wrap)
                match = name[v] == pltpu.roll(name[source], shift, 1)
                for r in rows:
                    more[r, v] = run[r, v] + jnp.where(match, pltpu.roll(run[r, source], shift, 1), 0.0)
                return carry

            lax.fori_loop(0, END_ROWS, one, 0)

            def keep(v, carry):
                for r in rows:
                    run[r, v] = more[r, v]
                return carry

            return lax.fori_loop(0, END_ROWS, keep, carry)

        lax.fori_loop(0, 12, double, 0)

    def scan_fields(source):
        def fill(v, carry):
            x = source[v]
            for c in every:
                run[c, v] = push[c, v] * x
                run[3 + c, v] = push[c, v] * x
            run[6, v] = gated(hinge[v], x)
            return carry

        lax.fori_loop(0, END_ROWS, fill, 0)
        scan((0, 1, 2, 6), True)
        scan((3, 4, 5), False)

    def at_edges(table):
        got = []
        for r in range(CROSS_ROWS):
            value = choose(table, END_ROWS, bits_of(host_row[r], END_ROWS), host_col[r])
            got.append(value)
        return got

    def apply(slow, last=False):
        x = around([now[v] for v in ends])
        crossing = [now_edge[r] for r in range(CROSS_ROWS)]
        if slow:
            scan_fields(now)

            def fill(v, carry):
                here = [push[c, v] for c in every]
                both_sides = [run[c, v] + run[3 + c, v] - 2.0 * here[c] * now[v] for c in every]
                part[0, v] = mass[v] * dot3(here, both_sides)
                part[1, v] = run[6, v]
                return carry

            lax.fori_loop(0, END_ROWS, fill, 0)
        sums, bounds = [], []
        for v in ends:
            if slow:
                sum_x, sum_bound = part[0, v], part[1, v]
            else:
                sum_x, sum_bound = zero, gated(hinge[v], x[v])
                for s in range(1, NEAR + 1):
                    sum_x = sum_x + gated(below[s - 1, v], x[v - s])
                    sum_x = sum_x + gated(above[s - 1, v], x[v + s])
                    sum_bound = sum_bound + gated(hinges[s - 1, v], x[v - s])
            value = choose(crossing, CROSS_ROWS, bits_of(link_row[v], CROSS_ROWS), link_col[v])
            sums.append(sum_x + gated(hinge[v], value))
            bounds.append(sum_bound)
        pulled = at_edges(bounds)
        pulled = [jnp.where(anchor[r] > 0.5, pulled[r], 0.0) for r in range(CROSS_ROWS)]
        for r, value in enumerate(both([-(pulled[r] + up(pulled[r + SLOT_ROWS])) for r in right])):
            now_edge[r] = value
            total_edge[r] = total_edge[r] + value
        if last:
            for v in ends:
                part[0, v] = sums[v]
            return
        for v in ends:
            value = choose(sums, END_ROWS, bits_of(mate_row[v], END_ROWS), mate_col[v])
            value = -(sums[v] + value)
            now[v] = value
            total[v] = total[v] + value

    def edges_moved():
        got = []
        for r in range(CROSS_ROWS):
            masks = bits_of(host_row[r], END_ROWS)
            fast = anchor[r] > 0.5
            got.append(
                [
                    jnp.where(fast, choose([moved[c, v] for v in ends], END_ROWS, masks, host_col[r]), moved_edge[c, r])
                    for c in every
                ]
            )
        return got

    def same(v, s):
        if s < 0:
            return near[-s - 1, v] > 0.5
        if v + s < END_ROWS:
            return near[s - 1, v + s] > 0.5
        return pltpu.roll(near[s - 1, v + s - END_ROWS], LANES - 1, 1) > 0.5

    def move(slow):
        if slow:
            scan_fields(total)

            def fill(v, carry):
                for c in every:
                    run[c, v] = run[c, v] + run[3 + c, v] - push[c, v] * total[v]
                return carry

            lax.fori_loop(0, END_ROWS, fill, 0)
        else:
            x = [total[v] for v in ends]
            for c in every:
                field = around([push[c, v] * x[v] for v in ends])
                for v in ends:
                    value = field[v]
                    for s in range(1, NEAR + 1):
                        value = value + jnp.where(same(v, -s), field[v - s], 0.0)
                        value = value + jnp.where(same(v, s), field[v + s], 0.0)
                    run[c, v] = value
        crossing = [total_edge[r] for r in range(CROSS_ROWS)]
        for v in ends:
            value = choose(crossing, CROSS_ROWS, bits_of(link_row[v], CROSS_ROWS), link_col[v])
            linked = link_row[v] < CROSS_ROWS
            for c in every:
                moved[c, v] = moved[c, v] + mass[v] * run[c, v] + jnp.where(linked, ties[c, v] * value, 0.0)
        edge_sums()

    def correct():
        def rate(d, g, size, s):
            excess = 2.0 * dot3(d, g) + dot3(g, g)
            return s * excess / (size + jnp.sqrt(size * size - excess))

        here = edges_moved()
        start = []
        for r in right:
            g = [edge_drift[c, r] - (here[r][c] - up(here[r + SLOT_ROWS][c])) for c in every]
            start.append(rate([edge_diff[c, r] for c in every], g, edge_length[r], edge_scale[r]))
        for r, value in enumerate(both(start)):
            now_edge[r], total_edge[r] = value, value
        for v in ends:
            masks = bits_of(mate_row[v], END_ROWS)
            there = [choose([moved[c, w] for w in ends], END_ROWS, masks, mate_col[v]) for c in every]
            g = [drift[c, v] - (moved[c, v] - there[c]) for c in every]
            value = rate([diff[c, v] for c in every], g, length[v], scale[v])
            now[v], total[v] = value, value

    me = lax.axis_index("dom")
    bands = range(3)

    def take(target, place, source):
        for v in ends:
            target[place, v : v + 1, :] = source(v)[pl.ds(me, 1), :]

    def band(ref, place, k):
        return ref[place, 8 * k : 8 * k + 8, :]

    def spots(place, k):
        return band(index, place, k) & (LANES - 1)

    def show(place, values):
        for k in bands:
            shown[place, 4 + 8 * k : min(12 + 8 * k, 24), :] = values[k][: min(8, END_ROWS - 8 * k)]
        shown[place, 0:4, :] = pltpu.roll(values[2], 1, 1)[0:4]
        shown[place, 24:28, :] = pltpu.roll(values[0], LANES - 1, 1)[0:4]

    def shifted(place, k, step):
        return shown[place, 4 + 8 * k + step : 12 + 8 * k + step, :]

    def edge_sums():
        for r in range(CROSS_ROWS):
            for c in every:
                moved_edge[c, r] = moved_edge[c, r] + edge_mass[r] * edge[c, r] * total_edge[r]

    def finish():
        take(mine, 3, lambda v: part.at[0, v])
        take(mine, 4, lambda v: total.at[v])
        for c in every:
            take(mine, c, lambda v: moved.at[c, v])
        crossing = [jnp.broadcast_to(total_edge[r, pl.ds(me, 1), :], (8, LANES)) for r in range(CROSS_ROWS)]
        x, links = [], []
        for k in bands:
            masks = bits_of(band(index, 0, k), END_ROWS)
            value = pick(
                lambda r: lanes_of(jnp.broadcast_to(mine[3, r : r + 1, :], (8, LANES)), spots(1, k)),
                END_ROWS,
                masks,
            )
            x.append(band(mine, 4, k) - (band(mine, 3, k) + value))
            masks = bits_of(band(index, 2, k), CROSS_ROWS)
            links.append(choose(crossing, CROSS_ROWS, masks, spots(3, k)))
        show(3, [band(mine, 5, k) for k in bands])
        for c in every:
            show(c, [band(mine, 6 + c, k) * x[k] for k in bands])
        for k in bands:
            linked = band(index, 2, k) < CROSS_ROWS
            value = [shifted(c, k, 0) for c in every]
            for step in (-3, -2, -1, 1, 2, 3):
                same = shifted(3, k, step) == band(mine, 5, k)
                value = [value[c] + jnp.where(same, shifted(c, k, step), 0.0) for c in every]
            for c in every:
                mine[c, 8 * k : 8 * k + 8, :] = (
                    band(mine, c, k)
                    + band(mine, 12, k) * value[c]
                    + jnp.where(linked, band(mine, 9 + c, k) * links[k], 0.0)
                )

    def rounds(slow):
        if slow:

            def one(order, carry):
                apply(True)
                return carry

            def turn(turns, carry):
                lax.fori_loop(0, ORDER, one, 0)
                move(True)

                @pl.when(turns < ITER)
                def _():
                    correct()

                return carry

            lax.fori_loop(0, ITER + 1, turn, 0)
            for c in every:
                take(mine, c, lambda v: moved.at[c, v])
            return

        take(mine, 5, lambda v: name.at[v])
        take(mine, 12, lambda v: mass.at[v])
        for c in every:
            take(mine, 6 + c, lambda v: push.at[c, v])
            take(mine, 9 + c, lambda v: ties.at[c, v])
        for place_in, source in enumerate((mate_row, mate_col, link_row, link_col)):
            take(index, place_in, lambda v: source.at[v])

        def turn(turns, carry):
            lax.fori_loop(0, ORDER // 2, lambda order, carry: (apply(False), apply(False), carry)[2], 0)
            move(False)
            correct()
            return carry

        lax.fori_loop(0, ITER, turn, 0)
        for order in range(ORDER):
            apply(False, order == ORDER - 1)
        edge_sums()
        finish()

    @pl.when(crowded)
    def _():
        rounds(True)

    @pl.when(jnp.logical_not(crowded))
    def _():
        rounds(False)

    own = [
        [jnp.broadcast_to(mine[c, v : v + 1, :], (8, LANES)) for v in ends]
        + [jnp.broadcast_to(moved_edge[c, r, pl.ds(me, 1), :], (8, LANES)) for r in range(CROSS_ROWS)]
        for c in every
    ]
    for k in range(2):
        code = place[8 * k : 8 * k + 8, :]
        bound = code >= 0
        code = jnp.maximum(code, 0)
        masks = bits_of(code >> 7, END_ROWS + CROSS_ROWS)
        for c in every:
            shift = choose(own[c], END_ROWS + CROSS_ROWS, masks, code & 127)
            shift = jnp.where(bound, shift, 0.0) / time_step
            for j in range(8):
                cut = slice((8 * k + j) * LANES, (8 * k + j + 1) * LANES)
                out[c : c + 1, cut] = vel[c : c + 1, cut] - shift[j : j + 1, :]
    drained.wait()


def on_device(
    protein_pos, protein_vel, inv_mass, bond_atoms, left_atoms, right_atoms, water_pos, water_vel
):
    f32, i32 = jnp.float32, jnp.int32
    inputs = (
        bond_atoms,
        right_atoms.reshape(SLOT_ROWS, LANES),
        left_atoms.reshape(SLOT_ROWS, LANES),
        protein_pos,
        protein_vel,
        inv_mass.reshape(ATOM_ROWS, LANES),
    )
    inputs = [pltpu.with_memory_space_constraint(x, pltpu.HBM) for x in inputs]
    pay, place = pl.pallas_call(
        prepare,
        in_specs=[pl.BlockSpec(memory_space=pltpu.HBM)] * len(inputs),
        out_shape=(
            jax.ShapeDtypeStruct((ROWS, LANES), f32),
            jax.ShapeDtypeStruct((ATOM_ROWS, LANES), i32),
        ),
        scratch_shapes=[
            *(pltpu.VMEM(x.shape, x.dtype) for x in inputs),
            pltpu.VMEM((40, LANES), i32),
            pltpu.VMEM((32, LANES), f32),
            pltpu.VMEM((24, LANES), f32),
            pltpu.VMEM((8, LANES), f32),
            pltpu.SemaphoreType.DMA((len(inputs),)),
        ],
        compiler_params=pltpu.CompilerParams(vmem_limit_bytes=8 << 20),
        name="prepare",
    )(*inputs)
    whole = lax.all_gather(pay, "dom", axis=0, tiled=True)

    def rows(*lead, dtype=f32):
        return pltpu.VMEM((*lead, 8, LANES), dtype)

    n, m = END_ROWS, CROSS_ROWS
    return pl.pallas_call(
        solve,
        out_specs=(pl.BlockSpec(memory_space=pltpu.VMEM), pl.BlockSpec(memory_space=pltpu.HBM)),
        out_shape=(
            jax.ShapeDtypeStruct(protein_vel.shape, f32),
            jax.ShapeDtypeStruct(water_pos.shape, f32),
        ),
        scratch_shapes=[
            *(rows(n, dtype=i32) for _ in range(4)),
            *(rows(m, dtype=i32) for _ in range(2)),
            *(rows(n) for _ in range(2)),
            rows(3, n),
            *(rows(n) for _ in range(2)),
            *(rows(3, n) for _ in range(2)),
            *(rows(NEAR, n) for _ in range(3)),
            rows(n),
            rows(NEAR, n),
            rows(3, m),
            *(rows(m) for _ in range(3)),
            *(rows(3, m) for _ in range(2)),
            rows(m),
            *(rows(n) for _ in range(2)),
            *(rows(m) for _ in range(2)),
            rows(2, n),
            *(rows(3, n) for _ in range(2)),
            rows(3, m),
            *(rows(7, n) for _ in range(2)),
            pltpu.VMEM((14, 24, LANES), f32),
            pltpu.VMEM((4, 24, LANES), i32),
            pltpu.VMEM((4, 32, LANES), f32),
            pltpu.VMEM((18, 8, LANES), f32),
            pltpu.VMEM(water_pos.shape, f32),
            pltpu.SemaphoreType.DMA,
        ],
        compiler_params=pltpu.CompilerParams(vmem_limit_bytes=16 << 20),
        name="solve",
    )(whole, place, protein_vel, water_pos, water_vel)


def solution(mesh):
    in_specs = (
        P(None, ("rep", "dom")),
        P(None, ("rep", "dom")),
        P(("rep", "dom")),
        P(None, ("rep", "dom")),
        P(("rep", "dom")),
        P(("rep", "dom")),
        P(None, ("rep", "dom")),
        P(None, ("rep", "dom")),
    )
    out_specs = (P(None, ("rep", "dom")), P(None, ("rep", "dom")))
    return jax.shard_map(
        on_device, mesh=mesh, in_specs=in_specs, out_specs=out_specs, check_vma=False
    )
```
